8 devices in a mesh: batch: 1 (over z), row: 2 (over y), col: 4 (over x, core).
Axes of the slice: x: 2, y: 2, z: 1, core: 2. Of those that a mesh axis runs over, the one named last changes fastest.
Arguments:
- lower_tri: bfloat16 [3072, 3072], P(('batch', 'row'), 'col')
- right_side: bfloat16 [3072, 16384], P(('batch', 'row'), 'col')
- grad_out: bfloat16 [3072, 16384], P(('batch', 'row'), 'col')
Outputs:
- output 1: bfloat16 [3072, 16384], P(('batch', 'row'), 'col')
- output 2: bfloat16 [3072, 3072], P(('batch', 'row'), 'col')
All inputs are finite; a program needn't handle non-finite values.
Results may differ from the reference program's by a relative error of at most 0.001.
Values are sent between devices in bfloat16 or wider.
A program may use at most 1 GiB of HBM per device.

```python
import jax
import jax.numpy as jnp

MAT_ORDER = 3072
BLOCK_SIZE = 256
RHS_COLS = 16384
MESH_ROWS = 2
MESH_COLS = 4
ROW_BLOCKS = MAT_ORDER // (BLOCK_SIZE * MESH_ROWS)
COL_BLOCKS = MAT_ORDER // (BLOCK_SIZE * MESH_COLS)


def rows_to_global(stored):
    num_cols = stored.shape[1]
    return stored.reshape(MESH_ROWS, ROW_BLOCKS, BLOCK_SIZE, num_cols).transpose(1, 0, 2, 3).reshape(MAT_ORDER, num_cols)


def rows_to_stored(natural):
    num_cols = natural.shape[1]
    return natural.reshape(ROW_BLOCKS, MESH_ROWS, BLOCK_SIZE, num_cols).transpose(1, 0, 2, 3).reshape(MAT_ORDER, num_cols)


def cols_to_global(stored):
    num_rows = stored.shape[0]
    return stored.reshape(num_rows, MESH_COLS, COL_BLOCKS, BLOCK_SIZE).transpose(0, 2, 1, 3).reshape(num_rows, MAT_ORDER)


def cols_to_stored(natural):
    num_rows = natural.shape[0]
    return natural.reshape(num_rows, COL_BLOCKS, MESH_COLS, BLOCK_SIZE).transpose(0, 2, 1, 3).reshape(num_rows, MAT_ORDER)


def setup_inputs(seed: int = 0, part: int = 0) -> dict:
    base_key = jax.random.fold_in(jax.random.key(seed), part)
    key_lower, key_right, key_grad = jax.random.split(base_key, 3)
    lower_mat = jax.random.normal(key_lower, (MAT_ORDER, MAT_ORDER), jnp.float32) * (MAT_ORDER ** -0.5)
    lower_mat = jnp.tril(lower_mat).astype(jnp.bfloat16)
    right_mat = jax.random.normal(key_right, (MAT_ORDER, RHS_COLS), jnp.float32) * (RHS_COLS ** -0.5)
    grad_mat = jax.random.normal(key_grad, (MAT_ORDER, RHS_COLS), jnp.float32)
    return {
        "lower_tri": cols_to_stored(rows_to_stored(lower_mat)),
        "right_side": rows_to_stored(right_mat.astype(jnp.bfloat16)),
        "grad_out": rows_to_stored(grad_mat.astype(jnp.bfloat16)),
    }


def reference(lower_tri, right_side, grad_out):
    lower_mat = cols_to_global(rows_to_global(lower_tri))
    right_mat = rows_to_global(right_side)
    grad_mat = rows_to_global(grad_out)
    grad_right = jnp.dot(lower_mat.T, grad_mat, preferred_element_type=jnp.float32)
    grad_lower = jnp.tril(jnp.dot(grad_mat, right_mat.T, preferred_element_type=jnp.float32))
    return (rows_to_stored(grad_right.astype(jnp.bfloat16)), cols_to_stored(rows_to_stored(grad_lower.astype(jnp.bfloat16))))
```

```python
import jax
import jax.numpy as jnp
from jax import lax
from jax.sharding import PartitionSpec as P

BLOCK_SIZE = 256
PAIR = 2 * BLOCK_SIZE


def dot_rows(lhs, rhs):
    return lax.dot_general(lhs, rhs, (((0,), (0,)), ((), ())), preferred_element_type=jnp.float32)


def dot_cols(lhs, rhs):
    return lax.dot_general(lhs, rhs, (((1,), (1,)), ((), ())), preferred_element_type=jnp.float32)


def solution(mesh):
    block_spec = P(("batch", "row"), "col")
    axes = ("row", "col")
    device = lambda row, col: row * 4 + col
    owners = [(row, 2 * x + row) for row in range(2) for x in range(2)]
    row_swap = [(0, 1), (1, 0)]
    cross_pairs = [(device(1 - row, col), device(row, col)) for row, col in owners]
    chip_pairs = [(device(row, col), device(row, (col + 2) % 4)) for row, col in owners]
    from_owner = [(device(row, col), device(row, col ^ 1)) for row, col in owners]
    to_owner = [(device(row, col ^ 1), device(row, col)) for row, col in owners]
    return_pairs = [(device(row, col), device(1 - row, col)) for row, col in owners]
    return_pairs_down = [(src, dst) for src, dst in return_pairs if src < 4]

    def per_device(lower_tri, right_side, grad_out):
        row = lax.axis_index("row")
        col = lax.axis_index("col")
        is_owner = (col % 2) == row
        is_left = (col // 2) == 0
        permute = lambda arr, pairs: lax.ppermute(arr, axes, pairs)

        other_45 = lax.ppermute(grad_out[1024:1536], "row", row_swap)
        packed = jnp.concatenate([lower_tri[PAIR * p:, BLOCK_SIZE * p:BLOCK_SIZE * (p + 1)] for p in range(3)], axis=0)
        packed_cross = permute(packed, cross_pairs)
        other_23 = lax.ppermute(grad_out[512:1024], "row", row_swap)
        other_1 = lax.ppermute(grad_out[256:512], "row", row_swap)
        other_0 = lax.ppermute(grad_out[0:256], "row", [(1, 0)])

        mine = jnp.concatenate([packed, packed_cross], axis=0)
        theirs = permute(mine, chip_pairs)
        even = jnp.where(is_left, mine, theirs)
        odd = jnp.where(is_left, theirs, mine)
        both = jnp.concatenate([even, odd], axis=1)
        both = jnp.where(is_owner, both, permute(both, from_owner))
        starts = [0, 1536, 2560]
        panel_own = [both[starts[p]:starts[p] + 1536 - PAIR * p] for p in range(3)]
        panel_oth = [both[3072 + starts[p]:3072 + starts[p] + 1536 - PAIR * p] for p in range(3)]

        def reduce_cols(parts):
            evens, odds = [], []
            for part in parts:
                for p in range(part.shape[1] // PAIR):
                    evens.append(part[:, PAIR * p:PAIR * p + BLOCK_SIZE])
                    odds.append(part[:, PAIR * p + BLOCK_SIZE:PAIR * (p + 1)])
            part = jnp.stack([jnp.concatenate(evens, axis=0), jnp.concatenate(odds, axis=0)])
            part = part + permute(part, to_owner)
            keep = jnp.where(is_left, part[0], part[1])
            send = jnp.where(is_left, part[1], part[0])
            return (keep + permute(send, chip_pairs)).astype(jnp.bfloat16)

        same = reduce_cols([dot_cols(grad_out[PAIR * p:PAIR * (p + 1)], right_side[:PAIR * (p + 1)]) for p in range(3)])
        same_blocks = [[same[0:512]], [same[512:1024], same[1024:1536]], [same[1536:2048], same[2048:2560], same[2560:3072]]]

        cross_a = reduce_cols([dot_cols(other_45, right_side)])
        cross_b = reduce_cols([dot_cols(other_23, right_side[:1024]), dot_cols(other_1, right_side[:512])])
        cross_c = reduce_cols([dot_cols(other_0, right_side[:512])])
        full_a = jnp.concatenate([cross_a[0:1024], cross_a[1280:1536]], axis=0)
        full_b = jnp.concatenate([cross_b[0:512], cross_b[768:1024], cross_b[1024:1280]], axis=0)
        got_a = permute(full_a, return_pairs)
        got_b = permute(full_b, return_pairs)
        got_c = permute(jnp.concatenate([cross_a[1024:1280], cross_b[512:768], cross_c], axis=0), return_pairs_down)
        cross_blocks = [
            [jnp.concatenate([got_c[512:768], got_b[768:1024]], axis=0)],
            [got_b[0:512], jnp.concatenate([got_c[256:512], got_b[512:768]], axis=0)],
            [got_a[0:512], got_a[512:1024], jnp.concatenate([got_c[0:256], got_a[1024:1280]], axis=0)],
        ]
        zero = jnp.zeros((PAIR, BLOCK_SIZE), jnp.bfloat16)
        assemble = lambda blocks: jnp.concatenate(
            [jnp.concatenate(blocks[q] + [zero] * (2 - q), axis=1) for q in range(3)], axis=0)
        grad_lower = jnp.where(is_owner, assemble(same_blocks), assemble(cross_blocks))
        row_pos = jnp.arange(1536)[:, None]
        col_pos = jnp.arange(768)[None, :]
        row_global = (row_pos // BLOCK_SIZE * 2 + row) * BLOCK_SIZE + row_pos % BLOCK_SIZE
        col_global = (col_pos // BLOCK_SIZE * 4 + col) * BLOCK_SIZE + col_pos % BLOCK_SIZE
        grad_lower = jnp.where(row_global >= col_global, grad_lower, 0.0).astype(jnp.bfloat16)

        sum_2 = dot_rows(panel_own[2], grad_out[1024:]) + dot_rows(panel_oth[2], other_45)
        sum_1 = (dot_rows(panel_own[1], grad_out[512:]) + dot_rows(panel_oth[1][512:], other_45)
                 + dot_rows(panel_oth[1][:512], other_23))
        sum_0 = (dot_rows(panel_own[0], grad_out) + dot_rows(panel_oth[0][1024:], other_45)
                 + dot_rows(panel_oth[0][512:1024], other_23) + dot_rows(panel_oth[0][256:512], other_1))
        last = sum_0[:256] + dot_rows(panel_oth[0][:256, :256], other_0)
        grad_right = jnp.zeros(grad_out.shape, jnp.bfloat16)
        for first, part in ((1024, sum_2), (512, sum_1), (256, sum_0[256:]), (0, last)):
            grad_right = lax.dynamic_update_slice(grad_right, part.astype(jnp.bfloat16), (first, 0))
        return grad_right, grad_lower

    return jax.shard_map(per_device, mesh=mesh, in_specs=(block_spec, block_spec, block_spec), out_specs=(block_spec, block_spec), check_vma=False)
```

```python
import jax
import jax.numpy as jnp
from jax import lax
from jax.experimental import pallas as pl
from jax.experimental.pallas import tpu as pltpu
from jax.sharding import PartitionSpec as P

MESH = pl.DeviceIdType.MESH
BLOCK = 256
NUM = 6
COLS = 4096
TILE = 512
VMEM_BYTES = 67043328
PANEL_START = (0, 6, 10)
FINAL_START = (0, 1, 2, 4, 6, 9)
COMMON = {(1, 0): 0, (2, 0): 1, (3, 0): 2, (3, 1): 3, (4, 0): 4, (4, 1): 5, (5, 0): 6, (5, 1): 7, (5, 2): 8}


def packed_row(p, m):
    return (PANEL_START[p] + m - 2 * p) * BLOCK


def dot_nt(lhs, rhs):
    return lax.dot_general(lhs, rhs, (((1,), (1,)), ((), ())), preferred_element_type=jnp.float32)


def kernel(lower, right, grad, out_right, out_same, out_cross, out_diag,
           grad_v, right_v, other_v, lower_v, slot, hop, fin_same, fin_cross, fin_diag, total, stage, turned,
           grad_send, grad_recv, load_sem, low_load, low_cross_send, low_cross_recv, low_send, low_recv,
           core_send, core_recv, hop_send, hop_recv, out_sem, fin_sem, core_free, hop_free):
    row = lax.axis_index("row")
    col = lax.axis_index("col")
    x = col // 2
    owner = (col % 2) == row
    guest = jnp.logical_not(owner)
    to_row = {"row": 1 - row}
    to_core = {"col": col + 1 - 2 * (col % 2)}
    to_chip = {"col": lax.rem(col + 2, 4)}

    def remote(src, dst, send, recv, where):
        return pltpu.make_async_remote_copy(src_ref=src, dst_ref=dst, send_sem=send, recv_sem=recv, device_id=where, device_id_type=MESH)

    def send_grad(m):
        return remote(grad.at[pl.ds(m * BLOCK, BLOCK)], other_v.at[pl.ds(m * BLOCK, BLOCK)], grad_send.at[m], grad_recv.at[m], to_row)

    def panel_src(p):
        return lower.at[pl.ds(2 * p * BLOCK, (NUM - 2 * p) * BLOCK), pl.ds(p * BLOCK, BLOCK)]

    def panel_dst(parity, p):
        return lower_v.at[x, parity, pl.ds(PANEL_START[p] * BLOCK, (NUM - 2 * p) * BLOCK)]

    def send_panel(p):
        return remote(panel_src(p), panel_dst(1, p), low_cross_send.at[p], low_cross_recv.at[p], to_row)

    def send_low(index, half, where):
        return remote(lower_v.at[half], lower_v.at[half], low_send.at[index], low_recv.at[index], where)

    def load(src, dst, m, k):
        return pltpu.make_async_copy(src.at[pl.ds(m * BLOCK, BLOCK)], dst.at[pl.ds(m * BLOCK, BLOCK)], load_sem.at[k, m])

    def send_core(group, m):
        part = slot.at[pl.ds(m * (m + 1) // 2, m + 1)]
        return remote(part, part, core_send.at[group, m], core_recv.at[group, m], to_core)

    def send_hop(group, m, side):
        base = m * (m + 1) // 2
        first, count = (base + m // 2 + 1, (m + 1) // 2) if side == 0 else (base, m // 2 + 1)
        return remote(slot.at[pl.ds(first, count)], hop.at[pl.ds(FINAL_START[m], count)], hop_send.at[group, m], hop_recv.at[group, m], to_chip)

    barrier = pltpu.get_barrier_semaphore()
    for where in (to_row, to_core, to_chip):
        pl.semaphore_signal(barrier, inc=1, device_id=where, device_id_type=MESH)
    pl.semaphore_wait(barrier, 3)

    @pl.when(guest)
    def _():
        for p in range(3):
            send_panel(p).start()

    for m in range(NUM - 1, 0, -1):
        send_grad(m).start()

    @pl.when(row == 1)
    def _():
        send_grad(0).start()

    for m in range(NUM):
        load(grad, grad_v, m, 0).start()
        load(right, right_v, m, 1).start()

    @pl.when(owner)
    def _():
        for p in range(3):
            pltpu.make_async_copy(panel_src(p), panel_dst(0, p), low_load.at[p]).start()

    def partial_sums(source, group, m):
        @pl.when(owner)
        def _():
            send_core(group, m).wait_recv()

        def one(n, carry):
            index = m * (m + 1) // 2 + (n % 2) * (m // 2 + 1) + n // 2
            value = dot_nt(source[pl.ds(m * BLOCK, BLOCK), :], right_v[pl.ds(pl.multiple_of(n * BLOCK, BLOCK), BLOCK), :])
            slot[index] = jnp.where(owner, slot[index], 0.0) + value
            return carry

        lax.fori_loop(0, m + 1, one, 0)

        @pl.when(guest)
        def _():
            send_core(group, m).start()

        for side in range(2):
            if side == 1 or m > 0:
                @pl.when(jnp.logical_and(owner, x == side))
                def _(side=side):
                    send_hop(group, m, side).start()

    def finish(group, m):
        for side in range(2):
            @pl.when(jnp.logical_and(owner, x == side))
            def _(side=side):
                if side == 0 or m > 0:
                    send_hop(group, m, 1 - side).wait_recv()
                if side == 1 or m > 0:
                    send_hop(group, m, side).wait_send()
                for p in range(m // 2 + 1):
                    n = 2 * p + side
                    target, place = (fin_cross, COMMON[m, p]) if (m, p) in COMMON else (fin_diag, m // 2)
                    if group == 0:
                        target, place = fin_same, FINAL_START[m] + p
                    if n > m:
                        target[place] = jnp.zeros((BLOCK, BLOCK), jnp.bfloat16)
                        continue
                    value = slot[m * (m + 1) // 2 + side * (m // 2 + 1) + p] + hop[FINAL_START[m] + p]
                    if n == m and group == 0:
                        rows = lax.broadcasted_iota(jnp.int32, (BLOCK, BLOCK), 0)
                        cols = lax.broadcasted_iota(jnp.int32, (BLOCK, BLOCK), 1)
                        value = jnp.where(rows >= cols, value, 0.0)
                    if n == m and group == 1:
                        value = jnp.where(row == 0, value, 0.0)
                    target[place] = value.astype(jnp.bfloat16)

    for m in range(NUM):
        load(grad, grad_v, m, 0).wait()
        load(right, right_v, m, 1).wait()
        partial_sums(grad_v, 0, m)

    @pl.when(owner)
    def _():
        for p in range(3):
            pltpu.make_async_copy(panel_src(p), panel_dst(0, p), low_load.at[p]).wait()
            send_panel(p).wait_recv()
        send_low(0, x, to_chip).start()
        send_low(1, x, to_core).start()

    for m in range(NUM):
        finish(0, m)

    @pl.when(owner)
    def _():
        pl.semaphore_signal(core_free, inc=1, device_id=to_core, device_id_type=MESH)
        pl.semaphore_signal(hop_free, inc=1, device_id=to_chip, device_id_type=MESH)
        send_low(0, 1 - x, to_chip).wait_recv()
        send_low(2, 1 - x, to_core).start()
        pl.semaphore_wait(hop_free, 1)

    @pl.when(guest)
    def _():
        send_low(1, x, to_core).wait_recv()
        send_low(2, 1 - x, to_core).wait_recv()
        for m in range(NUM):
            send_core(0, m).wait_send()
        pl.semaphore_wait(core_free, 1)

    def turn(n):
        p, half = n // 2, n % 2
        for parity in range(2):
            for m in range(n, NUM):
                turned[parity, :, pl.ds((m - n) * BLOCK, BLOCK)] = lower_v[half, parity, pl.ds(packed_row(p, m), BLOCK), :].T

    def put(n):
        return pltpu.make_async_copy(stage, out_right.at[pl.ds(n * BLOCK, BLOCK)], out_sem)

    def tiles(body):
        def one(t, carry):
            body(pl.ds(pl.multiple_of(t * TILE, TILE), TILE))
            return carry
        lax.fori_loop(0, COLS // TILE, one, 0)

    for m in range(NUM - 1, 0, -1):
        send_grad(m).wait_recv()
        partial_sums(other_v, 1, m)
        turn(m)
        if m < NUM - 1:
            put(m + 1).wait()
        depth = (NUM - m) * BLOCK

        def product(cols, m=m, depth=depth):
            value = jnp.dot(turned[0, :, :depth], grad_v[m * BLOCK:, cols], preferred_element_type=jnp.float32)
            value += jnp.dot(turned[1, :, :depth], other_v[m * BLOCK:, cols], preferred_element_type=jnp.float32)
            stage[:, cols] = value.astype(jnp.bfloat16)

        tiles(product)
        put(m).start()
        if m < NUM - 1:
            finish(1, m + 1)

    turn(0)

    def all_but_last(cols):
        value = jnp.dot(turned[0], grad_v[:, cols], preferred_element_type=jnp.float32)
        total[:, cols] = value + jnp.dot(turned[1, :, BLOCK:], other_v[BLOCK:, cols], preferred_element_type=jnp.float32)

    tiles(all_but_last)
    finish(1, 1)
    put(1).wait()

    @pl.when(row == 0)
    def _():
        send_grad(0).wait_recv()
        partial_sums(other_v, 1, 0)

        def last(cols):
            value = jnp.dot(turned[1, :, :BLOCK], other_v[:BLOCK, cols], preferred_element_type=jnp.float32)
            stage[:, cols] = (total[:, cols] + value).astype(jnp.bfloat16)

        tiles(last)
        put(0).start()
        finish(1, 0)

    @pl.when(row == 1)
    def _():
        def last(cols):
            stage[:, cols] = total[:, cols].astype(jnp.bfloat16)

        tiles(last)
        put(0).start()
        fin_diag[0] = jnp.zeros((BLOCK, BLOCK), jnp.bfloat16)

    @pl.when(owner)
    def _():
        copies = [pltpu.make_async_copy(src, dst, fin_sem.at[k])
                  for k, (src, dst) in enumerate(((fin_same, out_same), (fin_cross, out_cross), (fin_diag, out_diag)))]
        for copy in copies:
            copy.start()
        for copy in copies:
            copy.wait()

    put(0).wait()
    for m in range(NUM - 1, 0, -1):
        send_grad(m).wait_send()

    @pl.when(row == 1)
    def _():
        send_grad(0).wait_send()

    @pl.when(owner)
    def _():
        send_low(0, x, to_chip).wait_send()
        send_low(1, x, to_core).wait_send()
        send_low(2, 1 - x, to_core).wait_send()

    @pl.when(guest)
    def _():
        for p in range(3):
            send_panel(p).wait_send()
        for m in range(1, NUM):
            send_core(1, m).wait_send()

        @pl.when(row == 0)
        def _():
            send_core(1, 0).wait_send()


def solution(mesh):
    block_spec = P(("batch", "row"), "col")
    device = lambda row, col: row * 4 + col
    owners = [(row, 2 * chip + row) for row in range(2) for chip in range(2)]
    return_pairs = [(device(row, col), device(1 - row, col)) for row, col in owners]
    return_pairs_down = [(src, dst) for src, dst in return_pairs if src < 4]

    def per_device(lower_tri, right_side, grad_out):
        bf16, f32 = jnp.bfloat16, jnp.float32
        dma = pltpu.SemaphoreType.DMA
        block = lambda count: jax.ShapeDtypeStruct((count, BLOCK, BLOCK), bf16)
        hbm = pl.BlockSpec(memory_space=pl.ANY)
        grad_right, same, cross, diag = pl.pallas_call(
            kernel,
            out_shape=(jax.ShapeDtypeStruct(grad_out.shape, bf16), block(12), block(9), block(3)),
            in_specs=[hbm] * 3,
            out_specs=[hbm] * 4,
            scratch_shapes=[
                pltpu.VMEM((NUM * BLOCK, COLS), bf16), pltpu.VMEM((NUM * BLOCK, COLS), bf16), pltpu.VMEM((NUM * BLOCK, COLS), bf16),
                pltpu.VMEM((2, 2, 12 * BLOCK, BLOCK), bf16),
                pltpu.VMEM((21, BLOCK, BLOCK), f32), pltpu.VMEM((12, BLOCK, BLOCK), f32),
                pltpu.VMEM((12, BLOCK, BLOCK), bf16), pltpu.VMEM((9, BLOCK, BLOCK), bf16), pltpu.VMEM((3, BLOCK, BLOCK), bf16),
                pltpu.VMEM((BLOCK, COLS), f32), pltpu.VMEM((BLOCK, COLS), bf16), pltpu.VMEM((2, BLOCK, NUM * BLOCK), bf16),
                dma((NUM,)), dma((NUM,)), dma((2, NUM)), dma((3,)), dma((3,)), dma((3,)), dma((3,)), dma((3,)),
                dma((2, NUM)), dma((2, NUM)), dma((2, NUM)), dma((2, NUM)), dma, dma((3,)),
                pltpu.SemaphoreType.REGULAR, pltpu.SemaphoreType.REGULAR,
            ],
            compiler_params=pltpu.CompilerParams(collective_id=1, has_side_effects=True, vmem_limit_bytes=VMEM_BYTES),
        )(lower_tri, right_side, grad_out)

        got = lax.ppermute(cross, ("row", "col"), return_pairs)
        got_diag = lax.ppermute(diag, ("row", "col"), return_pairs_down)
        row, col = lax.axis_index("row"), lax.axis_index("col")
        is_owner = (col % 2) == row
        zero = jnp.zeros((BLOCK, BLOCK), bf16)

        def piece(m, p):
            if p > m // 2:
                return zero
            moved = got[COMMON[m, p]] if (m, p) in COMMON else got_diag[m // 2]
            return jnp.where(is_owner, same[FINAL_START[m] + p], moved)

        grad_lower = jnp.concatenate([jnp.concatenate([piece(m, p) for p in range(3)], axis=1) for m in range(NUM)], axis=0)
        return grad_right, grad_lower

    return jax.shard_map(per_device, mesh=mesh, in_specs=(block_spec, block_spec, block_spec), out_specs=(block_spec, block_spec), check_vma=False)
```

```python
import jax
import jax.numpy as jnp
from jax import lax
from jax.experimental import pallas as pl
from jax.experimental.pallas import tpu as pltpu
from jax.sharding import PartitionSpec as P

MESH = pl.DeviceIdType.MESH
BLOCK = 256
NUM = 6
COLS = 4096
TILE = 512
VMEM_BYTES = 67043328
PANEL_START = (0, 6, 10)
FINAL_START = (0, 1, 2, 4, 6, 9)
COMMON = {(1, 0): 0, (2, 0): 1, (3, 0): 2, (3, 1): 3, (4, 0): 4, (4, 1): 5, (5, 0): 6, (5, 1): 7, (5, 2): 8}


RETURNED = 6
RETURNED_FROM = 5
COPY_PARTS = 12


def packed(p, m):
    return PANEL_START[p] + m - 2 * p


def dot_nt(lhs, rhs):
    return lax.dot_general(lhs, rhs, (((1,), (1,)), ((), ())), preferred_element_type=jnp.float32)


def kernel(lower, right, grad, out_right, out_same, out_cross, out_diag, out_back,
           grad_v, right_v, other_v, lower_v, slot, hop, fin_same, fin_cross, fin_diag, total, stage, turned,
           grad_send, grad_recv, load_sem, low_load, low_cross_send, low_cross_recv, low_send, low_recv,
           core_send, core_recv, hop_send, hop_recv, back_send, back_recv, out_sem, fin_sem, core_free, hop_free):
    row = lax.axis_index("row")
    col = lax.axis_index("col")
    x = col // 2
    owner = (col % 2) == row
    guest = jnp.logical_not(owner)
    to_row = {"row": 1 - row}
    to_core = {"col": col + 1 - 2 * (col % 2)}
    to_chip = {"col": lax.rem(col + 2, 4)}
    to_diag = {"row": 1 - row, "col": col + 1 - 2 * (col % 2)}

    def remote(src, dst, send, recv, where):
        return pltpu.make_async_remote_copy(src_ref=src, dst_ref=dst, send_sem=send, recv_sem=recv, device_id=where, device_id_type=MESH)

    def send_grad(m):
        return remote(grad.at[pl.ds(m * BLOCK, BLOCK)], other_v.at[pl.ds(m * BLOCK, BLOCK)], grad_send.at[m], grad_recv.at[m], to_row)

    def load_low(target, p, m):
        return pltpu.make_async_copy(lower.at[pl.ds(m * BLOCK, BLOCK), pl.ds(p * BLOCK, BLOCK)], target.at[packed(p, m)], low_load.at[packed(p, m)])

    def each_low(target, act):
        for p in range(3):
            for m in range(2 * p, NUM):
                act(load_low(target, p, m))

    def cross_near():
        return remote(fin_same.at[pl.ds(0, 6)], lower_v.at[x, 1, pl.ds(0, 6)], low_cross_send.at[0], low_cross_recv.at[0], to_row)

    def cross_hand():
        return remote(fin_same.at[pl.ds(6, 6)], fin_cross.at[pl.ds(0, 6)], low_cross_send.at[1], low_cross_recv.at[1], to_core)

    def cross_far():
        return remote(fin_cross.at[pl.ds(0, 6)], lower_v.at[x, 1, pl.ds(6, 6)], low_cross_send.at[2], low_cross_recv.at[2], to_diag)

    def send_back():
        part = fin_cross.at[pl.ds(RETURNED, 9 - RETURNED)]
        return remote(part, part, back_send, back_recv, to_row)

    def send_low(index, half, where):
        return remote(lower_v.at[half], lower_v.at[half], low_send.at[index], low_recv.at[index], where)

    def load(src, dst, m, k):
        return pltpu.make_async_copy(src.at[pl.ds(m * BLOCK, BLOCK)], dst.at[pl.ds(m * BLOCK, BLOCK)], load_sem.at[k, m])

    def send_core(group, m):
        part = slot.at[pl.ds(m * (m + 1) // 2, m + 1)]
        return remote(part, part, core_send.at[group, m], core_recv.at[group, m], to_core)

    def send_hop(group, m, side):
        base = m * (m + 1) // 2
        first, count = (base + m // 2 + 1, (m + 1) // 2) if side == 0 else (base, m // 2 + 1)
        return remote(slot.at[pl.ds(first, count)], hop.at[pl.ds(FINAL_START[m], count)], hop_send.at[group, m], hop_recv.at[group, m], to_chip)

    barrier = pltpu.get_barrier_semaphore()
    for where in (to_row, to_core, to_chip, to_diag):
        pl.semaphore_signal(barrier, inc=1, device_id=where, device_id_type=MESH)
    pl.semaphore_wait(barrier, 4)

    send_grad(NUM - 1).start()

    @pl.when(guest)
    def _():
        each_low(fin_same, lambda copy: copy.start())

    @pl.when(owner)
    def _():
        each_low(lower_v.at[x, 0], lambda copy: copy.start())

    for m in range(NUM):
        load(grad, grad_v, m, 0).start()
        load(right, right_v, m, 1).start()

    @pl.when(guest)
    def _():
        each_low(fin_same, lambda copy: copy.wait())
        cross_hand().start()
        cross_near().start()

    @pl.when(owner)
    def _():
        cross_hand().wait_recv()
        cross_far().start()

    for m in range(NUM - 2, 0, -1):
        send_grad(m).start()

    @pl.when(row == 1)
    def _():
        send_grad(0).start()

    def partial_sums(source, group, m):
        @pl.when(owner)
        def _():
            send_core(group, m).wait_recv()

        def one(n, carry):
            index = m * (m + 1) // 2 + (n % 2) * (m // 2 + 1) + n // 2
            value = dot_nt(source[pl.ds(m * BLOCK, BLOCK), :], right_v[pl.ds(pl.multiple_of(n * BLOCK, BLOCK), BLOCK), :])
            slot[index] = jnp.where(owner, slot[index], 0.0) + value
            return carry

        lax.fori_loop(0, m + 1, one, 0)

        @pl.when(guest)
        def _():
            send_core(group, m).start()

        for side in range(2):
            if side == 1 or m > 0:
                @pl.when(jnp.logical_and(owner, x == side))
                def _(side=side):
                    send_hop(group, m, side).start()

    def finish(group, m):
        for side in range(2):
            @pl.when(jnp.logical_and(owner, x == side))
            def _(side=side):
                if side == 0 or m > 0:
                    send_hop(group, m, 1 - side).wait_recv()
                if side == 1 or m > 0:
                    send_hop(group, m, side).wait_send()
                for p in range(m // 2 + 1):
                    n = 2 * p + side
                    target, place = (fin_cross, COMMON[m, p]) if (m, p) in COMMON else (fin_diag, m // 2)
                    if group == 0:
                        target, place = fin_same, FINAL_START[m] + p
                    if n > m:
                        target[place] = jnp.zeros((BLOCK, BLOCK), jnp.bfloat16)
                        continue
                    value = slot[m * (m + 1) // 2 + side * (m // 2 + 1) + p] + hop[FINAL_START[m] + p]
                    if n == m and group == 0:
                        rows = lax.broadcasted_iota(jnp.int32, (BLOCK, BLOCK), 0)
                        cols = lax.broadcasted_iota(jnp.int32, (BLOCK, BLOCK), 1)
                        value = jnp.where(rows >= cols, value, 0.0)
                    if n == m and group == 1:
                        value = jnp.where(row == 0, value, 0.0)
                    target[place] = value.astype(jnp.bfloat16)

    for m in range(NUM):
        load(grad, grad_v, m, 0).wait()
        load(right, right_v, m, 1).wait()
        partial_sums(grad_v, 0, m)

    @pl.when(owner)
    def _():
        each_low(lower_v.at[x, 0], lambda copy: copy.wait())
        cross_near().wait_recv()
        cross_far().wait_recv()
        send_low(0, x, to_chip).start()
        send_low(1, x, to_core).start()

    for m in range(NUM):
        finish(0, m)

    @pl.when(owner)
    def _():
        pl.semaphore_signal(core_free, inc=1, device_id=to_core, device_id_type=MESH)
        pl.semaphore_signal(hop_free, inc=1, device_id=to_chip, device_id_type=MESH)
        send_low(0, 1 - x, to_chip).wait_recv()
        send_low(2, 1 - x, to_core).start()
        pl.semaphore_wait(hop_free, 1)
        cross_far().wait_send()

    @pl.when(guest)
    def _():
        send_low(1, x, to_core).wait_recv()
        send_low(2, 1 - x, to_core).wait_recv()
        for m in range(NUM):
            send_core(0, m).wait_send()
        pl.semaphore_wait(core_free, 1)

    def turn(n):
        p, half = n // 2, n % 2
        for parity in range(2):
            for m in range(n, NUM):
                turned[parity, :, pl.ds((m - n) * BLOCK, BLOCK)] = lower_v[half, parity, packed(p, m)].T

    def put(n):
        return pltpu.make_async_copy(stage, out_right.at[pl.ds(n * BLOCK, BLOCK)], out_sem)

    def tiles(body):
        def one(t, carry):
            body(pl.ds(pl.multiple_of(t * TILE, TILE), TILE))
            return carry
        lax.fori_loop(0, COLS // TILE, one, 0)

    for m in range(NUM - 1, 0, -1):
        send_grad(m).wait_recv()
        partial_sums(other_v, 1, m)
        turn(m)
        if m < NUM - 1:
            put(m + 1).wait()
        depth = (NUM - m) * BLOCK

        def product(cols, m=m, depth=depth):
            value = jnp.dot(turned[0, :, :depth], grad_v[m * BLOCK:, cols], preferred_element_type=jnp.float32)
            value += jnp.dot(turned[1, :, :depth], other_v[m * BLOCK:, cols], preferred_element_type=jnp.float32)
            stage[:, cols] = value.astype(jnp.bfloat16)

        tiles(product)
        put(m).start()
        if m < NUM - 1:
            finish(1, m + 1)
        if m + 1 == RETURNED_FROM:
            @pl.when(owner)
            def _():
                send_back().start()

    turn(0)

    def all_but_last(cols):
        value = jnp.dot(turned[0], grad_v[:, cols], preferred_element_type=jnp.float32)
        total[:, cols] = value + jnp.dot(turned[1, :, BLOCK:], other_v[BLOCK:, cols], preferred_element_type=jnp.float32)

    tiles(all_but_last)
    finish(1, 1)
    put(1).wait()

    @pl.when(row == 0)
    def _():
        send_grad(0).wait_recv()
        partial_sums(other_v, 1, 0)

        def last(cols):
            value = jnp.dot(turned[1, :, :BLOCK], other_v[:BLOCK, cols], preferred_element_type=jnp.float32)
            stage[:, cols] = (total[:, cols] + value).astype(jnp.bfloat16)

        tiles(last)
        put(0).start()
        finish(1, 0)

    @pl.when(row == 1)
    def _():
        def last(cols):
            stage[:, cols] = total[:, cols].astype(jnp.bfloat16)

        tiles(last)
        put(0).start()
        fin_diag[0] = jnp.zeros((BLOCK, BLOCK), jnp.bfloat16)

    @pl.when(owner)
    def _():
        copies = [pltpu.make_async_copy(src, dst, fin_sem.at[k])
                  for k, (src, dst) in enumerate(((fin_same, out_same), (fin_cross.at[pl.ds(0, RETURNED)], out_cross), (fin_diag, out_diag)))]
        for copy in copies:
            copy.start()
        for copy in copies:
            copy.wait()
        send_back().wait_send()

    @pl.when(guest)
    def _():
        send_back().wait_recv()
        copy = pltpu.make_async_copy(fin_cross.at[pl.ds(RETURNED, 9 - RETURNED)], out_back, fin_sem.at[0])
        copy.start()
        copy.wait()

    put(0).wait()
    for m in range(NUM - 1, 0, -1):
        send_grad(m).wait_send()

    @pl.when(row == 1)
    def _():
        send_grad(0).wait_send()

    @pl.when(owner)
    def _():
        send_low(0, x, to_chip).wait_send()
        send_low(1, x, to_core).wait_send()
        send_low(2, 1 - x, to_core).wait_send()

    @pl.when(guest)
    def _():
        cross_hand().wait_send()
        cross_near().wait_send()
        for m in range(1, NUM):
            send_core(1, m).wait_send()

        @pl.when(row == 0)
        def _():
            send_core(1, 0).wait_send()


def copy_kernel(source, target, buffer, read_sem, write_sem):
    rows = source.shape[0] // COPY_PARTS
    part = lambda ref, k: ref.at[pl.ds(k * rows, rows)]
    reads = [pltpu.make_async_copy(part(source, k), part(buffer, k), read_sem.at[k]) for k in range(COPY_PARTS)]
    writes = [pltpu.make_async_copy(part(buffer, k), part(target, k), write_sem.at[k]) for k in range(COPY_PARTS)]
    for read in reads:
        read.start()
    for read, write in zip(reads, writes):
        read.wait()
        write.start()
    for write in writes:
        write.wait()


def solution(mesh):
    block_spec = P(("batch", "row"), "col")
    device = lambda row, col: row * 4 + col
    owners = [(row, 2 * chip + row) for row in range(2) for chip in range(2)]
    return_pairs = [(device(row, col), device(1 - row, col)) for row, col in owners]
    return_pairs_down = [(src, dst) for src, dst in return_pairs if src < 4]

    def per_device(lower_tri, right_side, grad_out):
        bf16, f32 = jnp.bfloat16, jnp.float32
        dma = pltpu.SemaphoreType.DMA
        block = lambda count: jax.ShapeDtypeStruct((count, BLOCK, BLOCK), bf16)
        hbm = pl.BlockSpec(memory_space=pl.ANY)
        right_here, same, cross, diag, back = pl.pallas_call(
            kernel,
            out_shape=(jax.ShapeDtypeStruct(grad_out.shape, bf16), block(12), block(RETURNED), block(3), block(9 - RETURNED)),
            in_specs=[hbm] * 3,
            out_specs=[hbm] * 5,
            scratch_shapes=[
                pltpu.VMEM((NUM * BLOCK, COLS), bf16), pltpu.VMEM((NUM * BLOCK, COLS), bf16), pltpu.VMEM((NUM * BLOCK, COLS), bf16),
                pltpu.VMEM((2, 2, 12, BLOCK, BLOCK), bf16),
                pltpu.VMEM((21, BLOCK, BLOCK), f32), pltpu.VMEM((12, BLOCK, BLOCK), f32),
                pltpu.VMEM((12, BLOCK, BLOCK), bf16), pltpu.VMEM((9, BLOCK, BLOCK), bf16), pltpu.VMEM((3, BLOCK, BLOCK), bf16),
                pltpu.VMEM((BLOCK, COLS), f32), pltpu.VMEM((BLOCK, COLS), bf16), pltpu.VMEM((2, BLOCK, NUM * BLOCK), bf16),
                dma((NUM,)), dma((NUM,)), dma((2, NUM)), dma((12,)), dma((3,)), dma((3,)), dma((3,)), dma((3,)),
                dma((2, NUM)), dma((2, NUM)), dma((2, NUM)), dma((2, NUM)), dma, dma, dma, dma((3,)),
                pltpu.SemaphoreType.REGULAR, pltpu.SemaphoreType.REGULAR,
            ],
            compiler_params=pltpu.CompilerParams(collective_id=1, has_side_effects=True, vmem_limit_bytes=VMEM_BYTES),
        )(lower_tri, right_side, grad_out)

        grad_right = pl.pallas_call(
            copy_kernel,
            out_shape=jax.ShapeDtypeStruct(grad_out.shape, bf16),
            in_specs=[hbm],
            out_specs=hbm,
            scratch_shapes=[pltpu.VMEM(grad_out.shape, bf16), dma((COPY_PARTS,)), dma((COPY_PARTS,))],
            cost_estimate=pl.CostEstimate(flops=10 ** 10, bytes_accessed=4 * grad_out.size, transcendentals=0),
        )(right_here)
        got = lax.ppermute(cross, ("row", "col"), return_pairs)
        got_diag = lax.ppermute(diag, ("row", "col"), return_pairs_down)
        row, col = lax.axis_index("row"), lax.axis_index("col")
        is_owner = (col % 2) == row
        zero = jnp.zeros((BLOCK, BLOCK), bf16)

        def piece(m, p):
            if p > m // 2:
                return zero
            place = COMMON.get((m, p))
            if place is None:
                moved = got_diag[m // 2]
            else:
                moved = got[place] if place < RETURNED else back[place - RETURNED]
            return jnp.where(is_owner, same[FINAL_START[m] + p], moved)

        grad_lower = jnp.concatenate([jnp.concatenate([piece(m, p) for p in range(3)], axis=1) for m in range(NUM)], axis=0)
        return grad_right, grad_lower

    return jax.shard_map(per_device, mesh=mesh, in_specs=(block_spec, block_spec, block_spec), out_specs=(block_spec, block_spec), check_vma=False)
```

```python
import jax
import jax.numpy as jnp
from jax import lax
from jax.experimental import pallas as pl
from jax.experimental.pallas import tpu as pltpu
from jax.sharding import PartitionSpec as P

MESH = pl.DeviceIdType.MESH
BLOCK = 256
NUM = 6
COLS = 4096
TILE = 512
LAST = 1024
VMEM_BYTES = 67043328
HOP_START = (0, 1, 2, 4, 6, 9)
PLACE = {(1, 0): 0, (2, 0): 1, (3, 0): 2, (3, 1): 3, (4, 0): 4, (4, 1): 5, (5, 0): 6, (5, 1): 7, (5, 2): 8, (0, 0): 9, (2, 1): 10, (4, 2): 11}
RETURNED = 6
RETURNED_FROM = 5
COPY_PARTS = 12


def dot_nt(lhs, rhs):
    return lax.dot_general(lhs, rhs, (((1,), (1,)), ((), ())), preferred_element_type=jnp.float32)


def kernel(lower, right, grad, out_right, out_low, out_cross,
           grad_v, right_v, other_v, lower_v, slot, hop, fin_same, fin_cross, total, stage, turned,
           grad_send, grad_recv, load_sem, low_load, low_cross_send, low_cross_recv, low_send, low_recv,
           core_send, core_recv, hop_send, hop_recv, back_send, back_recv, corner_send, corner_recv, out_sem, last_sem, fin_sem, core_free, hop_free):
    row = lax.axis_index("row")
    col = lax.axis_index("col")
    x = col // 2
    owner = (col % 2) == row
    guest = jnp.logical_not(owner)
    to_row = {"row": 1 - row}
    to_core = {"col": col + 1 - 2 * (col % 2)}
    to_chip = {"col": lax.rem(col + 2, 4)}
    to_diag = {"row": 1 - row, "col": col + 1 - 2 * (col % 2)}

    def remote(src, dst, send, recv, where):
        return pltpu.make_async_remote_copy(src_ref=src, dst_ref=dst, send_sem=send, recv_sem=recv, device_id=where, device_id_type=MESH)

    def send_grad(m):
        return remote(grad.at[pl.ds(m * BLOCK, BLOCK)], other_v.at[pl.ds(m * BLOCK, BLOCK)], grad_send.at[m], grad_recv.at[m], to_row)

    def send_right():
        return remote(right.at[pl.ds(0, BLOCK)], other_v.at[pl.ds(0, BLOCK)], grad_send.at[0], grad_recv.at[0], to_row)

    def load_low(target, p, m):
        return pltpu.make_async_copy(lower.at[pl.ds(m * BLOCK, BLOCK), pl.ds(p * BLOCK, BLOCK)], target.at[PLACE[m, p]], low_load.at[PLACE[m, p]])

    def each_low(target, act):
        for p in range(3):
            for m in range(2 * p, NUM):
                act(load_low(target, p, m))

    def cross_near():
        return remote(fin_same.at[pl.ds(0, 6)], lower_v.at[x, 1, pl.ds(0, 6)], low_cross_send.at[0], low_cross_recv.at[0], to_row)

    def cross_hand():
        return remote(fin_same.at[pl.ds(6, 6)], fin_cross.at[pl.ds(0, 6)], low_cross_send.at[1], low_cross_recv.at[1], to_core)

    def cross_far(count):
        return remote(fin_cross.at[pl.ds(0, count)], lower_v.at[x, 1, pl.ds(6, count)], low_cross_send.at[2], low_cross_recv.at[2], to_diag)

    def send_back():
        part = fin_cross.at[pl.ds(RETURNED, 9 - RETURNED)]
        return remote(part, part, back_send.at[0], back_recv.at[0], to_row)

    def send_back_down():
        part = fin_cross.at[pl.ds(10, 2)]
        return remote(part, part, back_send.at[1], back_recv.at[1], to_row)

    def send_low(index, half, where):
        return remote(lower_v.at[half], lower_v.at[half], low_send.at[index], low_recv.at[index], where)

    def load(src, dst, m, k):
        return pltpu.make_async_copy(src.at[pl.ds(m * BLOCK, BLOCK)], dst.at[pl.ds(m * BLOCK, BLOCK)], load_sem.at[k, m])

    def send_core(group, m):
        part = slot.at[pl.ds(m * (m + 1) // 2, m + 1)]
        return remote(part, part, core_send.at[group, m], core_recv.at[group, m], to_core)

    def send_hop(group, m, side):
        base = m * (m + 1) // 2
        first, count = (base + m // 2 + 1, (m + 1) // 2) if side == 0 else (base, m // 2 + 1)
        return remote(slot.at[pl.ds(first, count)], hop.at[pl.ds(HOP_START[m], count)], hop_send.at[group, m], hop_recv.at[group, m], to_chip)

    @pl.when(guest)
    def _():
        fin_cross[9:] = jnp.zeros((3, BLOCK, BLOCK), jnp.bfloat16)

    barrier = pltpu.get_barrier_semaphore()
    for where in (to_row, to_core, to_chip, to_diag):
        pl.semaphore_signal(barrier, inc=1, device_id=where, device_id_type=MESH)
    pl.semaphore_wait(barrier, 4)

    send_grad(NUM - 1).start()

    @pl.when(guest)
    def _():
        each_low(fin_same, lambda copy: copy.start())

    @pl.when(owner)
    def _():
        each_low(lower_v.at[x, 0], lambda copy: copy.start())

    for m in range(NUM):
        load(grad, grad_v, m, 0).start()
        load(right, right_v, m, 1).start()

    @pl.when(guest)
    def _():
        each_low(fin_same, lambda copy: copy.wait())
        cross_hand().start()
        cross_near().start()

    @pl.when(owner)
    def _():
        cross_hand().wait_recv()

        @pl.when(row == 0)
        def _():
            cross_far(3).start()

        @pl.when(row == 1)
        def _():
            lower_v[x, 1, 9:] = jnp.zeros((3, BLOCK, BLOCK), jnp.bfloat16)
            cross_far(6).start()

    for m in range(NUM - 2, 0, -1):
        send_grad(m).start()

    @pl.when(row == 0)
    def _():
        send_right().start()

    @pl.when(row == 1)
    def _():
        send_grad(0).start()

    def partial_sums(source, group, m):
        @pl.when(owner)
        def _():
            send_core(group, m).wait_recv()

        def one(n, carry):
            index = m * (m + 1) // 2 + (n % 2) * (m // 2 + 1) + n // 2
            value = dot_nt(source[pl.ds(m * BLOCK, BLOCK), :], right_v[pl.ds(pl.multiple_of(n * BLOCK, BLOCK), BLOCK), :])
            slot[index] = jnp.where(owner, slot[index], 0.0) + value
            return carry

        lax.fori_loop(0, m + 1, one, 0)

        @pl.when(guest)
        def _():
            send_core(group, m).start()

        for side in range(2):
            if side == 1 or m > 0:
                @pl.when(jnp.logical_and(owner, x == side))
                def _(side=side):
                    send_hop(group, m, side).start()

    def finish(group, m):
        for side in range(2):
            @pl.when(jnp.logical_and(owner, x == side))
            def _(side=side):
                if side == 0 or m > 0:
                    send_hop(group, m, 1 - side).wait_recv()
                if side == 1 or m > 0:
                    send_hop(group, m, side).wait_send()
                for p in range(m // 2 + 1):
                    n = 2 * p + side
                    target = fin_cross if group else fin_same
                    if n > m:
                        target[PLACE[m, p]] = jnp.zeros((BLOCK, BLOCK), jnp.bfloat16)
                        continue
                    value = slot[m * (m + 1) // 2 + side * (m // 2 + 1) + p] + hop[HOP_START[m] + p]
                    if n == m and group == 0:
                        rows = lax.broadcasted_iota(jnp.int32, (BLOCK, BLOCK), 0)
                        cols = lax.broadcasted_iota(jnp.int32, (BLOCK, BLOCK), 1)
                        value = jnp.where(rows >= cols, value, 0.0)
                    if n == m and group == 1:
                        value = jnp.where(row == 0, value, 0.0)
                    target[PLACE[m, p]] = value.astype(jnp.bfloat16)

    def put_low(first, count, source):
        return pltpu.make_async_copy(source.at[pl.ds(first, count)], out_low.at[pl.ds(first, count)], fin_sem.at[0])

    def put_cross():
        return pltpu.make_async_copy(fin_cross.at[pl.ds(0, RETURNED)], out_cross, fin_sem.at[1])

    for m in range(NUM):
        load(grad, grad_v, m, 0).wait()
        load(right, right_v, m, 1).wait()
        partial_sums(grad_v, 0, m)

    @pl.when(owner)
    def _():
        each_low(lower_v.at[x, 0], lambda copy: copy.wait())
        cross_near().wait_recv()

        @pl.when(row == 0)
        def _():
            cross_far(6).wait_recv()

        @pl.when(row == 1)
        def _():
            cross_far(3).wait_recv()

        send_low(0, x, to_chip).start()
        send_low(1, x, to_core).start()

    for m in range(NUM):
        finish(0, m)

    @pl.when(owner)
    def _():
        pl.semaphore_signal(core_free, inc=1, device_id=to_core, device_id_type=MESH)
        pl.semaphore_signal(hop_free, inc=1, device_id=to_chip, device_id_type=MESH)
        send_low(0, 1 - x, to_chip).wait_recv()
        send_low(2, 1 - x, to_core).start()
        pl.semaphore_wait(hop_free, 1)
        put_low(0, 12, fin_same).start()

        @pl.when(row == 0)
        def _():
            cross_far(3).wait_send()

        @pl.when(row == 1)
        def _():
            cross_far(6).wait_send()

    @pl.when(guest)
    def _():
        send_low(1, x, to_core).wait_recv()
        send_low(2, 1 - x, to_core).wait_recv()
        for m in range(NUM):
            send_core(0, m).wait_send()
        pl.semaphore_wait(core_free, 1)

    def turn(n):
        p, half = n // 2, n % 2
        for parity in range(2):
            for m in range(n, NUM):
                turned[parity, :, pl.ds((m - n) * BLOCK, BLOCK)] = lower_v[half, parity, PLACE[m, p]].T

    def put(n):
        return pltpu.make_async_copy(stage, out_right.at[pl.ds(n * BLOCK, BLOCK)], out_sem)

    def tiles(body):
        def one(t, carry):
            body(pl.ds(pl.multiple_of(t * TILE, TILE), TILE))
            return carry
        lax.fori_loop(0, COLS // TILE, one, 0)

    for m in range(NUM - 1, 0, -1):
        send_grad(m).wait_recv()
        partial_sums(other_v, 1, m)
        turn(m)
        if m < NUM - 1:
            put(m + 1).wait()
        depth = (NUM - m) * BLOCK

        def product(cols, m=m, depth=depth):
            value = jnp.dot(turned[0, :, :depth], grad_v[m * BLOCK:, cols], preferred_element_type=jnp.float32)
            value += jnp.dot(turned[1, :, :depth], other_v[m * BLOCK:, cols], preferred_element_type=jnp.float32)
            stage[:, cols] = value.astype(jnp.bfloat16)

        tiles(product)
        put(m).start()
        if m < NUM - 1:
            finish(1, m + 1)
        if m + 1 == RETURNED_FROM:
            @pl.when(owner)
            def _():
                send_back().start()
        if m == 1:
            @pl.when(jnp.logical_and(owner, row == 0))
            def _():
                send_back_down().start()

    turn(0)

    def all_but_last(cols):
        value = jnp.dot(turned[0], grad_v[:, cols], preferred_element_type=jnp.float32)
        total[:, cols] = value + jnp.dot(turned[1, :, BLOCK:], other_v[BLOCK:, cols], preferred_element_type=jnp.float32)

    tiles(all_but_last)
    finish(1, 1)

    @pl.when(owner)
    def _():
        put_cross().start()

    put(1).wait()

    def put_last(t):
        cols = pl.ds(t * LAST, LAST)
        return pltpu.make_async_copy(stage.at[:, cols], out_right.at[pl.ds(0, BLOCK), cols], last_sem.at[t])

    @pl.when(row == 0)
    def _():
        send_grad(0).wait_recv()
        for t in range(COLS // LAST):
            cols = pl.ds(t * LAST, LAST)
            value = jnp.dot(turned[1, :, :BLOCK], other_v[:BLOCK, cols], preferred_element_type=jnp.float32)
            stage[:, cols] = (total[:, cols] + value).astype(jnp.bfloat16)
            put_last(t).start()

    def corner_core():
        return remote(slot.at[0], hop.at[0], corner_send.at[0], corner_recv.at[0], to_core)

    def corner_chip():
        return remote(slot.at[0], hop.at[1], corner_send.at[1], corner_recv.at[1], to_chip)

    @pl.when(row == 1)
    def _():
        for t in range(COLS // LAST):
            cols = pl.ds(t * LAST, LAST)
            stage[:, cols] = total[:, cols].astype(jnp.bfloat16)
            put_last(t).start()
        send_right().wait_recv()
        slot[0] = dot_nt(grad_v[:BLOCK, :], other_v[:BLOCK, :])

        @pl.when(owner)
        def _():
            corner_core().start()
            corner_core().wait_send()

        @pl.when(jnp.logical_and(guest, x == 1))
        def _():
            corner_core().wait_recv()
            slot[0] = slot[0] + hop[0]
            corner_chip().start()
            corner_chip().wait_send()

        @pl.when(jnp.logical_and(guest, x == 0))
        def _():
            corner_core().wait_recv()
            corner_chip().wait_recv()
            fin_cross[9] = (slot[0] + hop[0] + hop[1]).astype(jnp.bfloat16)

    @pl.when(guest)
    def _():
        send_back().wait_recv()

        @pl.when(row == 1)
        def _():
            send_back_down().wait_recv()

        put_low(RETURNED, 12 - RETURNED, fin_cross).start()
        put_low(RETURNED, 12 - RETURNED, fin_cross).wait()
        cross_hand().wait_send()
        cross_near().wait_send()
        for m in range(1, NUM):
            send_core(1, m).wait_send()

    @pl.when(owner)
    def _():
        put_low(0, 12, fin_same).wait()
        put_cross().wait()
        send_low(0, x, to_chip).wait_send()
        send_low(1, x, to_core).wait_send()
        send_low(2, 1 - x, to_core).wait_send()
        send_back().wait_send()

        @pl.when(row == 0)
        def _():
            send_back_down().wait_send()

    for t in range(COLS // LAST):
        put_last(t).wait()
    for m in range(NUM - 1, 0, -1):
        send_grad(m).wait_send()

    @pl.when(row == 0)
    def _():
        send_right().wait_send()

    @pl.when(row == 1)
    def _():
        send_grad(0).wait_send()


def copy_kernel(source, target, buffer, read_sem, write_sem):
    rows = source.shape[0] // COPY_PARTS
    part = lambda ref, k: ref.at[pl.ds(k * rows, rows)]
    reads = [pltpu.make_async_copy(part(source, k), part(buffer, k), read_sem.at[k]) for k in range(COPY_PARTS)]
    writes = [pltpu.make_async_copy(part(buffer, k), part(target, k), write_sem.at[k]) for k in range(COPY_PARTS)]
    for read in reads:
        read.start()
    for read, write in zip(reads, writes):
        read.wait()
        write.start()
    for write in writes:
        write.wait()


def solution(mesh):
    block_spec = P(("batch", "row"), "col")
    device = lambda row, col: row * 4 + col
    owners = [(row, 2 * chip + row) for row in range(2) for chip in range(2)]
    return_pairs = [(device(row, col), device(1 - row, col)) for row, col in owners]

    def per_device(lower_tri, right_side, grad_out):
        bf16, f32 = jnp.bfloat16, jnp.float32
        dma = pltpu.SemaphoreType.DMA
        block = lambda count: jax.ShapeDtypeStruct((count, BLOCK, BLOCK), bf16)
        hbm = pl.BlockSpec(memory_space=pl.ANY)
        right_here, low, cross = pl.pallas_call(
            kernel,
            out_shape=(jax.ShapeDtypeStruct(grad_out.shape, bf16), block(12), block(RETURNED)),
            in_specs=[hbm] * 3,
            out_specs=[hbm] * 3,
            scratch_shapes=[
                pltpu.VMEM((NUM * BLOCK, COLS), bf16), pltpu.VMEM((NUM * BLOCK, COLS), bf16), pltpu.VMEM((NUM * BLOCK, COLS), bf16),
                pltpu.VMEM((2, 2, 12, BLOCK, BLOCK), bf16),
                pltpu.VMEM((21, BLOCK, BLOCK), f32), pltpu.VMEM((12, BLOCK, BLOCK), f32),
                pltpu.VMEM((12, BLOCK, BLOCK), bf16), pltpu.VMEM((12, BLOCK, BLOCK), bf16),
                pltpu.VMEM((BLOCK, COLS), f32), pltpu.VMEM((BLOCK, COLS), bf16), pltpu.VMEM((2, BLOCK, NUM * BLOCK), bf16),
                dma((NUM,)), dma((NUM,)), dma((2, NUM)), dma((12,)), dma((3,)), dma((3,)), dma((3,)), dma((3,)),
                dma((2, NUM)), dma((2, NUM)), dma((2, NUM)), dma((2, NUM)), dma((2,)), dma((2,)), dma((2,)), dma((2,)), dma, dma((COLS // LAST,)), dma((2,)),
                pltpu.SemaphoreType.REGULAR, pltpu.SemaphoreType.REGULAR,
            ],
            compiler_params=pltpu.CompilerParams(collective_id=1, has_side_effects=True, vmem_limit_bytes=VMEM_BYTES),
        )(lower_tri, right_side, grad_out)

        grad_right = pl.pallas_call(
            copy_kernel,
            out_shape=jax.ShapeDtypeStruct(grad_out.shape, bf16),
            in_specs=[hbm],
            out_specs=hbm,
            scratch_shapes=[pltpu.VMEM(grad_out.shape, bf16), dma((COPY_PARTS,)), dma((COPY_PARTS,))],
            cost_estimate=pl.CostEstimate(flops=10 ** 10, bytes_accessed=4 * grad_out.size, transcendentals=0),
        )(right_here)
        got = lax.ppermute(cross, ("row", "col"), return_pairs)
        row, col = lax.axis_index("row"), lax.axis_index("col")
        is_owner = (col % 2) == row
        zero = jnp.zeros((BLOCK, BLOCK), bf16)

        def piece(m, p):
            if p > m // 2:
                return zero
            place = PLACE[m, p]
            return jnp.where(is_owner, low[place], got[place]) if place < RETURNED else low[place]

        grad_lower = jnp.concatenate([jnp.concatenate([piece(m, p) for p in range(3)], axis=1) for m in range(NUM)], axis=0)
        return grad_right, grad_lower

    return jax.shard_map(per_device, mesh=mesh, in_specs=(block_spec, block_spec, block_spec), out_specs=(block_spec, block_spec), check_vma=False)
```

```python
import jax
import jax.numpy as jnp
from jax import lax
from jax.experimental import pallas as pl
from jax.experimental.pallas import tpu as pltpu
from jax.sharding import PartitionSpec as P

MESH = pl.DeviceIdType.MESH
BLOCK = 256
NUM = 6
COLS = 4096
TILE = 512
LAST = 1024
HALF = BLOCK // 2
VMEM_BYTES = 67043328
HOP_START = (0, 1, 2, 4, 6, 9)
PLACE = {(1, 0): 0, (2, 0): 1, (3, 0): 2, (3, 1): 3, (4, 0): 4, (4, 1): 5, (5, 0): 6, (5, 1): 7, (5, 2): 8, (0, 0): 9, (2, 1): 10, (4, 2): 11}
RETURNED = 6
RETURNED_FROM = 5
COPY_PARTS = 12


def dot_nt(lhs, rhs):
    return lax.dot_general(lhs, rhs, (((1,), (1,)), ((), ())), preferred_element_type=jnp.float32)


def kernel(lower, right, grad, out_right, out_low, out_cross,
           grad_v, right_v, other_v, lower_v, slot, hop, fin_same, fin_cross, total, stage, turned,
           grad_send, grad_recv, last_send, last_recv, right_send, right_recv, load_sem, low_load, low_cross_send, low_cross_recv, low_send, low_recv,
           core_send, core_recv, hop_send, hop_recv, back_send, back_recv, corner_send, corner_recv, out_sem, put_sem, fin_sem, core_free, hop_free):
    row = lax.axis_index("row")
    col = lax.axis_index("col")
    x = col // 2
    owner = (col % 2) == row
    guest = jnp.logical_not(owner)
    to_row = {"row": 1 - row}
    to_core = {"col": col + 1 - 2 * (col % 2)}
    to_chip = {"col": lax.rem(col + 2, 4)}
    to_diag = {"row": 1 - row, "col": col + 1 - 2 * (col % 2)}

    def remote(src, dst, send, recv, where):
        return pltpu.make_async_remote_copy(src_ref=src, dst_ref=dst, send_sem=send, recv_sem=recv, device_id=where, device_id_type=MESH)

    def send_grad(m):
        return remote(grad.at[pl.ds(m * BLOCK, BLOCK)], other_v.at[pl.ds(m * BLOCK, BLOCK)], grad_send.at[m], grad_recv.at[m], to_row)

    def send_last(t):
        cols = pl.ds(t * LAST, LAST)
        return remote(grad.at[pl.ds(0, BLOCK), cols], other_v.at[pl.ds(0, BLOCK), cols], last_send.at[t], last_recv.at[t], to_row)

    def send_right(h):
        rows = pl.ds(h * HALF, HALF)
        return remote(right.at[rows], other_v.at[rows], right_send.at[h], right_recv.at[h], to_row)

    def load_low(target, p, m):
        return pltpu.make_async_copy(lower.at[pl.ds(m * BLOCK, BLOCK), pl.ds(p * BLOCK, BLOCK)], target.at[PLACE[m, p]], low_load.at[PLACE[m, p]])

    def each_low(target, act):
        for p in range(3):
            for m in range(2 * p, NUM):
                act(load_low(target, p, m))

    def cross_near():
        return remote(fin_same.at[pl.ds(0, 6)], lower_v.at[x, 1, pl.ds(0, 6)], low_cross_send.at[0], low_cross_recv.at[0], to_row)

    def cross_hand():
        return remote(fin_same.at[pl.ds(6, 6)], fin_cross.at[pl.ds(0, 6)], low_cross_send.at[1], low_cross_recv.at[1], to_core)

    def cross_far(count):
        return remote(fin_cross.at[pl.ds(0, count)], lower_v.at[x, 1, pl.ds(6, count)], low_cross_send.at[2], low_cross_recv.at[2], to_diag)

    def send_back():
        part = pl.ds(RETURNED, 9 - RETURNED)
        return remote(fin_cross.at[part], out_low.at[part], back_send.at[0], back_recv.at[0], to_row)

    def send_back_down():
        return remote(fin_cross.at[pl.ds(10, 2)], out_low.at[pl.ds(10, 2)], back_send.at[1], back_recv.at[1], to_row)

    def send_low(index, half, where):
        return remote(lower_v.at[half], lower_v.at[half], low_send.at[index], low_recv.at[index], where)

    def load(src, dst, m, k):
        return pltpu.make_async_copy(src.at[pl.ds(m * BLOCK, BLOCK)], dst.at[pl.ds(m * BLOCK, BLOCK)], load_sem.at[k, m])

    def put_low(first, count, source):
        return pltpu.make_async_copy(source.at[pl.ds(first, count)], out_low.at[pl.ds(first, count)], fin_sem.at[0])

    def put_cross():
        return pltpu.make_async_copy(fin_cross.at[pl.ds(0, RETURNED)], out_cross, fin_sem.at[1])

    def send_core(group, m):
        part = slot.at[pl.ds(m * (m + 1) // 2, m + 1)]
        return remote(part, part, core_send.at[group, m], core_recv.at[group, m], to_core)

    def send_hop(group, m, side):
        base = m * (m + 1) // 2
        first, count = (base + m // 2 + 1, (m + 1) // 2) if side == 0 else (base, m // 2 + 1)
        return remote(slot.at[pl.ds(first, count)], hop.at[pl.ds(HOP_START[m], count)], hop_send.at[group, m], hop_recv.at[group, m], to_chip)

    @pl.when(guest)
    def _():
        fin_cross[9:] = jnp.zeros((3, BLOCK, BLOCK), jnp.bfloat16)

    barrier = pltpu.get_barrier_semaphore()
    for where in (to_row, to_core, to_chip, to_diag):
        pl.semaphore_signal(barrier, inc=1, device_id=where, device_id_type=MESH)
    pl.semaphore_wait(barrier, 4)

    send_grad(NUM - 1).start()

    @pl.when(guest)
    def _():
        each_low(fin_same, lambda copy: copy.start())

    @pl.when(owner)
    def _():
        each_low(lower_v.at[x, 0], lambda copy: copy.start())

    for m in range(NUM):
        load(grad, grad_v, m, 0).start()
        load(right, right_v, m, 1).start()

    @pl.when(guest)
    def _():
        each_low(fin_same, lambda copy: copy.wait())
        cross_hand().start()
        cross_near().start()

    @pl.when(owner)
    def _():
        cross_hand().wait_recv()

        @pl.when(row == 0)
        def _():
            cross_far(3).start()

        @pl.when(row == 1)
        def _():
            lower_v[x, 1, 9:] = jnp.zeros((3, BLOCK, BLOCK), jnp.bfloat16)
            cross_far(6).start()

    for m in range(NUM - 2, 1, -1):
        send_grad(m).start()

    @pl.when(row == 0)
    def _():
        send_right(0).start()

    send_grad(1).start()

    @pl.when(row == 0)
    def _():
        send_right(1).start()

    @pl.when(row == 1)
    def _():
        for t in range(COLS // LAST):
            send_last(t).start()

    @pl.when(jnp.logical_and(guest, row == 0))
    def _():
        put_low(9, 3, fin_cross).start()

    def partial_sums(source, group, m):
        @pl.when(owner)
        def _():
            send_core(group, m).wait_recv()

        def one(n, carry):
            index = m * (m + 1) // 2 + (n % 2) * (m // 2 + 1) + n // 2
            value = dot_nt(source[pl.ds(m * BLOCK, BLOCK), :], right_v[pl.ds(pl.multiple_of(n * BLOCK, BLOCK), BLOCK), :])
            slot[index] = jnp.where(owner, slot[index], 0.0) + value
            return carry

        lax.fori_loop(0, m + 1, one, 0)

        @pl.when(guest)
        def _():
            send_core(group, m).start()

        for side in range(2):
            if side == 1 or m > 0:
                @pl.when(jnp.logical_and(owner, x == side))
                def _(side=side):
                    send_hop(group, m, side).start()

    def finish(group, m):
        for side in range(2):
            @pl.when(jnp.logical_and(owner, x == side))
            def _(side=side):
                if side == 0 or m > 0:
                    send_hop(group, m, 1 - side).wait_recv()
                if side == 1 or m > 0:
                    send_hop(group, m, side).wait_send()
                for p in range(m // 2 + 1):
                    n = 2 * p + side
                    target = fin_cross if group else fin_same
                    if n > m:
                        target[PLACE[m, p]] = jnp.zeros((BLOCK, BLOCK), jnp.bfloat16)
                        continue
                    value = slot[m * (m + 1) // 2 + side * (m // 2 + 1) + p] + hop[HOP_START[m] + p]
                    if n == m and group == 0:
                        rows = lax.broadcasted_iota(jnp.int32, (BLOCK, BLOCK), 0)
                        cols = lax.broadcasted_iota(jnp.int32, (BLOCK, BLOCK), 1)
                        value = jnp.where(rows >= cols, value, 0.0)
                    if n == m and group == 1:
                        value = jnp.where(row == 0, value, 0.0)
                    target[PLACE[m, p]] = value.astype(jnp.bfloat16)

    for m in range(NUM):
        load(grad, grad_v, m, 0).wait()
        load(right, right_v, m, 1).wait()
        partial_sums(grad_v, 0, m)

    @pl.when(owner)
    def _():
        each_low(lower_v.at[x, 0], lambda copy: copy.wait())
        cross_near().wait_recv()

        @pl.when(row == 0)
        def _():
            cross_far(6).wait_recv()

        @pl.when(row == 1)
        def _():
            cross_far(3).wait_recv()

        send_low(0, x, to_chip).start()
        send_low(1, x, to_core).start()

    for m in range(NUM):
        finish(0, m)

    @pl.when(owner)
    def _():
        pl.semaphore_signal(core_free, inc=1, device_id=to_core, device_id_type=MESH)
        pl.semaphore_signal(hop_free, inc=1, device_id=to_chip, device_id_type=MESH)
        send_low(0, 1 - x, to_chip).wait_recv()
        send_low(2, 1 - x, to_core).start()
        pl.semaphore_wait(hop_free, 1)
        put_low(0, 12, fin_same).start()

        @pl.when(row == 0)
        def _():
            cross_far(3).wait_send()

        @pl.when(row == 1)
        def _():
            cross_far(6).wait_send()

    @pl.when(guest)
    def _():
        send_low(1, x, to_core).wait_recv()
        send_low(2, 1 - x, to_core).wait_recv()
        for m in range(NUM):
            send_core(0, m).wait_send()
        pl.semaphore_wait(core_free, 1)

    def turn(n):
        p, half = n // 2, n % 2
        for parity in range(2):
            for m in range(n, NUM):
                turned[parity, :, pl.ds((m - n) * BLOCK, BLOCK)] = lower_v[half, parity, PLACE[m, p]].T

    def put(n):
        return pltpu.make_async_copy(stage, out_right.at[pl.ds(n * BLOCK, BLOCK)], out_sem)

    def tiles(body):
        def one(t, carry):
            body(pl.ds(pl.multiple_of(t * TILE, TILE), TILE))
            return carry
        lax.fori_loop(0, COLS // TILE, one, 0)

    def corner(h):
        cols = pl.ds(h * HALF, HALF)
        to_guest = lambda: remote(slot.at[0, :, cols], hop.at[0, :, cols], corner_send.at[0, h], corner_recv.at[0, h], to_core)
        to_first = lambda: remote(slot.at[0, :, cols], hop.at[1, :, cols], corner_send.at[1, h], corner_recv.at[1, h], to_chip)
        send_right(h).wait_recv()
        slot[0, :, cols] = dot_nt(grad_v[:BLOCK, :], other_v[pl.ds(h * HALF, HALF), :])

        @pl.when(owner)
        def _():
            to_guest().start()
            to_guest().wait_send()

        @pl.when(jnp.logical_and(guest, x == 1))
        def _():
            to_guest().wait_recv()
            slot[0, :, cols] = slot[0, :, cols] + hop[0, :, cols]
            to_first().start()
            to_first().wait_send()

        @pl.when(jnp.logical_and(guest, x == 0))
        def _():
            to_guest().wait_recv()
            to_first().wait_recv()
            fin_cross[9, :, cols] = (slot[0, :, cols] + hop[0, :, cols] + hop[1, :, cols]).astype(jnp.bfloat16)

    for m in range(NUM - 1, 0, -1):
        if m == 1:
            @pl.when(row == 1)
            def _():
                corner(0)
        send_grad(m).wait_recv()
        partial_sums(other_v, 1, m)
        turn(m)
        if m < NUM - 1:
            put(m + 1).wait()
        depth = (NUM - m) * BLOCK

        def product(cols, m=m, depth=depth):
            value = jnp.dot(turned[0, :, :depth], grad_v[m * BLOCK:, cols], preferred_element_type=jnp.float32)
            value += jnp.dot(turned[1, :, :depth], other_v[m * BLOCK:, cols], preferred_element_type=jnp.float32)
            stage[:, cols] = value.astype(jnp.bfloat16)

        tiles(product)
        put(m).start()
        if m < NUM - 1:
            finish(1, m + 1)
        if m + 1 == RETURNED_FROM:
            @pl.when(owner)
            def _():
                send_back().start()
        if m == 1:
            @pl.when(jnp.logical_and(owner, row == 0))
            def _():
                send_back_down().start()

    turn(0)

    def all_but_last(cols):
        value = jnp.dot(turned[0], grad_v[:, cols], preferred_element_type=jnp.float32)
        total[:, cols] = value + jnp.dot(turned[1, :, BLOCK:], other_v[BLOCK:, cols], preferred_element_type=jnp.float32)

    tiles(all_but_last)
    finish(1, 1)

    @pl.when(owner)
    def _():
        put_cross().start()

    put(1).wait()

    def put_last(t):
        cols = pl.ds(t * LAST, LAST)
        return pltpu.make_async_copy(stage.at[:, cols], out_right.at[pl.ds(0, BLOCK), cols], put_sem.at[t])

    @pl.when(row == 0)
    def _():
        for t in range(COLS // LAST):
            cols = pl.ds(t * LAST, LAST)
            send_last(t).wait_recv()
            value = jnp.dot(turned[1, :, :BLOCK], other_v[:BLOCK, cols], preferred_element_type=jnp.float32)
            stage[:, cols] = (total[:, cols] + value).astype(jnp.bfloat16)
            put_last(t).start()

    @pl.when(row == 1)
    def _():
        for t in range(COLS // LAST):
            cols = pl.ds(t * LAST, LAST)
            stage[:, cols] = total[:, cols].astype(jnp.bfloat16)
            put_last(t).start()
        corner(1)

    @pl.when(guest)
    def _():
        @pl.when(row == 0)
        def _():
            put_low(9, 3, fin_cross).wait()

        @pl.when(row == 1)
        def _():
            put_low(9, 1, fin_cross).start()
            put_low(9, 1, fin_cross).wait()
            send_back_down().wait_recv()

        send_back().wait_recv()
        cross_hand().wait_send()
        cross_near().wait_send()
        for m in range(1, NUM):
            send_core(1, m).wait_send()

    @pl.when(owner)
    def _():
        put_low(0, 12, fin_same).wait()
        put_cross().wait()
        send_low(0, x, to_chip).wait_send()
        send_low(1, x, to_core).wait_send()
        send_low(2, 1 - x, to_core).wait_send()
        send_back().wait_send()

        @pl.when(row == 0)
        def _():
            send_back_down().wait_send()

    for t in range(COLS // LAST):
        put_last(t).wait()
    for m in range(NUM - 1, 0, -1):
        send_grad(m).wait_send()

    @pl.when(row == 0)
    def _():
        for h in range(2):
            send_right(h).wait_send()

    @pl.when(row == 1)
    def _():
        for t in range(COLS // LAST):
            send_last(t).wait_send()


def copy_kernel(source, target, buffer, read_sem, write_sem):
    rows = source.shape[0] // COPY_PARTS
    part = lambda ref, k: ref.at[pl.ds(k * rows, rows)]
    reads = [pltpu.make_async_copy(part(source, k), part(buffer, k), read_sem.at[k]) for k in range(COPY_PARTS)]
    writes = [pltpu.make_async_copy(part(buffer, k), part(target, k), write_sem.at[k]) for k in range(COPY_PARTS)]
    for read in reads:
        read.start()
    for read, write in zip(reads, writes):
        read.wait()
        write.start()
    for write in writes:
        write.wait()


def solution(mesh):
    block_spec = P(("batch", "row"), "col")
    device = lambda row, col: row * 4 + col
    owners = [(row, 2 * chip + row) for row in range(2) for chip in range(2)]
    return_pairs = [(device(row, col), device(1 - row, col)) for row, col in owners]

    def per_device(lower_tri, right_side, grad_out):
        bf16, f32 = jnp.bfloat16, jnp.float32
        dma = pltpu.SemaphoreType.DMA
        block = lambda count: jax.ShapeDtypeStruct((count, BLOCK, BLOCK), bf16)
        hbm = pl.BlockSpec(memory_space=pl.ANY)
        right_here, low, cross = pl.pallas_call(
            kernel,
            out_shape=(jax.ShapeDtypeStruct(grad_out.shape, bf16), block(12), block(RETURNED)),
            in_specs=[hbm] * 3,
            out_specs=[hbm] * 3,
            scratch_shapes=[
                pltpu.VMEM((NUM * BLOCK, COLS), bf16), pltpu.VMEM((NUM * BLOCK, COLS), bf16), pltpu.VMEM((NUM * BLOCK, COLS), bf16),
                pltpu.VMEM((2, 2, 12, BLOCK, BLOCK), bf16),
                pltpu.VMEM((21, BLOCK, BLOCK), f32), pltpu.VMEM((12, BLOCK, BLOCK), f32),
                pltpu.VMEM((12, BLOCK, BLOCK), bf16), pltpu.VMEM((12, BLOCK, BLOCK), bf16),
                pltpu.VMEM((BLOCK, COLS), f32), pltpu.VMEM((BLOCK, COLS), bf16), pltpu.VMEM((2, BLOCK, NUM * BLOCK), bf16),
                dma((NUM,)), dma((NUM,)), dma((COLS // LAST,)), dma((COLS // LAST,)), dma((2,)), dma((2,)), dma((2, NUM)), dma((12,)), dma((3,)), dma((3,)), dma((3,)), dma((3,)),
                dma((2, NUM)), dma((2, NUM)), dma((2, NUM)), dma((2, NUM)), dma((2,)), dma((2,)), dma((2, 2)), dma((2, 2)), dma, dma((COLS // LAST,)), dma((2,)),
                pltpu.SemaphoreType.REGULAR, pltpu.SemaphoreType.REGULAR,
            ],
            compiler_params=pltpu.CompilerParams(collective_id=1, has_side_effects=True, vmem_limit_bytes=VMEM_BYTES),
        )(lower_tri, right_side, grad_out)

        grad_right = pl.pallas_call(
            copy_kernel,
            out_shape=jax.ShapeDtypeStruct(grad_out.shape, bf16),
            in_specs=[hbm],
            out_specs=hbm,
            scratch_shapes=[pltpu.VMEM(grad_out.shape, bf16), dma((COPY_PARTS,)), dma((COPY_PARTS,))],
            cost_estimate=pl.CostEstimate(flops=10 ** 10, bytes_accessed=4 * grad_out.size, transcendentals=0),
        )(right_here)
        got = lax.ppermute(cross, ("row", "col"), return_pairs)
        row, col = lax.axis_index("row"), lax.axis_index("col")
        is_owner = (col % 2) == row
        zero = jnp.zeros((BLOCK, BLOCK), bf16)

        def piece(m, p):
            if p > m // 2:
                return zero
            place = PLACE[m, p]
            return jnp.where(is_owner, low[place], got[place]) if place < RETURNED else low[place]

        grad_lower = jnp.concatenate([jnp.concatenate([piece(m, p) for p in range(3)], axis=1) for m in range(NUM)], axis=0)
        return grad_right, grad_lower

    return jax.shard_map(per_device, mesh=mesh, in_specs=(block_spec, block_spec, block_spec), out_specs=(block_spec, block_spec), check_vma=False)
```

```python
import jax
import jax.numpy as jnp
from jax import lax
from jax.experimental import pallas as pl
from jax.experimental.pallas import tpu as pltpu
from jax.sharding import PartitionSpec as P

MESH = pl.DeviceIdType.MESH
BLOCK = 256
NUM = 6
COLS = 4096
TILE = 512
LAST = 1024
HALF = BLOCK // 2
VMEM_BYTES = 67043328
HOP_START = (0, 1, 2, 4, 6, 9)
PLACE = {(1, 0): 0, (2, 0): 1, (3, 0): 2, (3, 1): 3, (4, 0): 4, (4, 1): 5, (5, 0): 6, (5, 1): 7, (5, 2): 8, (0, 0): 9, (2, 1): 10, (4, 2): 11}
RETURNED = 6
RETURNED_FROM = 5
COPY_PARTS = 12


def dot_nt(lhs, rhs):
    return lax.dot_general(lhs, rhs, (((1,), (1,)), ((), ())), preferred_element_type=jnp.float32)


def kernel(lower, right, grad, out_right, out_low, out_cross,
           grad_v, right_v, other_v, lower_v, slot, hop, fin_same, fin_cross, total, stage, turned,
           grad_send, grad_recv, last_send, last_recv, right_send, right_recv, detour_send, detour_recv, load_sem, low_load, low_cross_send, low_cross_recv, low_send, low_recv,
           core_send, core_recv, hop_send, hop_recv, back_send, back_recv, corner_send, corner_recv, out_sem, put_sem, fin_sem, core_free, hop_free):
    row = lax.axis_index("row")
    col = lax.axis_index("col")
    x = col // 2
    owner = (col % 2) == row
    guest = jnp.logical_not(owner)
    to_row = {"row": 1 - row}
    to_core = {"col": col + 1 - 2 * (col % 2)}
    to_chip = {"col": lax.rem(col + 2, 4)}
    to_diag = {"row": 1 - row, "col": col + 1 - 2 * (col % 2)}

    def remote(src, dst, send, recv, where):
        return pltpu.make_async_remote_copy(src_ref=src, dst_ref=dst, send_sem=send, recv_sem=recv, device_id=where, device_id_type=MESH)

    def send_grad(m):
        return remote(grad.at[pl.ds(m * BLOCK, BLOCK)], other_v.at[pl.ds(m * BLOCK, BLOCK)], grad_send.at[m], grad_recv.at[m], to_row)

    def send_last(t):
        cols = pl.ds(t * LAST, LAST)
        return remote(grad.at[pl.ds(0, BLOCK), cols], other_v.at[pl.ds(0, BLOCK), cols], last_send.at[t], last_recv.at[t], to_row)

    def send_right(k):
        where = (pl.ds(0, HALF), slice(None)) if k == 0 else (pl.ds(HALF, HALF), pl.ds((k - 1) * LAST, LAST))
        return remote(right.at[where], other_v.at[where], right_send.at[k], right_recv.at[k], to_row)

    def load_low(target, p, m):
        return pltpu.make_async_copy(lower.at[pl.ds(m * BLOCK, BLOCK), pl.ds(p * BLOCK, BLOCK)], target.at[PLACE[m, p]], low_load.at[PLACE[m, p]])

    def each_low(target, act):
        for p in range(3):
            for m in range(2 * p, NUM):
                act(load_low(target, p, m))

    def cross_near(count):
        return remote(fin_same.at[pl.ds(0, count)], lower_v.at[x, 1, pl.ds(0, count)], low_cross_send.at[0], low_cross_recv.at[0], to_row)

    def cross_hand():
        return remote(fin_same.at[pl.ds(4, 8)], fin_cross.at[pl.ds(0, 8)], low_cross_send.at[1], low_cross_recv.at[1], to_core)

    def cross_far(first, count):
        return remote(fin_cross.at[pl.ds(first - 4, count)], lower_v.at[x, 1, pl.ds(first, count)], low_cross_send.at[2], low_cross_recv.at[2], to_diag)

    def detour(k):
        source, target, where = (
            (fin_same.at[pl.ds(10, 2)], fin_cross.at[pl.ds(0, 2)], to_chip),
            (fin_cross.at[pl.ds(0, 2)], turned.at[:, :, pl.ds(0, BLOCK)], to_row),
            (turned.at[:, :, pl.ds(0, BLOCK)], lower_v.at[0, 1, pl.ds(10, 2)], to_chip))[k]
        return remote(source, target, detour_send.at[k], detour_recv.at[k], where)

    def cross_cases(sender_row, act):
        for case, counts in ((sender_row == 0, (5, 5, 4)),
                             (jnp.logical_and(sender_row == 1, x == 0), (5, 5, 5)),
                             (jnp.logical_and(sender_row == 1, x == 1), (4, 4, 5))):
            @pl.when(case)
            def _(counts=counts):
                act(*counts)

    def send_back():
        part = pl.ds(RETURNED, 9 - RETURNED)
        return remote(fin_cross.at[part], out_low.at[part], back_send.at[0], back_recv.at[0], to_row)

    def send_back_down():
        return remote(fin_cross.at[pl.ds(10, 2)], out_low.at[pl.ds(10, 2)], back_send.at[1], back_recv.at[1], to_row)

    def send_low(index, half, where):
        return remote(lower_v.at[half], lower_v.at[half], low_send.at[index], low_recv.at[index], where)

    def load(src, dst, m, k):
        return pltpu.make_async_copy(src.at[pl.ds(m * BLOCK, BLOCK)], dst.at[pl.ds(m * BLOCK, BLOCK)], load_sem.at[k, m])

    def put_low(first, count, source):
        return pltpu.make_async_copy(source.at[pl.ds(first, count)], out_low.at[pl.ds(first, count)], fin_sem.at[0])

    def put_cross():
        return pltpu.make_async_copy(fin_cross.at[pl.ds(0, RETURNED)], out_cross, fin_sem.at[1])

    def send_core(group, m):
        part = slot.at[pl.ds(m * (m + 1) // 2, m + 1)]
        return remote(part, part, core_send.at[group, m], core_recv.at[group, m], to_core)

    def send_hop(group, m, side):
        base = m * (m + 1) // 2
        first, count = (base + m // 2 + 1, (m + 1) // 2) if side == 0 else (base, m // 2 + 1)
        return remote(slot.at[pl.ds(first, count)], hop.at[pl.ds(HOP_START[m], count)], hop_send.at[group, m], hop_recv.at[group, m], to_chip)

    @pl.when(guest)
    def _():
        fin_cross[9:] = jnp.zeros((3, BLOCK, BLOCK), jnp.bfloat16)

    barrier = pltpu.get_barrier_semaphore()
    for where in (to_row, to_core, to_chip, to_diag):
        pl.semaphore_signal(barrier, inc=1, device_id=where, device_id_type=MESH)
    pl.semaphore_wait(barrier, 4)

    send_grad(NUM - 1).start()

    @pl.when(guest)
    def _():
        each_low(fin_same, lambda copy: copy.start())

    @pl.when(owner)
    def _():
        each_low(lower_v.at[x, 0], lambda copy: copy.start())

    for m in range(NUM):
        load(grad, grad_v, m, 0).start()
        load(right, right_v, m, 1).start()

    @pl.when(guest)
    def _():
        each_low(fin_same, lambda copy: copy.wait())
        cross_hand().start()

        @pl.when(jnp.logical_and(row == 1, x == 0))
        def _():
            detour(0).start()

        cross_cases(row, lambda near, first, far: cross_near(near).start())

        @pl.when(jnp.logical_and(row == 1, x == 1))
        def _():
            detour(0).wait_recv()
            detour(1).start()

    @pl.when(owner)
    def _():
        @pl.when(jnp.logical_or(row == 1, x == 1))
        def _():
            lower_v[x, 1, 9:] = jnp.zeros((3, BLOCK, BLOCK), jnp.bfloat16)

        cross_hand().wait_recv()
        cross_cases(row, lambda near, first, far: cross_far(first, far).start())

    for m in range(NUM - 2, 1, -1):
        send_grad(m).start()

    @pl.when(row == 0)
    def _():
        send_right(0).start()

    send_grad(1).start()

    @pl.when(row == 0)
    def _():
        for k in range(1, 1 + COLS // LAST):
            send_right(k).start()

    @pl.when(row == 1)
    def _():
        for t in range(COLS // LAST):
            send_last(t).start()

    @pl.when(jnp.logical_and(guest, row == 0))
    def _():
        put_low(9, 3, fin_cross).start()

    def partial_sums(source, group, m):
        @pl.when(owner)
        def _():
            send_core(group, m).wait_recv()

        def one(n, carry):
            index = m * (m + 1) // 2 + (n % 2) * (m // 2 + 1) + n // 2
            value = dot_nt(source[pl.ds(m * BLOCK, BLOCK), :], right_v[pl.ds(pl.multiple_of(n * BLOCK, BLOCK), BLOCK), :])
            slot[index] = jnp.where(owner, slot[index], 0.0) + value
            return carry

        lax.fori_loop(0, m + 1, one, 0)

        @pl.when(guest)
        def _():
            send_core(group, m).start()

        for side in range(2):
            if side == 1 or m > 0:
                @pl.when(jnp.logical_and(owner, x == side))
                def _(side=side):
                    send_hop(group, m, side).start()

    def finish(group, m):
        for side in range(2):
            @pl.when(jnp.logical_and(owner, x == side))
            def _(side=side):
                if side == 0 or m > 0:
                    send_hop(group, m, 1 - side).wait_recv()
                if side == 1 or m > 0:
                    send_hop(group, m, side).wait_send()
                for p in range(m // 2 + 1):
                    n = 2 * p + side
                    target = fin_cross if group else fin_same
                    if n > m:
                        target[PLACE[m, p]] = jnp.zeros((BLOCK, BLOCK), jnp.bfloat16)
                        continue
                    value = slot[m * (m + 1) // 2 + side * (m // 2 + 1) + p] + hop[HOP_START[m] + p]
                    if n == m and group == 0:
                        rows = lax.broadcasted_iota(jnp.int32, (BLOCK, BLOCK), 0)
                        cols = lax.broadcasted_iota(jnp.int32, (BLOCK, BLOCK), 1)
                        value = jnp.where(rows >= cols, value, 0.0)
                    if n == m and group == 1:
                        value = jnp.where(row == 0, value, 0.0)
                    target[PLACE[m, p]] = value.astype(jnp.bfloat16)

    for m in range(NUM):
        load(grad, grad_v, m, 0).wait()
        load(right, right_v, m, 1).wait()
        partial_sums(grad_v, 0, m)

    @pl.when(owner)
    def _():
        each_low(lower_v.at[x, 0], lambda copy: copy.wait())
        def arrived(near, first, far):
            cross_near(near).wait_recv()
            cross_far(first, far).wait_recv()

        cross_cases(1 - row, arrived)

        @pl.when(jnp.logical_and(row == 0, x == 1))
        def _():
            detour(1).wait_recv()
            detour(2).start()

        @pl.when(jnp.logical_and(row == 0, x == 0))
        def _():
            detour(2).wait_recv()

        send_low(0, x, to_chip).start()
        send_low(1, x, to_core).start()

    for m in range(NUM):
        finish(0, m)

    @pl.when(owner)
    def _():
        pl.semaphore_signal(core_free, inc=1, device_id=to_core, device_id_type=MESH)
        pl.semaphore_signal(hop_free, inc=1, device_id=to_chip, device_id_type=MESH)
        send_low(0, 1 - x, to_chip).wait_recv()
        send_low(2, 1 - x, to_core).start()
        pl.semaphore_wait(hop_free, 1)
        put_low(0, 12, fin_same).start()

        cross_cases(row, lambda near, first, far: cross_far(first, far).wait_send())

        @pl.when(jnp.logical_and(row == 0, x == 1))
        def _():
            detour(2).wait_send()

    @pl.when(guest)
    def _():
        send_low(1, x, to_core).wait_recv()
        send_low(2, 1 - x, to_core).wait_recv()
        for m in range(NUM):
            send_core(0, m).wait_send()
        pl.semaphore_wait(core_free, 1)

    def turn(n):
        p, half = n // 2, n % 2
        for parity in range(2):
            for m in range(n, NUM):
                turned[parity, :, pl.ds((m - n) * BLOCK, BLOCK)] = lower_v[half, parity, PLACE[m, p]].T

    def put(n):
        return pltpu.make_async_copy(stage, out_right.at[pl.ds(n * BLOCK, BLOCK)], out_sem)

    def tiles(body):
        def one(t, carry):
            body(pl.ds(pl.multiple_of(t * TILE, TILE), TILE))
            return carry
        lax.fori_loop(0, COLS // TILE, one, 0)

    def corner(h):
        cols = pl.ds(h * HALF, HALF)
        to_guest = lambda: remote(slot.at[0, :, cols], hop.at[0, :, cols], corner_send.at[0, h], corner_recv.at[0, h], to_core)
        to_first = lambda: remote(slot.at[0, :, cols], hop.at[1, :, cols], corner_send.at[1, h], corner_recv.at[1, h], to_chip)
        if h == 0:
            send_right(0).wait_recv()
            slot[0, :, cols] = dot_nt(grad_v[:BLOCK, :], other_v[:HALF, :])
        else:
            for t in range(COLS // LAST):
                send_right(1 + t).wait_recv()
                some = pl.ds(t * LAST, LAST)
                value = dot_nt(grad_v[:BLOCK, some], other_v[HALF:BLOCK, some])
                slot[0, :, cols] = value if t == 0 else slot[0, :, cols] + value

        @pl.when(owner)
        def _():
            to_guest().start()
            to_guest().wait_send()

        @pl.when(jnp.logical_and(guest, x == 1))
        def _():
            to_guest().wait_recv()
            slot[0, :, cols] = slot[0, :, cols] + hop[0, :, cols]
            to_first().start()
            to_first().wait_send()

        @pl.when(jnp.logical_and(guest, x == 0))
        def _():
            to_guest().wait_recv()
            to_first().wait_recv()
            fin_cross[9, :, cols] = (slot[0, :, cols] + hop[0, :, cols] + hop[1, :, cols]).astype(jnp.bfloat16)

    for m in range(NUM - 1, 0, -1):
        if m == 1:
            @pl.when(row == 1)
            def _():
                corner(0)
        send_grad(m).wait_recv()
        partial_sums(other_v, 1, m)
        turn(m)
        if m < NUM - 1:
            put(m + 1).wait()
        depth = (NUM - m) * BLOCK

        def product(cols, m=m, depth=depth):
            value = jnp.dot(turned[0, :, :depth], grad_v[m * BLOCK:, cols], preferred_element_type=jnp.float32)
            value += jnp.dot(turned[1, :, :depth], other_v[m * BLOCK:, cols], preferred_element_type=jnp.float32)
            stage[:, cols] = value.astype(jnp.bfloat16)

        tiles(product)
        put(m).start()
        if m < NUM - 1:
            finish(1, m + 1)
        if m + 1 == RETURNED_FROM:
            @pl.when(owner)
            def _():
                send_back().start()
        if m == 1:
            @pl.when(jnp.logical_and(owner, row == 0))
            def _():
                send_back_down().start()

    turn(0)

    def all_but_last(cols):
        value = jnp.dot(turned[0], grad_v[:, cols], preferred_element_type=jnp.float32)
        total[:, cols] = value + jnp.dot(turned[1, :, BLOCK:], other_v[BLOCK:, cols], preferred_element_type=jnp.float32)

    tiles(all_but_last)
    finish(1, 1)

    @pl.when(owner)
    def _():
        put_cross().start()

    put(1).wait()

    def put_last(t):
        cols = pl.ds(t * LAST, LAST)
        return pltpu.make_async_copy(stage.at[:, cols], out_right.at[pl.ds(0, BLOCK), cols], put_sem.at[t])

    @pl.when(row == 0)
    def _():
        for t in range(COLS // LAST):
            cols = pl.ds(t * LAST, LAST)
            send_last(t).wait_recv()
            value = jnp.dot(turned[1, :, :BLOCK], other_v[:BLOCK, cols], preferred_element_type=jnp.float32)
            stage[:, cols] = (total[:, cols] + value).astype(jnp.bfloat16)
            put_last(t).start()

    @pl.when(row == 1)
    def _():
        for t in range(COLS // LAST):
            cols = pl.ds(t * LAST, LAST)
            stage[:, cols] = total[:, cols].astype(jnp.bfloat16)
            put_last(t).start()
        corner(1)

    @pl.when(guest)
    def _():
        @pl.when(row == 0)
        def _():
            put_low(9, 3, fin_cross).wait()

        @pl.when(row == 1)
        def _():
            put_low(9, 1, fin_cross).start()
            put_low(9, 1, fin_cross).wait()
            send_back_down().wait_recv()

        send_back().wait_recv()
        cross_hand().wait_send()
        cross_cases(row, lambda near, first, far: cross_near(near).wait_send())

        @pl.when(jnp.logical_and(row == 1, x == 0))
        def _():
            detour(0).wait_send()

        @pl.when(jnp.logical_and(row == 1, x == 1))
        def _():
            detour(1).wait_send()

        for m in range(1, NUM):
            send_core(1, m).wait_send()

    @pl.when(owner)
    def _():
        put_low(0, 12, fin_same).wait()
        put_cross().wait()
        send_low(0, x, to_chip).wait_send()
        send_low(1, x, to_core).wait_send()
        send_low(2, 1 - x, to_core).wait_send()
        send_back().wait_send()

        @pl.when(row == 0)
        def _():
            send_back_down().wait_send()

    for t in range(COLS // LAST):
        put_last(t).wait()
    for m in range(NUM - 1, 0, -1):
        send_grad(m).wait_send()

    @pl.when(row == 0)
    def _():
        for k in range(1 + COLS // LAST):
            send_right(k).wait_send()

    @pl.when(row == 1)
    def _():
        for t in range(COLS // LAST):
            send_last(t).wait_send()


def copy_kernel(source, target, buffer, read_sem, write_sem):
    rows = source.shape[0] // COPY_PARTS
    part = lambda ref, k: ref.at[pl.ds(k * rows, rows)]
    reads = [pltpu.make_async_copy(part(source, k), part(buffer, k), read_sem.at[k]) for k in range(COPY_PARTS)]
    writes = [pltpu.make_async_copy(part(buffer, k), part(target, k), write_sem.at[k]) for k in range(COPY_PARTS)]
    for read in reads:
        read.start()
    for read, write in zip(reads, writes):
        read.wait()
        write.start()
    for write in writes:
        write.wait()


def solution(mesh):
    block_spec = P(("batch", "row"), "col")
    device = lambda row, col: row * 4 + col
    owners = [(row, 2 * chip + row) for row in range(2) for chip in range(2)]
    return_pairs = [(device(row, col), device(1 - row, col)) for row, col in owners]

    def per_device(lower_tri, right_side, grad_out):
        bf16, f32 = jnp.bfloat16, jnp.float32
        dma = pltpu.SemaphoreType.DMA
        block = lambda count: jax.ShapeDtypeStruct((count, BLOCK, BLOCK), bf16)
        hbm = pl.BlockSpec(memory_space=pl.ANY)
        right_here, low, cross = pl.pallas_call(
            kernel,
            out_shape=(jax.ShapeDtypeStruct(grad_out.shape, bf16), block(12), block(RETURNED)),
            in_specs=[hbm] * 3,
            out_specs=[hbm] * 3,
            scratch_shapes=[
                pltpu.VMEM((NUM * BLOCK, COLS), bf16), pltpu.VMEM((NUM * BLOCK, COLS), bf16), pltpu.VMEM((NUM * BLOCK, COLS), bf16),
                pltpu.VMEM((2, 2, 12, BLOCK, BLOCK), bf16),
                pltpu.VMEM((21, BLOCK, BLOCK), f32), pltpu.VMEM((12, BLOCK, BLOCK), f32),
                pltpu.VMEM((12, BLOCK, BLOCK), bf16), pltpu.VMEM((12, BLOCK, BLOCK), bf16),
                pltpu.VMEM((BLOCK, COLS), f32), pltpu.VMEM((BLOCK, COLS), bf16), pltpu.VMEM((2, BLOCK, NUM * BLOCK), bf16),
                dma((NUM,)), dma((NUM,)), dma((COLS // LAST,)), dma((COLS // LAST,)), dma((1 + COLS // LAST,)), dma((1 + COLS // LAST,)), dma((3,)), dma((3,)), dma((2, NUM)), dma((12,)), dma((3,)), dma((3,)), dma((3,)), dma((3,)),
                dma((2, NUM)), dma((2, NUM)), dma((2, NUM)), dma((2, NUM)), dma((2,)), dma((2,)), dma((2, 2)), dma((2, 2)), dma, dma((COLS // LAST,)), dma((2,)),
                pltpu.SemaphoreType.REGULAR, pltpu.SemaphoreType.REGULAR,
            ],
            compiler_params=pltpu.CompilerParams(collective_id=1, has_side_effects=True, vmem_limit_bytes=VMEM_BYTES),
        )(lower_tri, right_side, grad_out)

        grad_right = pl.pallas_call(
            copy_kernel,
            out_shape=jax.ShapeDtypeStruct(grad_out.shape, bf16),
            in_specs=[hbm],
            out_specs=hbm,
            scratch_shapes=[pltpu.VMEM(grad_out.shape, bf16), dma((COPY_PARTS,)), dma((COPY_PARTS,))],
            cost_estimate=pl.CostEstimate(flops=10 ** 10, bytes_accessed=4 * grad_out.size, transcendentals=0),
        )(right_here)
        got = lax.ppermute(cross, ("row", "col"), return_pairs)
        row, col = lax.axis_index("row"), lax.axis_index("col")
        is_owner = (col % 2) == row
        zero = jnp.zeros((BLOCK, BLOCK), bf16)

        def piece(m, p):
            if p > m // 2:
                return zero
            place = PLACE[m, p]
            return jnp.where(is_owner, low[place], got[place]) if place < RETURNED else low[place]

        grad_lower = jnp.concatenate([jnp.concatenate([piece(m, p) for p in range(3)], axis=1) for m in range(NUM)], axis=0)
        return grad_right, grad_lower

    return jax.shard_map(per_device, mesh=mesh, in_specs=(block_spec, block_spec, block_spec), out_specs=(block_spec, block_spec), check_vma=False)
```

```python
import jax
import jax.numpy as jnp
from jax import lax
from jax.experimental import pallas as pl
from jax.experimental.pallas import tpu as pltpu
from jax.sharding import PartitionSpec as P

MESH = pl.DeviceIdType.MESH
BLOCK = 256
NUM = 6
COLS = 4096
TILE = 512
LAST = 1024
NEAR = (0, 1)
FAR = (2, 3)
VMEM_BYTES = 67043328
HOP_START = (0, 1, 2, 4, 6, 9)
PLACE = {(1, 0): 0, (2, 0): 1, (3, 0): 2, (3, 1): 3, (4, 0): 4, (4, 1): 5, (5, 0): 6, (5, 1): 7, (5, 2): 8, (0, 0): 9, (2, 1): 10, (4, 2): 11}
RETURNED = 6
RETURNED_FROM = 5
COPY_PARTS = 12


def dot_nt(lhs, rhs):
    return lax.dot_general(lhs, rhs, (((1,), (1,)), ((), ())), preferred_element_type=jnp.float32)


def kernel(lower, right, grad, out_right, out_low, out_cross,
           grad_v, right_v, other_v, lower_v, slot, hop, corner, fin_same, fin_cross, total, stage, turned,
           grad_send, grad_recv, last_send, last_recv, detour_send, detour_recv, load_sem, low_load, low_cross_send, low_cross_recv, low_send, low_recv,
           core_send, core_recv, hop_send, hop_recv, back_send, back_recv, corner_send, corner_recv, out_sem, put_sem, fin_sem, core_free, hop_free):
    row = lax.axis_index("row")
    col = lax.axis_index("col")
    x = col // 2
    owner = (col % 2) == row
    guest = jnp.logical_not(owner)
    to_row = {"row": 1 - row}
    to_core = {"col": col + 1 - 2 * (col % 2)}
    to_chip = {"col": lax.rem(col + 2, 4)}
    to_diag = {"row": 1 - row, "col": col + 1 - 2 * (col % 2)}

    def remote(src, dst, send, recv, where):
        return pltpu.make_async_remote_copy(src_ref=src, dst_ref=dst, send_sem=send, recv_sem=recv, device_id=where, device_id_type=MESH)

    def send_grad(m):
        return remote(grad.at[pl.ds(m * BLOCK, BLOCK)], other_v.at[pl.ds(m * BLOCK, BLOCK)], grad_send.at[m], grad_recv.at[m], to_row)

    def send_last(t):
        cols = pl.ds(t * LAST, LAST)
        return remote(grad.at[pl.ds(0, BLOCK), cols], other_v.at[pl.ds(0, BLOCK), cols], last_send.at[t], last_recv.at[t], to_row)

    def send_right(t):
        cols = pl.ds(t * LAST, LAST)
        return remote(right.at[pl.ds(0, BLOCK), cols], other_v.at[pl.ds(0, BLOCK), cols], last_send.at[t], last_recv.at[t], to_row)

    def load_low(target, p, m):
        return pltpu.make_async_copy(lower.at[pl.ds(m * BLOCK, BLOCK), pl.ds(p * BLOCK, BLOCK)], target.at[PLACE[m, p]], low_load.at[PLACE[m, p]])

    def each_low(target, act):
        for p in range(3):
            for m in range(2 * p, NUM):
                act(load_low(target, p, m))

    def cross_near(count):
        return remote(fin_same.at[pl.ds(0, count)], lower_v.at[x, 1, pl.ds(0, count)], low_cross_send.at[0], low_cross_recv.at[0], to_row)

    def cross_hand():
        return remote(fin_same.at[pl.ds(4, 8)], fin_cross.at[pl.ds(0, 8)], low_cross_send.at[1], low_cross_recv.at[1], to_core)

    def cross_far(first, count):
        return remote(fin_cross.at[pl.ds(first - 4, count)], lower_v.at[x, 1, pl.ds(first, count)], low_cross_send.at[2], low_cross_recv.at[2], to_diag)

    def detour(k):
        source, target, where = (
            (fin_same.at[pl.ds(10, 2)], fin_cross.at[pl.ds(0, 2)], to_chip),
            (fin_cross.at[pl.ds(0, 2)], turned.at[:, :, pl.ds(0, BLOCK)], to_row),
            (turned.at[:, :, pl.ds(0, BLOCK)], lower_v.at[0, 1, pl.ds(10, 2)], to_chip))[k]
        return remote(source, target, detour_send.at[k], detour_recv.at[k], where)

    def cross_cases(sender_row, act):
        for case, counts in ((sender_row == 0, (5, 5, 4)),
                             (jnp.logical_and(sender_row == 1, x == 0), (4, 4, 6)),
                             (jnp.logical_and(sender_row == 1, x == 1), (4, 4, 5))):
            @pl.when(case)
            def _(counts=counts):
                act(*counts)

    def send_back(k):
        part = (pl.ds(RETURNED, 9 - RETURNED), pl.ds(0, 9), pl.ds(10, 2))[k]
        return remote(fin_cross.at[part], out_low.at[part], back_send.at[k], back_recv.at[k], to_row)

    def send_low(index, half, where):
        return remote(lower_v.at[half], lower_v.at[half], low_send.at[index], low_recv.at[index], where)

    def load(src, dst, m, k):
        return pltpu.make_async_copy(src.at[pl.ds(m * BLOCK, BLOCK)], dst.at[pl.ds(m * BLOCK, BLOCK)], load_sem.at[k, m])

    def put_low(first, count, source):
        return pltpu.make_async_copy(source.at[pl.ds(first, count)], out_low.at[pl.ds(first, count)], fin_sem.at[0])

    def put_cross():
        return pltpu.make_async_copy(fin_cross.at[pl.ds(0, RETURNED)], out_cross, fin_sem.at[1])

    def send_core(group, m):
        part = slot.at[pl.ds(m * (m + 1) // 2, m + 1)]
        return remote(part, part, core_send.at[group, m], core_recv.at[group, m], to_core)

    def send_hop(group, m, side):
        base = m * (m + 1) // 2
        first, count = (base + m // 2 + 1, (m + 1) // 2) if side == 0 else (base, m // 2 + 1)
        return remote(slot.at[pl.ds(first, count)], hop.at[pl.ds(HOP_START[m], count)], hop_send.at[group, m], hop_recv.at[group, m], to_chip)

    @pl.when(guest)
    def _():
        fin_cross[9:] = jnp.zeros((3, BLOCK, BLOCK), jnp.bfloat16)

    barrier = pltpu.get_barrier_semaphore()
    for where in (to_row, to_core, to_chip, to_diag):
        pl.semaphore_signal(barrier, inc=1, device_id=where, device_id_type=MESH)
    pl.semaphore_wait(barrier, 4)

    send_grad(NUM - 1).start()

    @pl.when(guest)
    def _():
        each_low(fin_same, lambda copy: copy.start())

    @pl.when(owner)
    def _():
        each_low(lower_v.at[x, 0], lambda copy: copy.start())

    for m in range(NUM):
        load(grad, grad_v, m, 0).start()
        load(right, right_v, m, 1).start()

    @pl.when(guest)
    def _():
        each_low(fin_same, lambda copy: copy.wait())
        cross_hand().start()

        @pl.when(jnp.logical_and(row == 1, x == 0))
        def _():
            detour(0).start()

        cross_cases(row, lambda near, first, far: cross_near(near).start())

        @pl.when(jnp.logical_and(row == 1, x == 1))
        def _():
            detour(0).wait_recv()
            detour(1).start()

    @pl.when(owner)
    def _():
        @pl.when(jnp.logical_or(row == 1, x == 1))
        def _():
            lower_v[x, 1, 9:] = jnp.zeros((3, BLOCK, BLOCK), jnp.bfloat16)

        cross_hand().wait_recv()
        cross_cases(row, lambda near, first, far: cross_far(first, far).start())

    for m in range(NUM - 2, 1, -1):
        send_grad(m).start()

    send_grad(1).start()

    @pl.when(row == 0)
    def _():
        for t in FAR:
            send_right(t).start()

    @pl.when(row == 1)
    def _():
        for t in range(COLS // LAST):
            send_last(t).start()

    @pl.when(jnp.logical_and(guest, row == 0))
    def _():
        put_low(9, 3, fin_cross).start()

    def partial_sums(source, group, m):
        @pl.when(owner)
        def _():
            send_core(group, m).wait_recv()

        def one(n, carry):
            index = m * (m + 1) // 2 + (n % 2) * (m // 2 + 1) + n // 2
            value = dot_nt(source[pl.ds(m * BLOCK, BLOCK), :], right_v[pl.ds(pl.multiple_of(n * BLOCK, BLOCK), BLOCK), :])
            slot[index] = jnp.where(owner, slot[index], 0.0) + value
            return carry

        lax.fori_loop(0, m + 1, one, 0)

        @pl.when(guest)
        def _():
            send_core(group, m).start()

        for side in range(2):
            if side == 1 or m > 0:
                @pl.when(jnp.logical_and(owner, x == side))
                def _(side=side):
                    send_hop(group, m, side).start()

    def finish(group, m):
        for side in range(2):
            @pl.when(jnp.logical_and(owner, x == side))
            def _(side=side):
                if side == 0 or m > 0:
                    send_hop(group, m, 1 - side).wait_recv()
                if side == 1 or m > 0:
                    send_hop(group, m, side).wait_send()
                for p in range(m // 2 + 1):
                    n = 2 * p + side
                    target = fin_cross if group else fin_same
                    if n > m:
                        target[PLACE[m, p]] = jnp.zeros((BLOCK, BLOCK), jnp.bfloat16)
                        continue
                    value = slot[m * (m + 1) // 2 + side * (m // 2 + 1) + p] + hop[HOP_START[m] + p]
                    if n == m and group == 0:
                        rows = lax.broadcasted_iota(jnp.int32, (BLOCK, BLOCK), 0)
                        cols = lax.broadcasted_iota(jnp.int32, (BLOCK, BLOCK), 1)
                        value = jnp.where(rows >= cols, value, 0.0)
                    if n == m and group == 1:
                        value = jnp.where(row == 0, value, 0.0)
                    target[PLACE[m, p]] = value.astype(jnp.bfloat16)

    for m in range(NUM):
        load(grad, grad_v, m, 0).wait()
        load(right, right_v, m, 1).wait()
        partial_sums(grad_v, 0, m)

    @pl.when(owner)
    def _():
        each_low(lower_v.at[x, 0], lambda copy: copy.wait())
        def arrived(near, first, far):
            cross_near(near).wait_recv()
            cross_far(first, far).wait_recv()

        cross_cases(1 - row, arrived)

        @pl.when(jnp.logical_and(row == 0, x == 1))
        def _():
            detour(1).wait_recv()
            detour(2).start()

        @pl.when(jnp.logical_and(row == 0, x == 0))
        def _():
            detour(2).wait_recv()

        send_low(0, x, to_chip).start()
        send_low(1, x, to_core).start()

    for m in range(NUM):
        finish(0, m)

    @pl.when(owner)
    def _():
        pl.semaphore_signal(core_free, inc=1, device_id=to_core, device_id_type=MESH)
        pl.semaphore_signal(hop_free, inc=1, device_id=to_chip, device_id_type=MESH)
        send_low(0, 1 - x, to_chip).wait_recv()
        send_low(2, 1 - x, to_core).start()
        pl.semaphore_wait(hop_free, 1)
        put_low(0, 12, fin_same).start()

        cross_cases(row, lambda near, first, far: cross_far(first, far).wait_send())

        @pl.when(jnp.logical_and(row == 0, x == 1))
        def _():
            detour(2).wait_send()

    @pl.when(guest)
    def _():
        send_low(1, x, to_core).wait_recv()
        send_low(2, 1 - x, to_core).wait_recv()
        for m in range(NUM):
            send_core(0, m).wait_send()
        pl.semaphore_wait(core_free, 1)

    def turn(n):
        p, half = n // 2, n % 2
        for parity in range(2):
            for m in range(n, NUM):
                turned[parity, :, pl.ds((m - n) * BLOCK, BLOCK)] = lower_v[half, parity, PLACE[m, p]].T

    def put(n):
        return pltpu.make_async_copy(stage, out_right.at[pl.ds(n * BLOCK, BLOCK)], out_sem)

    def tiles(body):
        def one(t, carry):
            body(pl.ds(pl.multiple_of(t * TILE, TILE), TILE))
            return carry
        lax.fori_loop(0, COLS // TILE, one, 0)

    first_core = (col % 2) == 0

    def corner_core():
        return remote(slot.at[0], corner.at[0], corner_send.at[0], corner_recv.at[0], to_core)

    def corner_chip():
        return remote(slot.at[0], corner.at[1], corner_send.at[1], corner_recv.at[1], to_chip)

    def corner_row():
        return remote(slot.at[0], corner.at[2], corner_send.at[2], corner_recv.at[2], to_row)

    def corner_start(grads, rights, pieces):
        for t in pieces:
            cols = pl.ds(t * LAST, LAST)
            value = dot_nt(grads[:BLOCK, cols], rights[:BLOCK, cols])
            slot[0] = value if t == pieces[0] else slot[0] + value

        @pl.when(jnp.logical_not(first_core))
        def _():
            corner_core().start()

        @pl.when(first_core)
        def _():
            corner_core().wait_recv()
            slot[0] = slot[0] + corner[0]

            @pl.when(x == 1)
            def _():
                corner_chip().start()

    def corner_end():
        @pl.when(jnp.logical_not(first_core))
        def _():
            corner_core().wait_send()

        @pl.when(jnp.logical_and(first_core, x == 1))
        def _():
            corner_chip().wait_send()

    for m in range(NUM - 1, 0, -1):
        send_grad(m).wait_recv()
        partial_sums(other_v, 1, m)
        turn(m)
        if m < NUM - 1:
            put(m + 1).wait()
        depth = (NUM - m) * BLOCK

        def product(cols, m=m, depth=depth):
            value = jnp.dot(turned[0, :, :depth], grad_v[m * BLOCK:, cols], preferred_element_type=jnp.float32)
            value += jnp.dot(turned[1, :, :depth], other_v[m * BLOCK:, cols], preferred_element_type=jnp.float32)
            stage[:, cols] = value.astype(jnp.bfloat16)

        tiles(product)
        put(m).start()
        if m < NUM - 1:
            finish(1, m + 1)
        if m + 1 == RETURNED_FROM:
            @pl.when(jnp.logical_and(owner, row == 1))
            def _():
                send_back(0).start()

    turn(0)

    def all_but_last(cols):
        value = jnp.dot(turned[0], grad_v[:, cols], preferred_element_type=jnp.float32)
        total[:, cols] = value + jnp.dot(turned[1, :, BLOCK:], other_v[BLOCK:, cols], preferred_element_type=jnp.float32)

    tiles(all_but_last)
    finish(1, 1)

    @pl.when(jnp.logical_and(owner, row == 0))
    def _():
        send_back(1).start()
        send_back(2).start()

    @pl.when(jnp.logical_and(owner, row == 1))
    def _():
        put_cross().start()

    put(1).wait()

    def put_last(t):
        cols = pl.ds(t * LAST, LAST)
        return pltpu.make_async_copy(stage.at[:, cols], out_right.at[pl.ds(0, BLOCK), cols], put_sem.at[t])

    @pl.when(row == 0)
    def _():
        for t in range(COLS // LAST):
            cols = pl.ds(t * LAST, LAST)
            send_last(t).wait_recv()
            value = jnp.dot(turned[1, :, :BLOCK], other_v[:BLOCK, cols], preferred_element_type=jnp.float32)
            stage[:, cols] = (total[:, cols] + value).astype(jnp.bfloat16)
            put_last(t).start()
            if t == NEAR[-1]:
                corner_start(other_v, right_v, NEAR)

            if t == NEAR[-1] + 1:
                @pl.when(jnp.logical_and(first_core, x == 0))
                def _():
                    corner_chip().wait_recv()
                    slot[0] = slot[0] + corner[1]
                    corner_row().start()

        corner_end()

        @pl.when(jnp.logical_and(first_core, x == 0))
        def _():
            corner_row().wait_send()

    @pl.when(row == 1)
    def _():
        for t in range(COLS // LAST):
            cols = pl.ds(t * LAST, LAST)
            stage[:, cols] = total[:, cols].astype(jnp.bfloat16)
            put_last(t).start()
        for t in FAR:
            send_right(t).wait_recv()
        corner_start(grad_v, other_v, FAR)
        corner_end()

        @pl.when(jnp.logical_and(first_core, x == 0))
        def _():
            corner_chip().wait_recv()
            corner_row().wait_recv()
            fin_cross[9] = (slot[0] + corner[1] + corner[2]).astype(jnp.bfloat16)


    @pl.when(guest)
    def _():
        @pl.when(row == 0)
        def _():
            put_low(9, 3, fin_cross).wait()
            send_back(0).wait_recv()

        @pl.when(row == 1)
        def _():
            put_low(9, 1, fin_cross).start()
            put_low(9, 1, fin_cross).wait()
            send_back(1).wait_recv()
            send_back(2).wait_recv()

        cross_hand().wait_send()
        cross_cases(row, lambda near, first, far: cross_near(near).wait_send())

        @pl.when(jnp.logical_and(row == 1, x == 0))
        def _():
            detour(0).wait_send()

        @pl.when(jnp.logical_and(row == 1, x == 1))
        def _():
            detour(1).wait_send()

        for m in range(1, NUM):
            send_core(1, m).wait_send()

    @pl.when(owner)
    def _():
        put_low(0, 12, fin_same).wait()
        send_low(0, x, to_chip).wait_send()
        send_low(1, x, to_core).wait_send()
        send_low(2, 1 - x, to_core).wait_send()

        @pl.when(row == 0)
        def _():
            send_back(1).wait_send()
            send_back(2).wait_send()

        @pl.when(row == 1)
        def _():
            put_cross().wait()
            send_back(0).wait_send()

    for t in range(COLS // LAST):
        put_last(t).wait()
    for m in range(NUM - 1, 0, -1):
        send_grad(m).wait_send()

    @pl.when(row == 0)
    def _():
        for t in FAR:
            send_right(t).wait_send()

    @pl.when(row == 1)
    def _():
        for t in range(COLS // LAST):
            send_last(t).wait_send()


def copy_kernel(source, target, buffer, read_sem, write_sem):
    rows = source.shape[0] // COPY_PARTS
    part = lambda ref, k: ref.at[pl.ds(k * rows, rows)]
    reads = [pltpu.make_async_copy(part(source, k), part(buffer, k), read_sem.at[k]) for k in range(COPY_PARTS)]
    writes = [pltpu.make_async_copy(part(buffer, k), part(target, k), write_sem.at[k]) for k in range(COPY_PARTS)]
    for read in reads:
        read.start()
    for read, write in zip(reads, writes):
        read.wait()
        write.start()
    for write in writes:
        write.wait()


def solution(mesh):
    block_spec = P(("batch", "row"), "col")
    device = lambda row, col: row * 4 + col
    owners = [(row, 2 * chip + row) for row in range(2) for chip in range(2)]
    return_pairs = [(device(row, col), device(1 - row, col)) for row, col in owners if row == 1]

    def per_device(lower_tri, right_side, grad_out):
        bf16, f32 = jnp.bfloat16, jnp.float32
        dma = pltpu.SemaphoreType.DMA
        block = lambda count: jax.ShapeDtypeStruct((count, BLOCK, BLOCK), bf16)
        hbm = pl.BlockSpec(memory_space=pl.ANY)
        right_here, low, cross = pl.pallas_call(
            kernel,
            out_shape=(jax.ShapeDtypeStruct(grad_out.shape, bf16), block(12), block(RETURNED)),
            in_specs=[hbm] * 3,
            out_specs=[hbm] * 3,
            scratch_shapes=[
                pltpu.VMEM((NUM * BLOCK, COLS), bf16), pltpu.VMEM((NUM * BLOCK, COLS), bf16), pltpu.VMEM((NUM * BLOCK, COLS), bf16),
                pltpu.VMEM((2, 2, 12, BLOCK, BLOCK), bf16),
                pltpu.VMEM((21, BLOCK, BLOCK), f32), pltpu.VMEM((12, BLOCK, BLOCK), f32), pltpu.VMEM((3, BLOCK, BLOCK), f32),
                pltpu.VMEM((12, BLOCK, BLOCK), bf16), pltpu.VMEM((12, BLOCK, BLOCK), bf16),
                pltpu.VMEM((BLOCK, COLS), f32), pltpu.VMEM((BLOCK, COLS), bf16), pltpu.VMEM((2, BLOCK, NUM * BLOCK), bf16),
                dma((NUM,)), dma((NUM,)), dma((COLS // LAST,)), dma((COLS // LAST,)), dma((3,)), dma((3,)), dma((2, NUM)), dma((12,)), dma((3,)), dma((3,)), dma((3,)), dma((3,)),
                dma((2, NUM)), dma((2, NUM)), dma((2, NUM)), dma((2, NUM)), dma((3,)), dma((3,)), dma((3,)), dma((3,)), dma, dma((COLS // LAST,)), dma((2,)),
                pltpu.SemaphoreType.REGULAR, pltpu.SemaphoreType.REGULAR,
            ],
            compiler_params=pltpu.CompilerParams(collective_id=1, has_side_effects=True, vmem_limit_bytes=VMEM_BYTES),
        )(lower_tri, right_side, grad_out)

        grad_right = pl.pallas_call(
            copy_kernel,
            out_shape=jax.ShapeDtypeStruct(grad_out.shape, bf16),
            in_specs=[hbm],
            out_specs=hbm,
            scratch_shapes=[pltpu.VMEM(grad_out.shape, bf16), dma((COPY_PARTS,)), dma((COPY_PARTS,))],
            cost_estimate=pl.CostEstimate(flops=10 ** 10, bytes_accessed=4 * grad_out.size, transcendentals=0),
        )(right_here)
        got = lax.ppermute(cross, ("row", "col"), return_pairs)
        row, col = lax.axis_index("row"), lax.axis_index("col")
        is_back = jnp.logical_and(col % 2 == 1, row == 0)
        zero = jnp.zeros((BLOCK, BLOCK), bf16)

        def piece(m, p):
            if p > m // 2:
                return zero
            place = PLACE[m, p]
            return jnp.where(is_back, got[place], low[place]) if place < RETURNED else low[place]

        grad_lower = jnp.concatenate([jnp.concatenate([piece(m, p) for p in range(3)], axis=1) for m in range(NUM)], axis=0)
        return grad_right, grad_lower

    return jax.shard_map(per_device, mesh=mesh, in_specs=(block_spec, block_spec, block_spec), out_specs=(block_spec, block_spec), check_vma=False)
```

```python
import jax
import jax.numpy as jnp
from jax import lax
from jax.experimental import pallas as pl
from jax.experimental.pallas import tpu as pltpu
from jax.sharding import PartitionSpec as P

MESH = pl.DeviceIdType.MESH
BLOCK = 256
NUM = 6
COLS = 4096
TILE = 512
LAST = 1024
NEAR = (0, 1)
FAR = (2, 3)
VMEM_BYTES = 67043328
HOP_START = (0, 1, 2, 4, 6, 9)
PLACE = {(1, 0): 0, (2, 0): 1, (3, 0): 2, (3, 1): 3, (4, 0): 4, (4, 1): 5, (5, 0): 6, (5, 1): 7, (5, 2): 8, (0, 0): 9, (2, 1): 10, (4, 2): 11}
RETURNED = 6
RETURNED_FROM = 5
COPY_PARTS = 12


def dot_nt(lhs, rhs):
    return lax.dot_general(lhs, rhs, (((1,), (1,)), ((), ())), preferred_element_type=jnp.float32)


def kernel(lower, right, grad, out_right, out_low, out_cross,
           grad_v, right_v, other_v, lower_v, slot, hop, corner, fin_same, fin_cross, total, stage, turned,
           grad_send, grad_recv, last_send, last_recv, detour_send, detour_recv, load_sem, low_load, low_cross_send, low_cross_recv, low_send, low_recv,
           core_send, core_recv, hop_send, hop_recv, back_send, back_recv, corner_send, corner_recv, out_sem, put_sem, fin_sem, core_free, hop_free):
    row = lax.axis_index("row")
    col = lax.axis_index("col")
    x = col // 2
    owner = (col % 2) == row
    guest = jnp.logical_not(owner)
    to_row = {"row": 1 - row}
    to_core = {"col": col + 1 - 2 * (col % 2)}
    to_chip = {"col": lax.rem(col + 2, 4)}
    to_diag = {"row": 1 - row, "col": col + 1 - 2 * (col % 2)}

    def remote(src, dst, send, recv, where):
        return pltpu.make_async_remote_copy(src_ref=src, dst_ref=dst, send_sem=send, recv_sem=recv, device_id=where, device_id_type=MESH)

    def send_grad(m):
        return remote(grad.at[pl.ds(m * BLOCK, BLOCK)], other_v.at[pl.ds(m * BLOCK, BLOCK)], grad_send.at[m], grad_recv.at[m], to_row)

    def send_last(t):
        cols = pl.ds(t * LAST, LAST)
        return remote(grad.at[pl.ds(0, BLOCK), cols], other_v.at[pl.ds(0, BLOCK), cols], last_send.at[t], last_recv.at[t], to_row)

    def send_right(t):
        cols = pl.ds(t * LAST, LAST)
        return remote(right.at[pl.ds(0, BLOCK), cols], other_v.at[pl.ds(0, BLOCK), cols], last_send.at[t], last_recv.at[t], to_row)

    def load_low(target, p, m):
        return pltpu.make_async_copy(lower.at[pl.ds(m * BLOCK, BLOCK), pl.ds(p * BLOCK, BLOCK)], target.at[PLACE[m, p]], low_load.at[PLACE[m, p]])

    def each_low(target, act):
        for p in range(3):
            for m in range(2 * p, NUM):
                act(load_low(target, p, m))

    def cross_near(count):
        return remote(fin_same.at[pl.ds(0, count)], lower_v.at[x, 1, pl.ds(0, count)], low_cross_send.at[0], low_cross_recv.at[0], to_row)

    def cross_hand():
        return remote(fin_same.at[pl.ds(4, 8)], fin_cross.at[pl.ds(0, 8)], low_cross_send.at[1], low_cross_recv.at[1], to_core)

    def cross_far(first, count):
        return remote(fin_cross.at[pl.ds(first - 4, count)], lower_v.at[x, 1, pl.ds(first, count)], low_cross_send.at[2], low_cross_recv.at[2], to_diag)

    def detour(k):
        source, target, where = (
            (fin_same.at[pl.ds(9, 3)], fin_cross.at[pl.ds(0, 3)], to_chip),
            (fin_cross.at[pl.ds(0, 3)], fin_same.at[pl.ds(0, 3)], to_row),
            (fin_same.at[pl.ds(0, 3)], lower_v.at[0, 1, pl.ds(9, 3)], to_chip))[k]
        return remote(source, target, detour_send.at[k], detour_recv.at[k], where)

    def cross_cases(sender_row, act):
        for case, counts in ((sender_row == 0, (5, 5, 4)),
                             (jnp.logical_and(sender_row == 1, x == 0), (4, 4, 5)),
                             (jnp.logical_and(sender_row == 1, x == 1), (4, 4, 5))):
            @pl.when(case)
            def _(counts=counts):
                act(*counts)

    def send_back(k):
        part = (pl.ds(0, 9), pl.ds(10, 2), pl.ds(RETURNED, 3), pl.ds(0, 1), pl.ds(RETURNED, 2))[k]
        return remote(fin_cross.at[part], out_low.at[part], back_send.at[k], back_recv.at[k], to_row)

    def back_cases(kind, act):
        @pl.when(x == 0)
        def _():
            act(kind)

        if kind == 2:
            @pl.when(x == 1)
            def _():
                act(4)

    def send_low(index, half, where):
        return remote(lower_v.at[half], lower_v.at[half], low_send.at[index], low_recv.at[index], where)

    def load(src, dst, m, k):
        return pltpu.make_async_copy(src.at[pl.ds(m * BLOCK, BLOCK)], dst.at[pl.ds(m * BLOCK, BLOCK)], load_sem.at[k, m])

    def put_low(first, count, source):
        return pltpu.make_async_copy(source.at[pl.ds(first, count)], out_low.at[pl.ds(first, count)], fin_sem.at[0])

    def put_zero(place, k):
        return pltpu.make_async_copy(fin_cross.at[pl.ds(9, 1)], out_low.at[pl.ds(place, 1)], fin_sem.at[k])

    def put_cross():
        return pltpu.make_async_copy(fin_cross.at[pl.ds(1, RETURNED - 1)], out_cross, fin_sem.at[1])

    def send_core(group, m):
        part = slot.at[pl.ds(m * (m + 1) // 2, m + 1)]
        return remote(part, part, core_send.at[group, m], core_recv.at[group, m], to_core)

    def send_hop(group, m, side):
        base = m * (m + 1) // 2
        first, count = (base + m // 2 + 1, (m + 1) // 2) if side == 0 else (base, m // 2 + 1)
        return remote(slot.at[pl.ds(first, count)], hop.at[pl.ds(HOP_START[m], count)], hop_send.at[group, m], hop_recv.at[group, m], to_chip)

    @pl.when(guest)
    def _():
        fin_cross[9:] = jnp.zeros((3, BLOCK, BLOCK), jnp.bfloat16)

    barrier = pltpu.get_barrier_semaphore()
    for where in (to_row, to_core, to_chip, to_diag):
        pl.semaphore_signal(barrier, inc=1, device_id=where, device_id_type=MESH)
    pl.semaphore_wait(barrier, 4)

    send_grad(NUM - 1).start()

    @pl.when(guest)
    def _():
        each_low(fin_same, lambda copy: copy.start())

    @pl.when(owner)
    def _():
        each_low(lower_v.at[x, 0], lambda copy: copy.start())

    for m in range(NUM):
        load(grad, grad_v, m, 0).start()
        load(right, right_v, m, 1).start()

    @pl.when(guest)
    def _():
        each_low(fin_same, lambda copy: copy.wait())
        cross_hand().start()

        @pl.when(jnp.logical_and(row == 1, x == 0))
        def _():
            detour(0).start()

        cross_cases(row, lambda near, first, far: cross_near(near).start())

        @pl.when(jnp.logical_and(row == 1, x == 1))
        def _():
            detour(0).wait_recv()
            detour(1).start()

    @pl.when(owner)
    def _():
        @pl.when(jnp.logical_or(row == 1, x == 1))
        def _():
            lower_v[x, 1, 9:] = jnp.zeros((3, BLOCK, BLOCK), jnp.bfloat16)

        cross_hand().wait_recv()
        cross_cases(row, lambda near, first, far: cross_far(first, far).start())

    for m in range(NUM - 2, 1, -1):
        send_grad(m).start()

    send_grad(1).start()

    @pl.when(row == 0)
    def _():
        for t in FAR:
            send_right(t).start()

    @pl.when(row == 1)
    def _():
        for t in range(COLS // LAST):
            send_last(t).start()

    @pl.when(jnp.logical_and(guest, row == 0))
    def _():
        put_low(9, 3, fin_cross).start()

        @pl.when(x == 1)
        def _():
            put_zero(0, 2).start()
            put_zero(8, 3).start()

    def partial_sums(source, group, m):
        @pl.when(owner)
        def _():
            send_core(group, m).wait_recv()

        def one(n, carry):
            index = m * (m + 1) // 2 + (n % 2) * (m // 2 + 1) + n // 2
            value = dot_nt(source[pl.ds(m * BLOCK, BLOCK), :], right_v[pl.ds(pl.multiple_of(n * BLOCK, BLOCK), BLOCK), :])
            slot[index] = jnp.where(owner, slot[index], 0.0) + value
            return carry

        lax.fori_loop(0, m + 1, one, 0)

        @pl.when(guest)
        def _():
            send_core(group, m).start()

        for side in range(2):
            if side == 1 or m > 0:
                @pl.when(jnp.logical_and(owner, x == side))
                def _(side=side):
                    send_hop(group, m, side).start()

    def finish(group, m):
        for side in range(2):
            @pl.when(jnp.logical_and(owner, x == side))
            def _(side=side):
                if side == 0 or m > 0:
                    send_hop(group, m, 1 - side).wait_recv()
                if side == 1 or m > 0:
                    send_hop(group, m, side).wait_send()
                for p in range(m // 2 + 1):
                    n = 2 * p + side
                    target = fin_cross if group else fin_same
                    if n > m:
                        target[PLACE[m, p]] = jnp.zeros((BLOCK, BLOCK), jnp.bfloat16)
                        continue
                    value = slot[m * (m + 1) // 2 + side * (m // 2 + 1) + p] + hop[HOP_START[m] + p]
                    if n == m and group == 0:
                        rows = lax.broadcasted_iota(jnp.int32, (BLOCK, BLOCK), 0)
                        cols = lax.broadcasted_iota(jnp.int32, (BLOCK, BLOCK), 1)
                        value = jnp.where(rows >= cols, value, 0.0)
                    if n == m and group == 1:
                        value = jnp.where(row == 0, value, 0.0)
                    target[PLACE[m, p]] = value.astype(jnp.bfloat16)

    for m in range(NUM):
        load(grad, grad_v, m, 0).wait()
        load(right, right_v, m, 1).wait()
        partial_sums(grad_v, 0, m)

    @pl.when(owner)
    def _():
        each_low(lower_v.at[x, 0], lambda copy: copy.wait())
        def arrived(near, first, far):
            cross_near(near).wait_recv()
            cross_far(first, far).wait_recv()

        cross_cases(1 - row, arrived)

        @pl.when(jnp.logical_and(row == 0, x == 1))
        def _():
            detour(1).wait_recv()
            detour(2).start()
            detour(2).wait_send()

        @pl.when(jnp.logical_and(row == 0, x == 0))
        def _():
            detour(2).wait_recv()

        send_low(0, x, to_chip).start()
        send_low(1, x, to_core).start()

    for m in range(NUM):
        finish(0, m)

    @pl.when(owner)
    def _():
        pl.semaphore_signal(core_free, inc=1, device_id=to_core, device_id_type=MESH)
        pl.semaphore_signal(hop_free, inc=1, device_id=to_chip, device_id_type=MESH)
        send_low(0, 1 - x, to_chip).wait_recv()
        send_low(2, 1 - x, to_core).start()
        pl.semaphore_wait(hop_free, 1)
        put_low(0, 12, fin_same).start()

        cross_cases(row, lambda near, first, far: cross_far(first, far).wait_send())

    @pl.when(guest)
    def _():
        send_low(1, x, to_core).wait_recv()
        send_low(2, 1 - x, to_core).wait_recv()
        for m in range(NUM):
            send_core(0, m).wait_send()
        pl.semaphore_wait(core_free, 1)

    def turn(n):
        p, half = n // 2, n % 2
        for parity in range(2):
            for m in range(n, NUM):
                turned[parity, :, pl.ds((m - n) * BLOCK, BLOCK)] = lower_v[half, parity, PLACE[m, p]].T

    def put(n):
        return pltpu.make_async_copy(stage, out_right.at[pl.ds(n * BLOCK, BLOCK)], out_sem)

    def tiles(body):
        def one(t, carry):
            body(pl.ds(pl.multiple_of(t * TILE, TILE), TILE))
            return carry
        lax.fori_loop(0, COLS // TILE, one, 0)

    first_core = (col % 2) == 0

    def corner_core():
        return remote(slot.at[0], corner.at[0], corner_send.at[0], corner_recv.at[0], to_core)

    def corner_chip():
        return remote(slot.at[0], corner.at[1], corner_send.at[1], corner_recv.at[1], to_chip)

    def corner_row():
        return remote(slot.at[0], corner.at[2], corner_send.at[2], corner_recv.at[2], to_row)

    def corner_start(grads, rights, pieces):
        for t in pieces:
            cols = pl.ds(t * LAST, LAST)
            value = dot_nt(grads[:BLOCK, cols], rights[:BLOCK, cols])
            slot[0] = value if t == pieces[0] else slot[0] + value

        @pl.when(jnp.logical_not(first_core))
        def _():
            corner_core().start()

        @pl.when(first_core)
        def _():
            corner_core().wait_recv()
            slot[0] = slot[0] + corner[0]

            @pl.when(x == 1)
            def _():
                corner_chip().start()

    def corner_end():
        @pl.when(jnp.logical_not(first_core))
        def _():
            corner_core().wait_send()

        @pl.when(jnp.logical_and(first_core, x == 1))
        def _():
            corner_chip().wait_send()

    for m in range(NUM - 1, 0, -1):
        send_grad(m).wait_recv()
        partial_sums(other_v, 1, m)
        turn(m)
        if m < NUM - 1:
            put(m + 1).wait()
        depth = (NUM - m) * BLOCK

        def product(cols, m=m, depth=depth):
            value = jnp.dot(turned[0, :, :depth], grad_v[m * BLOCK:, cols], preferred_element_type=jnp.float32)
            value += jnp.dot(turned[1, :, :depth], other_v[m * BLOCK:, cols], preferred_element_type=jnp.float32)
            stage[:, cols] = value.astype(jnp.bfloat16)

        tiles(product)
        put(m).start()
        if m < NUM - 1:
            finish(1, m + 1)
        if m + 1 == RETURNED_FROM:
            @pl.when(jnp.logical_and(owner, row == 1))
            def _():
                back_cases(2, lambda k: send_back(k).start())

    turn(0)

    def all_but_last(cols):
        value = jnp.dot(turned[0], grad_v[:, cols], preferred_element_type=jnp.float32)
        total[:, cols] = value + jnp.dot(turned[1, :, BLOCK:], other_v[BLOCK:, cols], preferred_element_type=jnp.float32)

    tiles(all_but_last)
    finish(1, 1)

    @pl.when(jnp.logical_and(owner, row == 0))
    def _():
        send_back(0).start()
        send_back(1).start()

    @pl.when(jnp.logical_and(owner, row == 1))
    def _():
        put_cross().start()
        back_cases(3, lambda k: send_back(k).start())

    put(1).wait()

    def put_last(t):
        cols = pl.ds(t * LAST, LAST)
        return pltpu.make_async_copy(stage.at[:, cols], out_right.at[pl.ds(0, BLOCK), cols], put_sem.at[t])

    @pl.when(row == 0)
    def _():
        for t in range(COLS // LAST):
            cols = pl.ds(t * LAST, LAST)
            send_last(t).wait_recv()
            value = jnp.dot(turned[1, :, :BLOCK], other_v[:BLOCK, cols], preferred_element_type=jnp.float32)
            stage[:, cols] = (total[:, cols] + value).astype(jnp.bfloat16)
            put_last(t).start()
            if t == NEAR[-1]:
                corner_start(other_v, right_v, NEAR)

            if t == NEAR[-1] + 1:
                @pl.when(jnp.logical_and(first_core, x == 0))
                def _():
                    corner_chip().wait_recv()
                    slot[0] = slot[0] + corner[1]
                    corner_row().start()

        corner_end()

        @pl.when(jnp.logical_and(first_core, x == 0))
        def _():
            corner_row().wait_send()

    @pl.when(row == 1)
    def _():
        for t in range(COLS // LAST):
            cols = pl.ds(t * LAST, LAST)
            stage[:, cols] = total[:, cols].astype(jnp.bfloat16)
            put_last(t).start()
        for t in FAR:
            send_right(t).wait_recv()
        corner_start(grad_v, other_v, FAR)
        corner_end()

        @pl.when(jnp.logical_and(first_core, x == 0))
        def _():
            corner_chip().wait_recv()
            corner_row().wait_recv()
            fin_cross[9] = (slot[0] + corner[1] + corner[2]).astype(jnp.bfloat16)


    @pl.when(guest)
    def _():
        @pl.when(row == 0)
        def _():
            put_low(9, 3, fin_cross).wait()

            @pl.when(x == 1)
            def _():
                put_zero(0, 2).wait()
                put_zero(8, 3).wait()

            for kind in (2, 3):
                back_cases(kind, lambda k: send_back(k).wait_recv())

        @pl.when(row == 1)
        def _():
            put_low(9, 1, fin_cross).start()
            put_low(9, 1, fin_cross).wait()
            send_back(0).wait_recv()
            send_back(1).wait_recv()

        cross_hand().wait_send()
        cross_cases(row, lambda near, first, far: cross_near(near).wait_send())

        @pl.when(jnp.logical_and(row == 1, x == 0))
        def _():
            detour(0).wait_send()

        @pl.when(jnp.logical_and(row == 1, x == 1))
        def _():
            detour(1).wait_send()

        for m in range(1, NUM):
            send_core(1, m).wait_send()

    @pl.when(owner)
    def _():
        put_low(0, 12, fin_same).wait()
        send_low(0, x, to_chip).wait_send()
        send_low(1, x, to_core).wait_send()
        send_low(2, 1 - x, to_core).wait_send()

        @pl.when(row == 0)
        def _():
            send_back(0).wait_send()
            send_back(1).wait_send()

        @pl.when(row == 1)
        def _():
            put_cross().wait()
            for kind in (2, 3):
                back_cases(kind, lambda k: send_back(k).wait_send())

    for t in range(COLS // LAST):
        put_last(t).wait()
    for m in range(NUM - 1, 0, -1):
        send_grad(m).wait_send()

    @pl.when(row == 0)
    def _():
        for t in FAR:
            send_right(t).wait_send()

    @pl.when(row == 1)
    def _():
        for t in range(COLS // LAST):
            send_last(t).wait_send()


def copy_kernel(source, target, buffer, read_sem, write_sem):
    rows = source.shape[0] // COPY_PARTS
    part = lambda ref, k: ref.at[pl.ds(k * rows, rows)]
    reads = [pltpu.make_async_copy(part(source, k), part(buffer, k), read_sem.at[k]) for k in range(COPY_PARTS)]
    writes = [pltpu.make_async_copy(part(buffer, k), part(target, k), write_sem.at[k]) for k in range(COPY_PARTS)]
    for read in reads:
        read.start()
    for read, write in zip(reads, writes):
        read.wait()
        write.start()
    for write in writes:
        write.wait()


def solution(mesh):
    block_spec = P(("batch", "row"), "col")
    device = lambda row, col: row * 4 + col
    owners = [(row, 2 * chip + row) for row in range(2) for chip in range(2)]
    return_pairs = [(device(row, col), device(1 - row, col)) for row, col in owners if row == 1]

    def per_device(lower_tri, right_side, grad_out):
        bf16, f32 = jnp.bfloat16, jnp.float32
        dma = pltpu.SemaphoreType.DMA
        block = lambda count: jax.ShapeDtypeStruct((count, BLOCK, BLOCK), bf16)
        hbm = pl.BlockSpec(memory_space=pl.ANY)
        right_here, low, cross = pl.pallas_call(
            kernel,
            out_shape=(jax.ShapeDtypeStruct(grad_out.shape, bf16), block(12), block(RETURNED - 1)),
            in_specs=[hbm] * 3,
            out_specs=[hbm] * 3,
            scratch_shapes=[
                pltpu.VMEM((NUM * BLOCK, COLS), bf16), pltpu.VMEM((NUM * BLOCK, COLS), bf16), pltpu.VMEM((NUM * BLOCK, COLS), bf16),
                pltpu.VMEM((2, 2, 12, BLOCK, BLOCK), bf16),
                pltpu.VMEM((21, BLOCK, BLOCK), f32), pltpu.VMEM((12, BLOCK, BLOCK), f32), pltpu.VMEM((3, BLOCK, BLOCK), f32),
                pltpu.VMEM((12, BLOCK, BLOCK), bf16), pltpu.VMEM((12, BLOCK, BLOCK), bf16),
                pltpu.VMEM((BLOCK, COLS), f32), pltpu.VMEM((BLOCK, COLS), bf16), pltpu.VMEM((2, BLOCK, NUM * BLOCK), bf16),
                dma((NUM,)), dma((NUM,)), dma((COLS // LAST,)), dma((COLS // LAST,)), dma((3,)), dma((3,)), dma((2, NUM)), dma((12,)), dma((3,)), dma((3,)), dma((3,)), dma((3,)),
                dma((2, NUM)), dma((2, NUM)), dma((2, NUM)), dma((2, NUM)), dma((5,)), dma((5,)), dma((3,)), dma((3,)), dma, dma((COLS // LAST,)), dma((4,)),
                pltpu.SemaphoreType.REGULAR, pltpu.SemaphoreType.REGULAR,
            ],
            compiler_params=pltpu.CompilerParams(collective_id=1, has_side_effects=True, vmem_limit_bytes=VMEM_BYTES),
        )(lower_tri, right_side, grad_out)

        grad_right = pl.pallas_call(
            copy_kernel,
            out_shape=jax.ShapeDtypeStruct(grad_out.shape, bf16),
            in_specs=[hbm],
            out_specs=hbm,
            scratch_shapes=[pltpu.VMEM(grad_out.shape, bf16), dma((COPY_PARTS,)), dma((COPY_PARTS,))],
            cost_estimate=pl.CostEstimate(flops=10 ** 10, bytes_accessed=4 * grad_out.size, transcendentals=0),
        )(right_here)
        got = lax.ppermute(cross, ("row", "col"), return_pairs)
        row, col = lax.axis_index("row"), lax.axis_index("col")
        is_back = jnp.logical_and(col % 2 == 1, row == 0)
        zero = jnp.zeros((BLOCK, BLOCK), bf16)

        def piece(m, p):
            if p > m // 2:
                return zero
            place = PLACE[m, p]
            return jnp.where(is_back, got[place - 1], low[place]) if 0 < place < RETURNED else low[place]

        grad_lower = jnp.concatenate([jnp.concatenate([piece(m, p) for p in range(3)], axis=1) for m in range(NUM)], axis=0)
        return grad_right, grad_lower

    return jax.shard_map(per_device, mesh=mesh, in_specs=(block_spec, block_spec, block_spec), out_specs=(block_spec, block_spec), check_vma=False)
```

```python
import jax
import jax.numpy as jnp
from jax import lax
from jax.experimental import pallas as pl
from jax.experimental.pallas import tpu as pltpu
from jax.sharding import PartitionSpec as P

MESH = pl.DeviceIdType.MESH
BLOCK = 256
NUM = 6
COLS = 4096
TILE = 512
LAST = 1024
NEAR = (0, 1)
FAR = (2, 3)
VMEM_BYTES = 67043328
HOP_START = (0, 1, 2, 4, 6, 9)
PLACE = {(1, 0): 0, (2, 0): 1, (3, 0): 2, (3, 1): 3, (4, 0): 4, (4, 1): 5, (5, 0): 6, (5, 1): 7, (5, 2): 8, (0, 0): 9, (2, 1): 10, (4, 2): 11}
RETURNED = 6
SPARE = (0, 3)
RETURNED_FROM = 5
COPY_PARTS = 12


def dot_nt(lhs, rhs):
    return lax.dot_general(lhs, rhs, (((1,), (1,)), ((), ())), preferred_element_type=jnp.float32)


def kernel(lower, right, grad, out_right, out_low, out_cross,
           grad_v, right_v, other_v, lower_v, slot, hop, corner, fin_same, fin_cross, total, stage, turned,
           grad_send, grad_recv, last_send, last_recv, detour_send, detour_recv, load_sem, low_load, low_cross_send, low_cross_recv, low_send, low_recv,
           core_send, core_recv, hop_send, hop_recv, back_send, back_recv, corner_send, corner_recv, out_sem, put_sem, fin_sem, core_free, hop_free):
    row = lax.axis_index("row")
    col = lax.axis_index("col")
    x = col // 2
    owner = (col % 2) == row
    guest = jnp.logical_not(owner)
    to_row = {"row": 1 - row}
    to_core = {"col": col + 1 - 2 * (col % 2)}
    to_chip = {"col": lax.rem(col + 2, 4)}
    to_diag = {"row": 1 - row, "col": col + 1 - 2 * (col % 2)}

    def remote(src, dst, send, recv, where):
        return pltpu.make_async_remote_copy(src_ref=src, dst_ref=dst, send_sem=send, recv_sem=recv, device_id=where, device_id_type=MESH)

    def send_grad(m):
        return remote(grad.at[pl.ds(m * BLOCK, BLOCK)], other_v.at[pl.ds(m * BLOCK, BLOCK)], grad_send.at[m], grad_recv.at[m], to_row)

    def send_last(t):
        cols = pl.ds(t * LAST, LAST)
        return remote(grad.at[pl.ds(0, BLOCK), cols], other_v.at[pl.ds(0, BLOCK), cols], last_send.at[t], last_recv.at[t], to_row)

    def send_right(t):
        cols = pl.ds(t * LAST, LAST)
        return remote(right.at[pl.ds(0, BLOCK), cols], other_v.at[pl.ds(0, BLOCK), cols], last_send.at[t], last_recv.at[t], to_row)

    def load_low(target, p, m):
        return pltpu.make_async_copy(lower.at[pl.ds(m * BLOCK, BLOCK), pl.ds(p * BLOCK, BLOCK)], target.at[PLACE[m, p]], low_load.at[PLACE[m, p]])

    def each_low(target, act):
        for p in range(3):
            for m in range(2 * p, NUM):
                act(load_low(target, p, m))

    def cross_near(count):
        return remote(fin_same.at[pl.ds(0, count)], lower_v.at[x, 1, pl.ds(0, count)], low_cross_send.at[0], low_cross_recv.at[0], to_row)

    def cross_hand():
        return remote(fin_same.at[pl.ds(3, 9)], fin_cross.at[pl.ds(0, 9)], low_cross_send.at[1], low_cross_recv.at[1], to_core)

    def cross_far(first, count):
        return remote(fin_cross.at[pl.ds(first - 3, count)], lower_v.at[x, 1, pl.ds(first, count)], low_cross_send.at[2], low_cross_recv.at[2], to_diag)

    def detour(k):
        source, target, where = (
            (fin_same.at[pl.ds(9, 3)], fin_cross.at[pl.ds(0, 3)], to_chip),
            (fin_cross.at[pl.ds(0, 3)], fin_same.at[pl.ds(0, 3)], to_row),
            (fin_same.at[pl.ds(0, 3)], lower_v.at[0, 1, pl.ds(9, 3)], to_chip))[k]
        return remote(source, target, detour_send.at[k], detour_recv.at[k], where)

    def cross_cases(sender_row, act):
        for case, counts in ((sender_row == 0, (5, 5, 4)),
                             (jnp.logical_and(sender_row == 1, x == 0), (4, 4, 5)),
                             (jnp.logical_and(sender_row == 1, x == 1), (3, 3, 6))):
            @pl.when(case)
            def _(counts=counts):
                act(*counts)

    def send_back(k):
        part = (pl.ds(0, 9), pl.ds(10, 2), pl.ds(RETURNED, 3))[k]
        return remote(fin_cross.at[part], out_low.at[part], back_send.at[k], back_recv.at[k], to_row)

    def send_low(index, half, where):
        return remote(lower_v.at[half], lower_v.at[half], low_send.at[index], low_recv.at[index], where)

    def load(src, dst, m, k):
        return pltpu.make_async_copy(src.at[pl.ds(m * BLOCK, BLOCK)], dst.at[pl.ds(m * BLOCK, BLOCK)], load_sem.at[k, m])

    def put_low(first, count, source):
        return pltpu.make_async_copy(source.at[pl.ds(first, count)], out_low.at[pl.ds(first, count)], fin_sem.at[0])

    def put_zero():
        return pltpu.make_async_copy(fin_cross.at[pl.ds(9, 1)], out_low.at[pl.ds(8, 1)], fin_sem.at[1])

    def put_cross(act):
        def part(first, count, place, k):
            return pltpu.make_async_copy(fin_cross.at[pl.ds(first, count)], out_cross.at[pl.ds(place, count)], fin_sem.at[k])

        @pl.when(x == 0)
        def _():
            act(part(0, RETURNED, 0, 1))

        @pl.when(x == 1)
        def _():
            act(part(RETURNED, 1, 0, 1))
            act(part(1, 2, 1, 2))
            act(part(RETURNED + 1, 1, 3, 3))
            act(part(4, 2, 4, 4))

    def send_core(group, m):
        part = slot.at[pl.ds(m * (m + 1) // 2, m + 1)]
        return remote(part, part, core_send.at[group, m], core_recv.at[group, m], to_core)

    def send_hop(group, m, side):
        base = m * (m + 1) // 2
        first, count = (base + m // 2 + 1, (m + 1) // 2) if side == 0 else (base, m // 2 + 1)
        return remote(slot.at[pl.ds(first, count)], hop.at[pl.ds(HOP_START[m], count)], hop_send.at[group, m], hop_recv.at[group, m], to_chip)

    @pl.when(guest)
    def _():
        fin_cross[9:] = jnp.zeros((3, BLOCK, BLOCK), jnp.bfloat16)

    barrier = pltpu.get_barrier_semaphore()
    for where in (to_row, to_core, to_chip, to_diag):
        pl.semaphore_signal(barrier, inc=1, device_id=where, device_id_type=MESH)
    pl.semaphore_wait(barrier, 4)

    send_grad(NUM - 1).start()

    @pl.when(guest)
    def _():
        each_low(fin_same, lambda copy: copy.start())

    @pl.when(owner)
    def _():
        each_low(lower_v.at[x, 0], lambda copy: copy.start())

    for m in range(NUM):
        load(grad, grad_v, m, 0).start()
        load(right, right_v, m, 1).start()

    @pl.when(guest)
    def _():
        each_low(fin_same, lambda copy: copy.wait())
        cross_hand().start()

        @pl.when(jnp.logical_and(row == 1, x == 0))
        def _():
            detour(0).start()

        cross_cases(row, lambda near, first, far: cross_near(near).start())

        @pl.when(jnp.logical_and(row == 1, x == 1))
        def _():
            detour(0).wait_recv()
            detour(1).start()

    @pl.when(owner)
    def _():
        @pl.when(jnp.logical_or(row == 1, x == 1))
        def _():
            lower_v[x, 1, 9:] = jnp.zeros((3, BLOCK, BLOCK), jnp.bfloat16)

        cross_hand().wait_recv()
        cross_cases(row, lambda near, first, far: cross_far(first, far).start())

    for m in range(NUM - 2, 1, -1):
        send_grad(m).start()

    send_grad(1).start()

    @pl.when(row == 0)
    def _():
        for t in FAR:
            send_right(t).start()

    @pl.when(row == 1)
    def _():
        for t in range(COLS // LAST):
            send_last(t).start()

    @pl.when(jnp.logical_and(guest, row == 0))
    def _():
        put_low(9, 3, fin_cross).start()

        @pl.when(x == 1)
        def _():
            put_zero().start()

    def partial_sums(source, group, m):
        @pl.when(owner)
        def _():
            send_core(group, m).wait_recv()

        def one(n, carry):
            index = m * (m + 1) // 2 + (n % 2) * (m // 2 + 1) + n // 2
            value = dot_nt(source[pl.ds(m * BLOCK, BLOCK), :], right_v[pl.ds(pl.multiple_of(n * BLOCK, BLOCK), BLOCK), :])
            slot[index] = jnp.where(owner, slot[index], 0.0) + value
            return carry

        lax.fori_loop(0, m + 1, one, 0)

        @pl.when(guest)
        def _():
            send_core(group, m).start()

        for side in range(2):
            if side == 1 or m > 0:
                @pl.when(jnp.logical_and(owner, x == side))
                def _(side=side):
                    send_hop(group, m, side).start()

    def finish(group, m):
        for side in range(2):
            @pl.when(jnp.logical_and(owner, x == side))
            def _(side=side):
                if side == 0 or m > 0:
                    send_hop(group, m, 1 - side).wait_recv()
                if side == 1 or m > 0:
                    send_hop(group, m, side).wait_send()
                for p in range(m // 2 + 1):
                    n = 2 * p + side
                    target = fin_cross if group else fin_same
                    if n > m:
                        target[PLACE[m, p]] = jnp.zeros((BLOCK, BLOCK), jnp.bfloat16)
                        continue
                    value = slot[m * (m + 1) // 2 + side * (m // 2 + 1) + p] + hop[HOP_START[m] + p]
                    if n == m and group == 0:
                        rows = lax.broadcasted_iota(jnp.int32, (BLOCK, BLOCK), 0)
                        cols = lax.broadcasted_iota(jnp.int32, (BLOCK, BLOCK), 1)
                        value = jnp.where(rows >= cols, value, 0.0)
                    if n == m and group == 1:
                        value = jnp.where(row == 0, value, 0.0)
                    target[PLACE[m, p]] = value.astype(jnp.bfloat16)

    for m in range(NUM):
        load(grad, grad_v, m, 0).wait()
        load(right, right_v, m, 1).wait()
        partial_sums(grad_v, 0, m)

    @pl.when(owner)
    def _():
        each_low(lower_v.at[x, 0], lambda copy: copy.wait())
        def arrived(near, first, far):
            cross_near(near).wait_recv()
            cross_far(first, far).wait_recv()

        cross_cases(1 - row, arrived)

        @pl.when(jnp.logical_and(row == 0, x == 1))
        def _():
            detour(1).wait_recv()
            detour(2).start()
            detour(2).wait_send()

        @pl.when(jnp.logical_and(row == 0, x == 0))
        def _():
            detour(2).wait_recv()

        send_low(0, x, to_chip).start()
        send_low(1, x, to_core).start()

    for m in range(NUM):
        finish(0, m)

    @pl.when(owner)
    def _():
        pl.semaphore_signal(core_free, inc=1, device_id=to_core, device_id_type=MESH)
        pl.semaphore_signal(hop_free, inc=1, device_id=to_chip, device_id_type=MESH)
        send_low(0, 1 - x, to_chip).wait_recv()
        send_low(2, 1 - x, to_core).start()
        pl.semaphore_wait(hop_free, 1)
        put_low(0, 12, fin_same).start()

        cross_cases(row, lambda near, first, far: cross_far(first, far).wait_send())

    @pl.when(guest)
    def _():
        send_low(1, x, to_core).wait_recv()
        send_low(2, 1 - x, to_core).wait_recv()
        for m in range(NUM):
            send_core(0, m).wait_send()
        pl.semaphore_wait(core_free, 1)

    def turn(n):
        p, half = n // 2, n % 2
        for parity in range(2):
            for m in range(n, NUM):
                turned[parity, :, pl.ds((m - n) * BLOCK, BLOCK)] = lower_v[half, parity, PLACE[m, p]].T

    def put(n):
        return pltpu.make_async_copy(stage, out_right.at[pl.ds(n * BLOCK, BLOCK)], out_sem)

    def tiles(body):
        def one(t, carry):
            body(pl.ds(pl.multiple_of(t * TILE, TILE), TILE))
            return carry
        lax.fori_loop(0, COLS // TILE, one, 0)

    first_core = (col % 2) == 0

    def corner_core():
        return remote(slot.at[0], corner.at[0], corner_send.at[0], corner_recv.at[0], to_core)

    def corner_chip():
        return remote(slot.at[0], corner.at[1], corner_send.at[1], corner_recv.at[1], to_chip)

    def corner_row():
        return remote(slot.at[0], corner.at[2], corner_send.at[2], corner_recv.at[2], to_row)

    def corner_start(grads, rights, pieces):
        for t in pieces:
            cols = pl.ds(t * LAST, LAST)
            value = dot_nt(grads[:BLOCK, cols], rights[:BLOCK, cols])
            slot[0] = value if t == pieces[0] else slot[0] + value

        @pl.when(jnp.logical_not(first_core))
        def _():
            corner_core().start()

        @pl.when(first_core)
        def _():
            corner_core().wait_recv()
            slot[0] = slot[0] + corner[0]

            @pl.when(x == 1)
            def _():
                corner_chip().start()

    def corner_end():
        @pl.when(jnp.logical_not(first_core))
        def _():
            corner_core().wait_send()

        @pl.when(jnp.logical_and(first_core, x == 1))
        def _():
            corner_chip().wait_send()

    for m in range(NUM - 1, 0, -1):
        send_grad(m).wait_recv()
        partial_sums(other_v, 1, m)
        turn(m)
        if m < NUM - 1:
            put(m + 1).wait()
        depth = (NUM - m) * BLOCK

        def product(cols, m=m, depth=depth):
            value = jnp.dot(turned[0, :, :depth], grad_v[m * BLOCK:, cols], preferred_element_type=jnp.float32)
            value += jnp.dot(turned[1, :, :depth], other_v[m * BLOCK:, cols], preferred_element_type=jnp.float32)
            stage[:, cols] = value.astype(jnp.bfloat16)

        tiles(product)
        put(m).start()
        if m < NUM - 1:
            finish(1, m + 1)
        if m + 1 == RETURNED_FROM:
            @pl.when(jnp.logical_and(owner, jnp.logical_and(row == 1, x == 0)))
            def _():
                send_back(2).start()

    turn(0)

    def all_but_last(cols):
        value = jnp.dot(turned[0], grad_v[:, cols], preferred_element_type=jnp.float32)
        total[:, cols] = value + jnp.dot(turned[1, :, BLOCK:], other_v[BLOCK:, cols], preferred_element_type=jnp.float32)

    tiles(all_but_last)
    finish(1, 1)

    @pl.when(jnp.logical_and(owner, row == 0))
    def _():
        send_back(0).start()
        send_back(1).start()

    @pl.when(jnp.logical_and(owner, row == 1))
    def _():
        put_cross(lambda copy: copy.start())

    put(1).wait()

    def put_last(t):
        cols = pl.ds(t * LAST, LAST)
        return pltpu.make_async_copy(stage.at[:, cols], out_right.at[pl.ds(0, BLOCK), cols], put_sem.at[t])

    @pl.when(row == 0)
    def _():
        for t in range(COLS // LAST):
            cols = pl.ds(t * LAST, LAST)
            send_last(t).wait_recv()
            value = jnp.dot(turned[1, :, :BLOCK], other_v[:BLOCK, cols], preferred_element_type=jnp.float32)
            stage[:, cols] = (total[:, cols] + value).astype(jnp.bfloat16)
            put_last(t).start()
            if t == NEAR[-1]:
                corner_start(other_v, right_v, NEAR)

            if t == NEAR[-1] + 1:
                @pl.when(jnp.logical_and(first_core, x == 0))
                def _():
                    corner_chip().wait_recv()
                    slot[0] = slot[0] + corner[1]
                    corner_row().start()

        corner_end()

        @pl.when(jnp.logical_and(first_core, x == 0))
        def _():
            corner_row().wait_send()

    @pl.when(row == 1)
    def _():
        for t in range(COLS // LAST):
            cols = pl.ds(t * LAST, LAST)
            stage[:, cols] = total[:, cols].astype(jnp.bfloat16)
            put_last(t).start()
        for t in FAR:
            send_right(t).wait_recv()
        corner_start(grad_v, other_v, FAR)
        corner_end()

        @pl.when(jnp.logical_and(first_core, x == 0))
        def _():
            corner_chip().wait_recv()
            corner_row().wait_recv()
            fin_cross[9] = (slot[0] + corner[1] + corner[2]).astype(jnp.bfloat16)


    @pl.when(guest)
    def _():
        @pl.when(row == 0)
        def _():
            put_low(9, 3, fin_cross).wait()

            @pl.when(x == 0)
            def _():
                send_back(2).wait_recv()

            @pl.when(x == 1)
            def _():
                put_zero().wait()

        @pl.when(row == 1)
        def _():
            put_low(9, 1, fin_cross).start()
            put_low(9, 1, fin_cross).wait()
            send_back(0).wait_recv()
            send_back(1).wait_recv()

        cross_hand().wait_send()
        cross_cases(row, lambda near, first, far: cross_near(near).wait_send())

        @pl.when(jnp.logical_and(row == 1, x == 0))
        def _():
            detour(0).wait_send()

        @pl.when(jnp.logical_and(row == 1, x == 1))
        def _():
            detour(1).wait_send()

        for m in range(1, NUM):
            send_core(1, m).wait_send()

    @pl.when(owner)
    def _():
        put_low(0, 12, fin_same).wait()
        send_low(0, x, to_chip).wait_send()
        send_low(1, x, to_core).wait_send()
        send_low(2, 1 - x, to_core).wait_send()

        @pl.when(row == 0)
        def _():
            send_back(0).wait_send()
            send_back(1).wait_send()

        @pl.when(row == 1)
        def _():
            put_cross(lambda copy: copy.wait())

            @pl.when(x == 0)
            def _():
                send_back(2).wait_send()

    for t in range(COLS // LAST):
        put_last(t).wait()
    for m in range(NUM - 1, 0, -1):
        send_grad(m).wait_send()

    @pl.when(row == 0)
    def _():
        for t in FAR:
            send_right(t).wait_send()

    @pl.when(row == 1)
    def _():
        for t in range(COLS // LAST):
            send_last(t).wait_send()


def copy_kernel(source, target, buffer, read_sem, write_sem):
    rows = source.shape[0] // COPY_PARTS
    part = lambda ref, k: ref.at[pl.ds(k * rows, rows)]
    reads = [pltpu.make_async_copy(part(source, k), part(buffer, k), read_sem.at[k]) for k in range(COPY_PARTS)]
    writes = [pltpu.make_async_copy(part(buffer, k), part(target, k), write_sem.at[k]) for k in range(COPY_PARTS)]
    for read in reads:
        read.start()
    for read, write in zip(reads, writes):
        read.wait()
        write.start()
    for write in writes:
        write.wait()


def solution(mesh):
    block_spec = P(("batch", "row"), "col")
    device = lambda row, col: row * 4 + col
    owners = [(row, 2 * chip + row) for row in range(2) for chip in range(2)]
    return_pairs = [(device(row, col), device(1 - row, col)) for row, col in owners if row == 1]

    def per_device(lower_tri, right_side, grad_out):
        bf16, f32 = jnp.bfloat16, jnp.float32
        dma = pltpu.SemaphoreType.DMA
        block = lambda count: jax.ShapeDtypeStruct((count, BLOCK, BLOCK), bf16)
        hbm = pl.BlockSpec(memory_space=pl.ANY)
        right_here, low, cross = pl.pallas_call(
            kernel,
            out_shape=(jax.ShapeDtypeStruct(grad_out.shape, bf16), block(12), block(RETURNED)),
            in_specs=[hbm] * 3,
            out_specs=[hbm] * 3,
            scratch_shapes=[
                pltpu.VMEM((NUM * BLOCK, COLS), bf16), pltpu.VMEM((NUM * BLOCK, COLS), bf16), pltpu.VMEM((NUM * BLOCK, COLS), bf16),
                pltpu.VMEM((2, 2, 12, BLOCK, BLOCK), bf16),
                pltpu.VMEM((21, BLOCK, BLOCK), f32), pltpu.VMEM((12, BLOCK, BLOCK), f32), pltpu.VMEM((3, BLOCK, BLOCK), f32),
                pltpu.VMEM((12, BLOCK, BLOCK), bf16), pltpu.VMEM((12, BLOCK, BLOCK), bf16),
                pltpu.VMEM((BLOCK, COLS), f32), pltpu.VMEM((BLOCK, COLS), bf16), pltpu.VMEM((2, BLOCK, NUM * BLOCK), bf16),
                dma((NUM,)), dma((NUM,)), dma((COLS // LAST,)), dma((COLS // LAST,)), dma((3,)), dma((3,)), dma((2, NUM)), dma((12,)), dma((3,)), dma((3,)), dma((3,)), dma((3,)),
                dma((2, NUM)), dma((2, NUM)), dma((2, NUM)), dma((2, NUM)), dma((3,)), dma((3,)), dma((3,)), dma((3,)), dma, dma((COLS // LAST,)), dma((5,)),
                pltpu.SemaphoreType.REGULAR, pltpu.SemaphoreType.REGULAR,
            ],
            compiler_params=pltpu.CompilerParams(collective_id=1, has_side_effects=True, vmem_limit_bytes=VMEM_BYTES),
        )(lower_tri, right_side, grad_out)

        grad_right = pl.pallas_call(
            copy_kernel,
            out_shape=jax.ShapeDtypeStruct(grad_out.shape, bf16),
            in_specs=[hbm],
            out_specs=hbm,
            scratch_shapes=[pltpu.VMEM(grad_out.shape, bf16), dma((COPY_PARTS,)), dma((COPY_PARTS,))],
            cost_estimate=pl.CostEstimate(flops=10 ** 10, bytes_accessed=4 * grad_out.size, transcendentals=0),
        )(right_here)
        got = lax.ppermute(cross, ("row", "col"), return_pairs)
        row, col = lax.axis_index("row"), lax.axis_index("col")
        is_back = jnp.logical_and(col % 2 == 1, row == 0)
        swapped = jnp.logical_and(is_back, col // 2 == 1)
        zero = jnp.zeros((BLOCK, BLOCK), bf16)
        got = jnp.where(is_back, got, low[:RETURNED])
        spare = [jnp.where(swapped, zero, got[place]) for place in SPARE]
        moved = [jnp.where(swapped, got[place], low[RETURNED + k]) for k, place in enumerate(SPARE)]
        got, spare, moved = lax.optimization_barrier((got, spare, moved))
        blocks = [spare[0], got[1], got[2], spare[1], got[4], got[5], moved[0], moved[1]] + [low[k] for k in range(8, 12)]
        piece = lambda m, p: blocks[PLACE[m, p]] if p <= m // 2 else zero
        grad_lower = jnp.concatenate([jnp.concatenate([piece(m, p) for p in range(3)], axis=1) for m in range(NUM)], axis=0)
        return grad_right, grad_lower

    return jax.shard_map(per_device, mesh=mesh, in_specs=(block_spec, block_spec, block_spec), out_specs=(block_spec, block_spec), check_vma=False)
```

```python
import jax
import jax.numpy as jnp
from jax import lax
from jax.experimental import pallas as pl
from jax.experimental.pallas import tpu as pltpu
from jax.sharding import PartitionSpec as P

MESH = pl.DeviceIdType.MESH
BLOCK = 256
NUM = 6
COLS = 4096
TILE = 512
LAST = 1024
NEAR = (0, 1)
FAR = (2, 3)
VMEM_BYTES = 67043328
HOP_START = (0, 1, 2, 4, 6, 9)
PLACE = {(1, 0): 0, (2, 0): 1, (3, 0): 2, (3, 1): 3, (4, 0): 4, (4, 1): 5, (5, 0): 6, (5, 1): 7, (5, 2): 8, (0, 0): 9, (2, 1): 10, (4, 2): 11}
RETURNED = 6
SPARE = (0, 3)
RETURNED_FROM = 5
COPY_PARTS = 12


def dot_nt(lhs, rhs):
    return lax.dot_general(lhs, rhs, (((1,), (1,)), ((), ())), preferred_element_type=jnp.float32)


def kernel(lower, right, grad, out_right, out_low, out_cross,
           grad_v, right_v, other_v, lower_v, slot, hop, corner, fin_same, fin_cross, total, stage, turned,
           grad_send, grad_recv, last_send, last_recv, detour_send, detour_recv, load_sem, low_load, low_cross_send, low_cross_recv, low_send, low_recv,
           core_send, core_recv, hop_send, hop_recv, back_send, back_recv, corner_send, corner_recv, out_sem, put_sem, fin_sem, core_free, hop_free):
    row = lax.axis_index("row")
    col = lax.axis_index("col")
    x = col // 2
    owner = (col % 2) == row
    guest = jnp.logical_not(owner)
    to_row = {"row": 1 - row}
    to_core = {"col": col + 1 - 2 * (col % 2)}
    to_chip = {"col": lax.rem(col + 2, 4)}
    to_diag = {"row": 1 - row, "col": col + 1 - 2 * (col % 2)}

    def remote(src, dst, send, recv, where):
        return pltpu.make_async_remote_copy(src_ref=src, dst_ref=dst, send_sem=send, recv_sem=recv, device_id=where, device_id_type=MESH)

    def send_grad(m):
        return remote(grad.at[pl.ds(m * BLOCK, BLOCK)], other_v.at[pl.ds(m * BLOCK, BLOCK)], grad_send.at[m], grad_recv.at[m], to_row)

    def send_last(t):
        cols = pl.ds(t * LAST, LAST)
        return remote(grad.at[pl.ds(0, BLOCK), cols], other_v.at[pl.ds(0, BLOCK), cols], last_send.at[t], last_recv.at[t], to_row)

    def send_right(t):
        cols = pl.ds(t * LAST, LAST)
        return remote(right.at[pl.ds(0, BLOCK), cols], other_v.at[pl.ds(0, BLOCK), cols], last_send.at[t], last_recv.at[t], to_row)

    def load_low(target, p, m):
        return pltpu.make_async_copy(lower.at[pl.ds(m * BLOCK, BLOCK), pl.ds(p * BLOCK, BLOCK)], target.at[PLACE[m, p]], low_load.at[PLACE[m, p]])

    def each_low(target, act):
        for p in range(3):
            for m in range(2 * p, NUM):
                act(load_low(target, p, m))

    def cross_near(count):
        return remote(fin_same.at[pl.ds(0, count)], lower_v.at[x, 1, pl.ds(0, count)], low_cross_send.at[0], low_cross_recv.at[0], to_row)

    def cross_hand():
        return remote(fin_same.at[pl.ds(3, 9)], fin_cross.at[pl.ds(0, 9)], low_cross_send.at[1], low_cross_recv.at[1], to_core)

    def cross_far(first, count):
        return remote(fin_cross.at[pl.ds(first - 3, count)], lower_v.at[x, 1, pl.ds(first, count)], low_cross_send.at[2], low_cross_recv.at[2], to_diag)

    def detour(k):
        source, target, where = (
            (fin_same.at[pl.ds(8, 4)], fin_cross.at[pl.ds(0, 4)], to_chip),
            (fin_cross.at[pl.ds(0, 4)], fin_same.at[pl.ds(0, 4)], to_row),
            (fin_same.at[pl.ds(0, 4)], lower_v.at[0, 1, pl.ds(8, 4)], to_chip))[k]
        return remote(source, target, detour_send.at[k], detour_recv.at[k], where)

    def cross_cases(sender_row, act):
        for case, counts in ((sender_row == 0, (5, 5, 4)),
                             (jnp.logical_and(sender_row == 1, x == 0), (4, 4, 4)),
                             (jnp.logical_and(sender_row == 1, x == 1), (4, 4, 5))):
            @pl.when(case)
            def _(counts=counts):
                act(*counts)

    def send_back(k):
        part = (pl.ds(0, 9), pl.ds(10, 2), pl.ds(RETURNED, 3))[k]
        return remote(fin_cross.at[part], out_low.at[part], back_send.at[k], back_recv.at[k], to_row)

    def send_low(index, half, where):
        return remote(lower_v.at[half], lower_v.at[half], low_send.at[index], low_recv.at[index], where)

    def load(src, dst, m, k):
        return pltpu.make_async_copy(src.at[pl.ds(m * BLOCK, BLOCK)], dst.at[pl.ds(m * BLOCK, BLOCK)], load_sem.at[k, m])

    def put_low(first, count, source):
        return pltpu.make_async_copy(source.at[pl.ds(first, count)], out_low.at[pl.ds(first, count)], fin_sem.at[0])

    def put_zero():
        return pltpu.make_async_copy(fin_cross.at[pl.ds(9, 1)], out_low.at[pl.ds(8, 1)], fin_sem.at[1])

    def put_cross(act):
        def part(first, count, place, k):
            return pltpu.make_async_copy(fin_cross.at[pl.ds(first, count)], out_cross.at[pl.ds(place, count)], fin_sem.at[k])

        @pl.when(x == 0)
        def _():
            act(part(0, RETURNED, 0, 1))

        @pl.when(x == 1)
        def _():
            act(part(RETURNED, 1, 0, 1))
            act(part(1, 2, 1, 2))
            act(part(RETURNED + 1, 1, 3, 3))
            act(part(4, 2, 4, 4))

    def send_core(group, m):
        part = slot.at[pl.ds(m * (m + 1) // 2, m + 1)]
        return remote(part, part, core_send.at[group, m], core_recv.at[group, m], to_core)

    def send_hop(group, m, side):
        base = m * (m + 1) // 2
        first, count = (base + m // 2 + 1, (m + 1) // 2) if side == 0 else (base, m // 2 + 1)
        return remote(slot.at[pl.ds(first, count)], hop.at[pl.ds(HOP_START[m], count)], hop_send.at[group, m], hop_recv.at[group, m], to_chip)

    @pl.when(guest)
    def _():
        fin_cross[9:] = jnp.zeros((3, BLOCK, BLOCK), jnp.bfloat16)

    barrier = pltpu.get_barrier_semaphore()
    for where in (to_row, to_core, to_chip, to_diag):
        pl.semaphore_signal(barrier, inc=1, device_id=where, device_id_type=MESH)
    pl.semaphore_wait(barrier, 4)

    send_grad(NUM - 1).start()

    @pl.when(guest)
    def _():
        each_low(fin_same, lambda copy: copy.start())

    @pl.when(owner)
    def _():
        each_low(lower_v.at[x, 0], lambda copy: copy.start())

    for m in range(NUM):
        load(grad, grad_v, m, 0).start()
        load(right, right_v, m, 1).start()

    @pl.when(guest)
    def _():
        each_low(fin_same, lambda copy: copy.wait())
        cross_hand().start()

        @pl.when(jnp.logical_and(row == 1, x == 0))
        def _():
            detour(0).start()

        cross_cases(row, lambda near, first, far: cross_near(near).start())

        @pl.when(jnp.logical_and(row == 1, x == 1))
        def _():
            detour(0).wait_recv()
            detour(1).start()

    @pl.when(owner)
    def _():
        @pl.when(jnp.logical_or(row == 1, x == 1))
        def _():
            lower_v[x, 1, 9:] = jnp.zeros((3, BLOCK, BLOCK), jnp.bfloat16)

        cross_hand().wait_recv()
        cross_cases(row, lambda near, first, far: cross_far(first, far).start())

    for m in range(NUM - 2, 1, -1):
        send_grad(m).start()

    send_grad(1).start()

    @pl.when(row == 0)
    def _():
        for t in FAR:
            send_right(t).start()

    @pl.when(row == 1)
    def _():
        for t in range(COLS // LAST):
            send_last(t).start()

    @pl.when(jnp.logical_and(guest, row == 0))
    def _():
        put_low(9, 3, fin_cross).start()

        @pl.when(x == 1)
        def _():
            put_zero().start()

    def partial_sums(source, group, m):
        @pl.when(owner)
        def _():
            send_core(group, m).wait_recv()

        def one(n, carry):
            index = m * (m + 1) // 2 + (n % 2) * (m // 2 + 1) + n // 2
            value = dot_nt(source[pl.ds(m * BLOCK, BLOCK), :], right_v[pl.ds(pl.multiple_of(n * BLOCK, BLOCK), BLOCK), :])
            slot[index] = jnp.where(owner, slot[index], 0.0) + value
            return carry

        lax.fori_loop(0, m + 1, one, 0)

        @pl.when(guest)
        def _():
            send_core(group, m).start()

        for side in range(2):
            if side == 1 or m > 0:
                @pl.when(jnp.logical_and(owner, x == side))
                def _(side=side):
                    send_hop(group, m, side).start()

    def finish(group, m):
        for side in range(2):
            @pl.when(jnp.logical_and(owner, x == side))
            def _(side=side):
                if side == 0 or m > 0:
                    send_hop(group, m, 1 - side).wait_recv()
                if side == 1 or m > 0:
                    send_hop(group, m, side).wait_send()
                for p in range(m // 2 + 1):
                    n = 2 * p + side
                    target = fin_cross if group else fin_same
                    if n > m:
                        target[PLACE[m, p]] = jnp.zeros((BLOCK, BLOCK), jnp.bfloat16)
                        continue
                    value = slot[m * (m + 1) // 2 + side * (m // 2 + 1) + p] + hop[HOP_START[m] + p]
                    if n == m and group == 0:
                        rows = lax.broadcasted_iota(jnp.int32, (BLOCK, BLOCK), 0)
                        cols = lax.broadcasted_iota(jnp.int32, (BLOCK, BLOCK), 1)
                        value = jnp.where(rows >= cols, value, 0.0)
                    if n == m and group == 1:
                        value = jnp.where(row == 0, value, 0.0)
                    target[PLACE[m, p]] = value.astype(jnp.bfloat16)

    for m in range(NUM):
        load(grad, grad_v, m, 0).wait()
        load(right, right_v, m, 1).wait()
        partial_sums(grad_v, 0, m)

    @pl.when(owner)
    def _():
        each_low(lower_v.at[x, 0], lambda copy: copy.wait())
        def arrived(near, first, far):
            cross_near(near).wait_recv()
            cross_far(first, far).wait_recv()

        cross_cases(1 - row, arrived)

        @pl.when(jnp.logical_and(row == 0, x == 1))
        def _():
            detour(1).wait_recv()
            detour(2).start()
            detour(2).wait_send()

        @pl.when(jnp.logical_and(row == 0, x == 0))
        def _():
            detour(2).wait_recv()

        send_low(0, x, to_chip).start()
        send_low(1, x, to_core).start()

    for m in range(NUM):
        finish(0, m)

    @pl.when(owner)
    def _():
        pl.semaphore_signal(core_free, inc=1, device_id=to_core, device_id_type=MESH)
        pl.semaphore_signal(hop_free, inc=1, device_id=to_chip, device_id_type=MESH)
        send_low(0, 1 - x, to_chip).wait_recv()
        send_low(2, 1 - x, to_core).start()
        pl.semaphore_wait(hop_free, 1)
        put_low(0, 12, fin_same).start()

        cross_cases(row, lambda near, first, far: cross_far(first, far).wait_send())

    @pl.when(guest)
    def _():
        send_low(1, x, to_core).wait_recv()
        send_low(2, 1 - x, to_core).wait_recv()
        for m in range(NUM):
            send_core(0, m).wait_send()
        pl.semaphore_wait(core_free, 1)

    def turn(n):
        p, half = n // 2, n % 2
        for parity in range(2):
            for m in range(n, NUM):
                turned[parity, :, pl.ds((m - n) * BLOCK, BLOCK)] = lower_v[half, parity, PLACE[m, p]].T

    def put(n):
        return pltpu.make_async_copy(stage, out_right.at[pl.ds(n * BLOCK, BLOCK)], out_sem)

    def tiles(body):
        def one(t, carry):
            body(pl.ds(pl.multiple_of(t * TILE, TILE), TILE))
            return carry
        lax.fori_loop(0, COLS // TILE, one, 0)

    first_core = (col % 2) == 0

    def corner_core():
        return remote(slot.at[0], corner.at[0], corner_send.at[0], corner_recv.at[0], to_core)

    def corner_chip():
        return remote(slot.at[0], corner.at[1], corner_send.at[1], corner_recv.at[1], to_chip)

    def corner_row():
        return remote(slot.at[0], corner.at[2], corner_send.at[2], corner_recv.at[2], to_row)

    def corner_start(grads, rights, pieces):
        for t in pieces:
            cols = pl.ds(t * LAST, LAST)
            value = dot_nt(grads[:BLOCK, cols], rights[:BLOCK, cols])
            slot[0] = value if t == pieces[0] else slot[0] + value

        @pl.when(jnp.logical_not(first_core))
        def _():
            corner_core().start()

        @pl.when(first_core)
        def _():
            corner_core().wait_recv()
            slot[0] = slot[0] + corner[0]

            @pl.when(x == 1)
            def _():
                corner_chip().start()

    def corner_end():
        @pl.when(jnp.logical_not(first_core))
        def _():
            corner_core().wait_send()

        @pl.when(jnp.logical_and(first_core, x == 1))
        def _():
            corner_chip().wait_send()

    for m in range(NUM - 1, 0, -1):
        send_grad(m).wait_recv()
        partial_sums(other_v, 1, m)
        turn(m)
        if m < NUM - 1:
            put(m + 1).wait()
        depth = (NUM - m) * BLOCK

        def product(cols, m=m, depth=depth):
            value = jnp.dot(turned[0, :, :depth], grad_v[m * BLOCK:, cols], preferred_element_type=jnp.float32)
            value += jnp.dot(turned[1, :, :depth], other_v[m * BLOCK:, cols], preferred_element_type=jnp.float32)
            stage[:, cols] = value.astype(jnp.bfloat16)

        tiles(product)
        put(m).start()
        if m < NUM - 1:
            finish(1, m + 1)
        if m + 1 == RETURNED_FROM:
            @pl.when(jnp.logical_and(owner, jnp.logical_and(row == 1, x == 0)))
            def _():
                send_back(2).start()

    turn(0)

    def all_but_last(cols):
        value = jnp.dot(turned[0], grad_v[:, cols], preferred_element_type=jnp.float32)
        total[:, cols] = value + jnp.dot(turned[1, :, BLOCK:], other_v[BLOCK:, cols], preferred_element_type=jnp.float32)

    tiles(all_but_last)
    finish(1, 1)

    @pl.when(jnp.logical_and(owner, row == 0))
    def _():
        send_back(0).start()
        send_back(1).start()

    @pl.when(jnp.logical_and(owner, row == 1))
    def _():
        put_cross(lambda copy: copy.start())

    put(1).wait()

    def put_last(t):
        cols = pl.ds(t * LAST, LAST)
        return pltpu.make_async_copy(stage.at[:, cols], out_right.at[pl.ds(0, BLOCK), cols], put_sem.at[t])

    @pl.when(row == 0)
    def _():
        for t in range(COLS // LAST):
            cols = pl.ds(t * LAST, LAST)
            send_last(t).wait_recv()
            value = jnp.dot(turned[1, :, :BLOCK], other_v[:BLOCK, cols], preferred_element_type=jnp.float32)
            stage[:, cols] = (total[:, cols] + value).astype(jnp.bfloat16)
            put_last(t).start()
            if t == NEAR[-1]:
                corner_start(other_v, right_v, NEAR)

            if t == NEAR[-1] + 1:
                @pl.when(jnp.logical_and(first_core, x == 0))
                def _():
                    corner_chip().wait_recv()
                    slot[0] = slot[0] + corner[1]
                    corner_row().start()

        corner_end()

        @pl.when(jnp.logical_and(first_core, x == 0))
        def _():
            corner_row().wait_send()

    @pl.when(row == 1)
    def _():
        for t in range(COLS // LAST):
            cols = pl.ds(t * LAST, LAST)
            stage[:, cols] = total[:, cols].astype(jnp.bfloat16)
            put_last(t).start()
        for t in FAR:
            send_right(t).wait_recv()
        corner_start(grad_v, other_v, FAR)
        corner_end()

        @pl.when(jnp.logical_and(first_core, x == 0))
        def _():
            corner_chip().wait_recv()
            corner_row().wait_recv()
            fin_cross[9] = (slot[0] + corner[1] + corner[2]).astype(jnp.bfloat16)


    @pl.when(guest)
    def _():
        @pl.when(row == 0)
        def _():
            put_low(9, 3, fin_cross).wait()

            @pl.when(x == 0)
            def _():
                send_back(2).wait_recv()

            @pl.when(x == 1)
            def _():
                put_zero().wait()

        @pl.when(row == 1)
        def _():
            put_low(9, 1, fin_cross).start()
            put_low(9, 1, fin_cross).wait()
            send_back(0).wait_recv()
            send_back(1).wait_recv()

        cross_hand().wait_send()
        cross_cases(row, lambda near, first, far: cross_near(near).wait_send())

        @pl.when(jnp.logical_and(row == 1, x == 0))
        def _():
            detour(0).wait_send()

        @pl.when(jnp.logical_and(row == 1, x == 1))
        def _():
            detour(1).wait_send()

        for m in range(1, NUM):
            send_core(1, m).wait_send()

    @pl.when(owner)
    def _():
        put_low(0, 12, fin_same).wait()
        send_low(0, x, to_chip).wait_send()
        send_low(1, x, to_core).wait_send()
        send_low(2, 1 - x, to_core).wait_send()

        @pl.when(row == 0)
        def _():
            send_back(0).wait_send()
            send_back(1).wait_send()

        @pl.when(row == 1)
        def _():
            put_cross(lambda copy: copy.wait())

            @pl.when(x == 0)
            def _():
                send_back(2).wait_send()

    for t in range(COLS // LAST):
        put_last(t).wait()
    for m in range(NUM - 1, 0, -1):
        send_grad(m).wait_send()

    @pl.when(row == 0)
    def _():
        for t in FAR:
            send_right(t).wait_send()

    @pl.when(row == 1)
    def _():
        for t in range(COLS // LAST):
            send_last(t).wait_send()


def copy_kernel(source, target, buffer, read_sem, write_sem):
    rows = source.shape[0] // COPY_PARTS
    part = lambda ref, k: ref.at[pl.ds(k * rows, rows)]
    reads = [pltpu.make_async_copy(part(source, k), part(buffer, k), read_sem.at[k]) for k in range(COPY_PARTS)]
    writes = [pltpu.make_async_copy(part(buffer, k), part(target, k), write_sem.at[k]) for k in range(COPY_PARTS)]
    for read in reads:
        read.start()
    for read, write in zip(reads, writes):
        read.wait()
        write.start()
    for write in writes:
        write.wait()


def solution(mesh):
    block_spec = P(("batch", "row"), "col")
    device = lambda row, col: row * 4 + col
    owners = [(row, 2 * chip + row) for row in range(2) for chip in range(2)]
    return_pairs = [(device(row, col), device(1 - row, col)) for row, col in owners if row == 1]

    def per_device(lower_tri, right_side, grad_out):
        bf16, f32 = jnp.bfloat16, jnp.float32
        dma = pltpu.SemaphoreType.DMA
        block = lambda count: jax.ShapeDtypeStruct((count, BLOCK, BLOCK), bf16)
        hbm = pl.BlockSpec(memory_space=pl.ANY)
        right_here, low, cross = pl.pallas_call(
            kernel,
            out_shape=(jax.ShapeDtypeStruct(grad_out.shape, bf16), block(12), block(RETURNED)),
            in_specs=[hbm] * 3,
            out_specs=[hbm] * 3,
            scratch_shapes=[
                pltpu.VMEM((NUM * BLOCK, COLS), bf16), pltpu.VMEM((NUM * BLOCK, COLS), bf16), pltpu.VMEM((NUM * BLOCK, COLS), bf16),
                pltpu.VMEM((2, 2, 12, BLOCK, BLOCK), bf16),
                pltpu.VMEM((21, BLOCK, BLOCK), f32), pltpu.VMEM((12, BLOCK, BLOCK), f32), pltpu.VMEM((3, BLOCK, BLOCK), f32),
                pltpu.VMEM((12, BLOCK, BLOCK), bf16), pltpu.VMEM((12, BLOCK, BLOCK), bf16),
                pltpu.VMEM((BLOCK, COLS), f32), pltpu.VMEM((BLOCK, COLS), bf16), pltpu.VMEM((2, BLOCK, NUM * BLOCK), bf16),
                dma((NUM,)), dma((NUM,)), dma((COLS // LAST,)), dma((COLS // LAST,)), dma((3,)), dma((3,)), dma((2, NUM)), dma((12,)), dma((3,)), dma((3,)), dma((3,)), dma((3,)),
                dma((2, NUM)), dma((2, NUM)), dma((2, NUM)), dma((2, NUM)), dma((3,)), dma((3,)), dma((3,)), dma((3,)), dma, dma((COLS // LAST,)), dma((5,)),
                pltpu.SemaphoreType.REGULAR, pltpu.SemaphoreType.REGULAR,
            ],
            compiler_params=pltpu.CompilerParams(collective_id=1, has_side_effects=True, vmem_limit_bytes=VMEM_BYTES),
        )(lower_tri, right_side, grad_out)

        grad_right = pl.pallas_call(
            copy_kernel,
            out_shape=jax.ShapeDtypeStruct(grad_out.shape, bf16),
            in_specs=[hbm],
            out_specs=hbm,
            scratch_shapes=[pltpu.VMEM(grad_out.shape, bf16), dma((COPY_PARTS,)), dma((COPY_PARTS,))],
            cost_estimate=pl.CostEstimate(flops=10 ** 10, bytes_accessed=4 * grad_out.size, transcendentals=0),
        )(right_here)
        got = lax.ppermute(cross, ("row", "col"), return_pairs)
        row, col = lax.axis_index("row"), lax.axis_index("col")
        is_back = jnp.logical_and(col % 2 == 1, row == 0)
        swapped = jnp.logical_and(is_back, col // 2 == 1)
        zero = jnp.zeros((BLOCK, BLOCK), bf16)
        got = jnp.where(is_back, got, low[:RETURNED])
        spare = [jnp.where(swapped, zero, got[place]) for place in SPARE]
        moved = [jnp.where(swapped, got[place], low[RETURNED + k]) for k, place in enumerate(SPARE)]
        got, spare, moved = lax.optimization_barrier((got, spare, moved))
        blocks = [spare[0], got[1], got[2], spare[1], got[4], got[5], moved[0], moved[1]] + [low[k] for k in range(8, 12)]
        piece = lambda m, p: blocks[PLACE[m, p]] if p <= m // 2 else zero
        grad_lower = jnp.concatenate([jnp.concatenate([piece(m, p) for p in range(3)], axis=1) for m in range(NUM)], axis=0)
        return grad_right, grad_lower

    return jax.shard_map(per_device, mesh=mesh, in_specs=(block_spec, block_spec, block_spec), out_specs=(block_spec, block_spec), check_vma=False)
```

```python
import jax
import jax.numpy as jnp
from jax import lax
from jax.experimental import pallas as pl
from jax.experimental.pallas import tpu as pltpu
from jax.sharding import PartitionSpec as P

MESH = pl.DeviceIdType.MESH
BLOCK = 256
NUM = 6
COLS = 4096
TILE = 512
LAST = 1024
NEAR = (0, 1)
FAR = (2, 3)
VMEM_BYTES = 67043328
HOP_START = (0, 1, 2, 4, 6, 9)
PLACE = {(1, 0): 0, (2, 0): 1, (3, 0): 2, (3, 1): 3, (4, 0): 4, (4, 1): 5, (5, 0): 6, (5, 1): 7, (5, 2): 8, (0, 0): 9, (2, 1): 10, (4, 2): 11}
RETURNED = 6
SPARE = (0, 3)
RETURNED_FROM = 5
COPY_ENDS = (0, 32, 64, 128, 256, 384, 512, 640, 768, 896, 1024, 1152, 1280, 1408, 1536)
COPY_PARTS = len(COPY_ENDS) - 1


def dot_nt(lhs, rhs):
    return lax.dot_general(lhs, rhs, (((1,), (1,)), ((), ())), preferred_element_type=jnp.float32)


def kernel(lower, right, grad, out_right, out_low, out_cross,
           grad_v, right_v, other_v, lower_v, slot, hop, corner, fin_same, fin_cross, total, stage, turned,
           grad_send, grad_recv, last_send, last_recv, detour_send, detour_recv, load_sem, low_load, low_cross_send, low_cross_recv, low_send, low_recv,
           core_send, core_recv, hop_send, hop_recv, back_send, back_recv, corner_send, corner_recv, out_sem, put_sem, fin_sem, core_free, hop_free):
    row = lax.axis_index("row")
    col = lax.axis_index("col")
    x = col // 2
    owner = (col % 2) == row
    guest = jnp.logical_not(owner)
    to_row = {"row": 1 - row}
    to_core = {"col": col + 1 - 2 * (col % 2)}
    to_chip = {"col": lax.rem(col + 2, 4)}
    to_diag = {"row": 1 - row, "col": col + 1 - 2 * (col % 2)}

    def remote(src, dst, send, recv, where):
        return pltpu.make_async_remote_copy(src_ref=src, dst_ref=dst, send_sem=send, recv_sem=recv, device_id=where, device_id_type=MESH)

    def send_grad(m):
        return remote(grad.at[pl.ds(m * BLOCK, BLOCK)], other_v.at[pl.ds(m * BLOCK, BLOCK)], grad_send.at[m], grad_recv.at[m], to_row)

    def send_last(t):
        cols = pl.ds(t * LAST, LAST)
        return remote(grad.at[pl.ds(0, BLOCK), cols], other_v.at[pl.ds(0, BLOCK), cols], last_send.at[t], last_recv.at[t], to_row)

    def send_right(t):
        cols = pl.ds(t * LAST, LAST)
        return remote(right.at[pl.ds(0, BLOCK), cols], other_v.at[pl.ds(0, BLOCK), cols], last_send.at[t], last_recv.at[t], to_row)

    def load_low(target, p, m):
        return pltpu.make_async_copy(lower.at[pl.ds(m * BLOCK, BLOCK), pl.ds(p * BLOCK, BLOCK)], target.at[PLACE[m, p]], low_load.at[PLACE[m, p]])

    def each_low(target, act):
        for p in range(3):
            for m in range(2 * p, NUM):
                act(load_low(target, p, m))

    def cross_near(count):
        return remote(fin_same.at[pl.ds(0, count)], lower_v.at[x, 1, pl.ds(0, count)], low_cross_send.at[0], low_cross_recv.at[0], to_row)

    def cross_hand():
        return remote(fin_same.at[pl.ds(3, 9)], fin_cross.at[pl.ds(0, 9)], low_cross_send.at[1], low_cross_recv.at[1], to_core)

    def cross_far(first, count):
        return remote(fin_cross.at[pl.ds(first - 3, count)], lower_v.at[x, 1, pl.ds(first, count)], low_cross_send.at[2], low_cross_recv.at[2], to_diag)

    def detour(k):
        source, target, where = (
            (fin_same.at[pl.ds(8, 4)], fin_cross.at[pl.ds(0, 4)], to_chip),
            (fin_cross.at[pl.ds(0, 4)], fin_same.at[pl.ds(0, 4)], to_row),
            (fin_same.at[pl.ds(0, 4)], lower_v.at[0, 1, pl.ds(8, 4)], to_chip))[k]
        return remote(source, target, detour_send.at[k], detour_recv.at[k], where)

    def cross_cases(sender_row, act):
        for case, counts in ((sender_row == 0, (5, 5, 4)),
                             (jnp.logical_and(sender_row == 1, x == 0), (4, 4, 4)),
                             (jnp.logical_and(sender_row == 1, x == 1), (4, 4, 5))):
            @pl.when(case)
            def _(counts=counts):
                act(*counts)

    def send_back(k):
        part = (pl.ds(0, 9), pl.ds(10, 2), pl.ds(RETURNED, 3))[k]
        return remote(fin_cross.at[part], out_low.at[part], back_send.at[k], back_recv.at[k], to_row)

    def send_low(index, half, where):
        return remote(lower_v.at[half], lower_v.at[half], low_send.at[index], low_recv.at[index], where)

    def load(src, dst, m, k):
        return pltpu.make_async_copy(src.at[pl.ds(m * BLOCK, BLOCK)], dst.at[pl.ds(m * BLOCK, BLOCK)], load_sem.at[k, m])

    def put_low(first, count, source):
        return pltpu.make_async_copy(source.at[pl.ds(first, count)], out_low.at[pl.ds(first, count)], fin_sem.at[0])

    def put_zero():
        return pltpu.make_async_copy(fin_cross.at[pl.ds(9, 1)], out_low.at[pl.ds(8, 1)], fin_sem.at[1])

    def put_cross(act):
        def part(first, count, place, k):
            return pltpu.make_async_copy(fin_cross.at[pl.ds(first, count)], out_cross.at[pl.ds(place, count)], fin_sem.at[k])

        @pl.when(x == 0)
        def _():
            act(part(0, RETURNED, 0, 1))

        @pl.when(x == 1)
        def _():
            act(part(RETURNED, 1, 0, 1))
            act(part(1, 2, 1, 2))
            act(part(RETURNED + 1, 1, 3, 3))
            act(part(4, 2, 4, 4))

    def send_core(group, m):
        part = slot.at[pl.ds(m * (m + 1) // 2, m + 1)]
        return remote(part, part, core_send.at[group, m], core_recv.at[group, m], to_core)

    def send_hop(group, m, side):
        base = m * (m + 1) // 2
        first, count = (base + m // 2 + 1, (m + 1) // 2) if side == 0 else (base, m // 2 + 1)
        return remote(slot.at[pl.ds(first, count)], hop.at[pl.ds(HOP_START[m], count)], hop_send.at[group, m], hop_recv.at[group, m], to_chip)

    @pl.when(guest)
    def _():
        fin_cross[9:] = jnp.zeros((3, BLOCK, BLOCK), jnp.bfloat16)

    barrier = pltpu.get_barrier_semaphore()
    for where in (to_diag, to_row, to_chip, to_core):
        pl.semaphore_signal(barrier, inc=1, device_id=where, device_id_type=MESH)
    pl.semaphore_wait(barrier, 4)

    send_grad(NUM - 1).start()

    @pl.when(guest)
    def _():
        each_low(fin_same, lambda copy: copy.start())

    @pl.when(owner)
    def _():
        each_low(lower_v.at[x, 0], lambda copy: copy.start())

    for m in range(NUM):
        load(grad, grad_v, m, 0).start()
        load(right, right_v, m, 1).start()

    @pl.when(guest)
    def _():
        each_low(fin_same, lambda copy: copy.wait())
        cross_hand().start()

        @pl.when(jnp.logical_and(row == 1, x == 0))
        def _():
            detour(0).start()

        cross_cases(row, lambda near, first, far: cross_near(near).start())

        @pl.when(jnp.logical_and(row == 1, x == 1))
        def _():
            detour(0).wait_recv()
            detour(1).start()

    @pl.when(owner)
    def _():
        @pl.when(jnp.logical_or(row == 1, x == 1))
        def _():
            lower_v[x, 1, 9:] = jnp.zeros((3, BLOCK, BLOCK), jnp.bfloat16)

        cross_hand().wait_recv()
        cross_cases(row, lambda near, first, far: cross_far(first, far).start())

    for m in range(NUM - 2, 1, -1):
        send_grad(m).start()

    send_grad(1).start()

    @pl.when(row == 0)
    def _():
        for t in FAR:
            send_right(t).start()

    @pl.when(row == 1)
    def _():
        for t in range(COLS // LAST):
            send_last(t).start()

    @pl.when(jnp.logical_and(guest, row == 0))
    def _():
        put_low(9, 3, fin_cross).start()

        @pl.when(x == 1)
        def _():
            put_zero().start()

    def partial_sums(source, group, m):
        @pl.when(owner)
        def _():
            send_core(group, m).wait_recv()

        def one(n, carry):
            index = m * (m + 1) // 2 + (n % 2) * (m // 2 + 1) + n // 2
            value = dot_nt(source[pl.ds(m * BLOCK, BLOCK), :], right_v[pl.ds(pl.multiple_of(n * BLOCK, BLOCK), BLOCK), :])
            slot[index] = jnp.where(owner, slot[index], 0.0) + value
            return carry

        lax.fori_loop(0, m + 1, one, 0)

        @pl.when(guest)
        def _():
            send_core(group, m).start()

        for side in range(2):
            if side == 1 or m > 0:
                @pl.when(jnp.logical_and(owner, x == side))
                def _(side=side):
                    send_hop(group, m, side).start()

    def finish(group, m):
        for side in range(2):
            @pl.when(jnp.logical_and(owner, x == side))
            def _(side=side):
                if side == 0 or m > 0:
                    send_hop(group, m, 1 - side).wait_recv()
                if side == 1 or m > 0:
                    send_hop(group, m, side).wait_send()
                for p in range(m // 2 + 1):
                    n = 2 * p + side
                    target = fin_cross if group else fin_same
                    if n > m:
                        target[PLACE[m, p]] = jnp.zeros((BLOCK, BLOCK), jnp.bfloat16)
                        continue
                    value = slot[m * (m + 1) // 2 + side * (m // 2 + 1) + p] + hop[HOP_START[m] + p]
                    if n == m and group == 0:
                        rows = lax.broadcasted_iota(jnp.int32, (BLOCK, BLOCK), 0)
                        cols = lax.broadcasted_iota(jnp.int32, (BLOCK, BLOCK), 1)
                        value = jnp.where(rows >= cols, value, 0.0)
                    if n == m and group == 1:
                        value = jnp.where(row == 0, value, 0.0)
                    target[PLACE[m, p]] = value.astype(jnp.bfloat16)

    for m in range(NUM):
        load(grad, grad_v, m, 0).wait()
        load(right, right_v, m, 1).wait()
        partial_sums(grad_v, 0, m)

    @pl.when(owner)
    def _():
        each_low(lower_v.at[x, 0], lambda copy: copy.wait())
        def arrived(near, first, far):
            cross_near(near).wait_recv()
            cross_far(first, far).wait_recv()

        cross_cases(1 - row, arrived)

        @pl.when(jnp.logical_and(row == 0, x == 1))
        def _():
            detour(1).wait_recv()
            detour(2).start()
            detour(2).wait_send()

        @pl.when(jnp.logical_and(row == 0, x == 0))
        def _():
            detour(2).wait_recv()

        send_low(0, x, to_chip).start()
        send_low(1, x, to_core).start()

    for m in range(NUM):
        finish(0, m)

    @pl.when(owner)
    def _():
        pl.semaphore_signal(core_free, inc=1, device_id=to_core, device_id_type=MESH)
        pl.semaphore_signal(hop_free, inc=1, device_id=to_chip, device_id_type=MESH)
        send_low(0, 1 - x, to_chip).wait_recv()
        send_low(2, 1 - x, to_core).start()
        pl.semaphore_wait(hop_free, 1)
        put_low(0, 12, fin_same).start()

        cross_cases(row, lambda near, first, far: cross_far(first, far).wait_send())

    @pl.when(guest)
    def _():
        send_low(1, x, to_core).wait_recv()
        send_low(2, 1 - x, to_core).wait_recv()
        for m in range(NUM):
            send_core(0, m).wait_send()
        pl.semaphore_wait(core_free, 1)

    def turn(n):
        p, half = n // 2, n % 2
        for parity in range(2):
            for m in range(n, NUM):
                turned[parity, :, pl.ds((m - n) * BLOCK, BLOCK)] = lower_v[half, parity, PLACE[m, p]].T

    def put(n):
        return pltpu.make_async_copy(stage, out_right.at[pl.ds(n * BLOCK, BLOCK)], out_sem)

    def tiles(body):
        def one(t, carry):
            body(pl.ds(pl.multiple_of(t * TILE, TILE), TILE))
            return carry
        lax.fori_loop(0, COLS // TILE, one, 0)

    first_core = (col % 2) == 0

    def corner_core():
        return remote(slot.at[0], corner.at[0], corner_send.at[0], corner_recv.at[0], to_core)

    def corner_chip():
        return remote(slot.at[0], corner.at[1], corner_send.at[1], corner_recv.at[1], to_chip)

    def corner_row():
        return remote(slot.at[0], corner.at[2], corner_send.at[2], corner_recv.at[2], to_row)

    def corner_start(grads, rights, pieces):
        for t in pieces:
            cols = pl.ds(t * LAST, LAST)
            value = dot_nt(grads[:BLOCK, cols], rights[:BLOCK, cols])
            slot[0] = value if t == pieces[0] else slot[0] + value

        @pl.when(jnp.logical_not(first_core))
        def _():
            corner_core().start()

        @pl.when(first_core)
        def _():
            corner_core().wait_recv()
            slot[0] = slot[0] + corner[0]

            @pl.when(x == 1)
            def _():
                corner_chip().start()

    def corner_end():
        @pl.when(jnp.logical_not(first_core))
        def _():
            corner_core().wait_send()

        @pl.when(jnp.logical_and(first_core, x == 1))
        def _():
            corner_chip().wait_send()

    for m in range(NUM - 1, 0, -1):
        send_grad(m).wait_recv()
        partial_sums(other_v, 1, m)
        turn(m)
        if m < NUM - 1:
            put(m + 1).wait()
        depth = (NUM - m) * BLOCK

        def product(cols, m=m, depth=depth):
            value = jnp.dot(turned[0, :, :depth], grad_v[m * BLOCK:, cols], preferred_element_type=jnp.float32)
            value += jnp.dot(turned[1, :, :depth], other_v[m * BLOCK:, cols], preferred_element_type=jnp.float32)
            stage[:, cols] = value.astype(jnp.bfloat16)

        tiles(product)
        put(m).start()
        if m < NUM - 1:
            finish(1, m + 1)
        if m + 1 == RETURNED_FROM:
            @pl.when(jnp.logical_and(owner, jnp.logical_and(row == 1, x == 0)))
            def _():
                send_back(2).start()

    turn(0)

    def all_but_last(cols):
        value = jnp.dot(turned[0], grad_v[:, cols], preferred_element_type=jnp.float32)
        total[:, cols] = value + jnp.dot(turned[1, :, BLOCK:], other_v[BLOCK:, cols], preferred_element_type=jnp.float32)

    tiles(all_but_last)
    finish(1, 1)

    @pl.when(jnp.logical_and(owner, row == 0))
    def _():
        send_back(0).start()
        send_back(1).start()

    @pl.when(jnp.logical_and(owner, row == 1))
    def _():
        put_cross(lambda copy: copy.start())

    put(1).wait()

    def put_last(t):
        cols = pl.ds(t * LAST, LAST)
        return pltpu.make_async_copy(stage.at[:, cols], out_right.at[pl.ds(0, BLOCK), cols], put_sem.at[t])

    @pl.when(row == 0)
    def _():
        for t in range(COLS // LAST):
            cols = pl.ds(t * LAST, LAST)
            send_last(t).wait_recv()
            value = jnp.dot(turned[1, :, :BLOCK], other_v[:BLOCK, cols], preferred_element_type=jnp.float32)
            stage[:, cols] = (total[:, cols] + value).astype(jnp.bfloat16)
            put_last(t).start()
            if t == NEAR[-1]:
                corner_start(other_v, right_v, NEAR)

            if t == NEAR[-1] + 1:
                @pl.when(jnp.logical_and(first_core, x == 0))
                def _():
                    corner_chip().wait_recv()
                    slot[0] = slot[0] + corner[1]
                    corner_row().start()

        corner_end()

        @pl.when(jnp.logical_and(first_core, x == 0))
        def _():
            corner_row().wait_send()

    @pl.when(row == 1)
    def _():
        for t in range(COLS // LAST):
            cols = pl.ds(t * LAST, LAST)
            stage[:, cols] = total[:, cols].astype(jnp.bfloat16)
            put_last(t).start()
        for t in FAR:
            send_right(t).wait_recv()
        corner_start(grad_v, other_v, FAR)
        corner_end()

        @pl.when(jnp.logical_and(first_core, x == 0))
        def _():
            corner_chip().wait_recv()
            corner_row().wait_recv()
            fin_cross[9] = (slot[0] + corner[1] + corner[2]).astype(jnp.bfloat16)


    @pl.when(guest)
    def _():
        @pl.when(row == 0)
        def _():
            put_low(9, 3, fin_cross).wait()

            @pl.when(x == 0)
            def _():
                send_back(2).wait_recv()

            @pl.when(x == 1)
            def _():
                put_zero().wait()

        @pl.when(row == 1)
        def _():
            put_low(9, 1, fin_cross).start()
            put_low(9, 1, fin_cross).wait()
            send_back(0).wait_recv()
            send_back(1).wait_recv()

        cross_hand().wait_send()
        cross_cases(row, lambda near, first, far: cross_near(near).wait_send())

        @pl.when(jnp.logical_and(row == 1, x == 0))
        def _():
            detour(0).wait_send()

        @pl.when(jnp.logical_and(row == 1, x == 1))
        def _():
            detour(1).wait_send()

        for m in range(1, NUM):
            send_core(1, m).wait_send()

    @pl.when(owner)
    def _():
        put_low(0, 12, fin_same).wait()
        send_low(0, x, to_chip).wait_send()
        send_low(1, x, to_core).wait_send()
        send_low(2, 1 - x, to_core).wait_send()

        @pl.when(row == 0)
        def _():
            send_back(0).wait_send()
            send_back(1).wait_send()

        @pl.when(row == 1)
        def _():
            put_cross(lambda copy: copy.wait())

            @pl.when(x == 0)
            def _():
                send_back(2).wait_send()

    for t in range(COLS // LAST):
        put_last(t).wait()
    for m in range(NUM - 1, 0, -1):
        send_grad(m).wait_send()

    @pl.when(row == 0)
    def _():
        for t in FAR:
            send_right(t).wait_send()

    @pl.when(row == 1)
    def _():
        for t in range(COLS // LAST):
            send_last(t).wait_send()


def copy_kernel(source, target, buffer, read_sem, write_sem):
    part = lambda ref, k: ref.at[pl.ds(COPY_ENDS[k], COPY_ENDS[k + 1] - COPY_ENDS[k])]
    reads = [pltpu.make_async_copy(part(source, k), part(buffer, k), read_sem.at[k]) for k in range(COPY_PARTS)]
    writes = [pltpu.make_async_copy(part(buffer, k), part(target, k), write_sem.at[k]) for k in range(COPY_PARTS)]
    for read in reads:
        read.start()
    for read, write in zip(reads, writes):
        read.wait()
        write.start()
    for write in writes:
        write.wait()


def solution(mesh):
    block_spec = P(("batch", "row"), "col")
    device = lambda row, col: row * 4 + col
    owners = [(row, 2 * chip + row) for row in range(2) for chip in range(2)]
    return_pairs = [(device(row, col), device(1 - row, col)) for row, col in owners if row == 1]

    def per_device(lower_tri, right_side, grad_out):
        bf16, f32 = jnp.bfloat16, jnp.float32
        dma = pltpu.SemaphoreType.DMA
        block = lambda count: jax.ShapeDtypeStruct((count, BLOCK, BLOCK), bf16)
        hbm = pl.BlockSpec(memory_space=pl.ANY)
        right_here, low, cross = pl.pallas_call(
            kernel,
            out_shape=(jax.ShapeDtypeStruct(grad_out.shape, bf16), block(12), block(RETURNED)),
            in_specs=[hbm] * 3,
            out_specs=[hbm] * 3,
            scratch_shapes=[
                pltpu.VMEM((NUM * BLOCK, COLS), bf16), pltpu.VMEM((NUM * BLOCK, COLS), bf16), pltpu.VMEM((NUM * BLOCK, COLS), bf16),
                pltpu.VMEM((2, 2, 12, BLOCK, BLOCK), bf16),
                pltpu.VMEM((21, BLOCK, BLOCK), f32), pltpu.VMEM((12, BLOCK, BLOCK), f32), pltpu.VMEM((3, BLOCK, BLOCK), f32),
                pltpu.VMEM((12, BLOCK, BLOCK), bf16), pltpu.VMEM((12, BLOCK, BLOCK), bf16),
                pltpu.VMEM((BLOCK, COLS), f32), pltpu.VMEM((BLOCK, COLS), bf16), pltpu.VMEM((2, BLOCK, NUM * BLOCK), bf16),
                dma((NUM,)), dma((NUM,)), dma((COLS // LAST,)), dma((COLS // LAST,)), dma((3,)), dma((3,)), dma((2, NUM)), dma((12,)), dma((3,)), dma((3,)), dma((3,)), dma((3,)),
                dma((2, NUM)), dma((2, NUM)), dma((2, NUM)), dma((2, NUM)), dma((3,)), dma((3,)), dma((3,)), dma((3,)), dma, dma((COLS // LAST,)), dma((5,)),
                pltpu.SemaphoreType.REGULAR, pltpu.SemaphoreType.REGULAR,
            ],
            compiler_params=pltpu.CompilerParams(collective_id=1, has_side_effects=True, vmem_limit_bytes=VMEM_BYTES),
        )(lower_tri, right_side, grad_out)

        grad_right = pl.pallas_call(
            copy_kernel,
            out_shape=jax.ShapeDtypeStruct(grad_out.shape, bf16),
            in_specs=[hbm],
            out_specs=hbm,
            scratch_shapes=[pltpu.VMEM(grad_out.shape, bf16), dma((COPY_PARTS,)), dma((COPY_PARTS,))],
            cost_estimate=pl.CostEstimate(flops=10 ** 10, bytes_accessed=4 * grad_out.size, transcendentals=0),
        )(right_here)
        got = lax.ppermute(cross, ("row", "col"), return_pairs)
        row, col = lax.axis_index("row"), lax.axis_index("col")
        is_back = jnp.logical_and(col % 2 == 1, row == 0)
        swapped = jnp.logical_and(is_back, col // 2 == 1)
        zero = jnp.zeros((BLOCK, BLOCK), bf16)
        got = jnp.where(is_back, got, low[:RETURNED])
        spare = [jnp.where(swapped, zero, got[place]) for place in SPARE]
        moved = [jnp.where(swapped, got[place], low[RETURNED + k]) for k, place in enumerate(SPARE)]
        got, spare, moved = lax.optimization_barrier((got, spare, moved))
        blocks = [spare[0], got[1], got[2], spare[1], got[4], got[5], moved[0], moved[1]] + [low[k] for k in range(8, 12)]
        piece = lambda m, p: blocks[PLACE[m, p]] if p <= m // 2 else zero
        grad_lower = jnp.concatenate([jnp.concatenate([piece(m, p) for p in range(3)], axis=1) for m in range(NUM)], axis=0)
        return grad_right, grad_lower

    return jax.shard_map(per_device, mesh=mesh, in_specs=(block_spec, block_spec, block_spec), out_specs=(block_spec, block_spec), check_vma=False)
```

```python
import jax
import jax.numpy as jnp
from jax import lax
from jax.experimental import pallas as pl
from jax.experimental.pallas import tpu as pltpu
from jax.sharding import PartitionSpec as P

MESH = pl.DeviceIdType.MESH
BLOCK = 256
NUM = 6
COLS = 4096
TILE = 512
LAST = 512
NEAR = (0, 1, 2, 3)
FAR = (4, 5, 6, 7)
VMEM_BYTES = 67043328
HOP_START = (0, 1, 2, 4, 6, 9)
PLACE = {(1, 0): 0, (2, 0): 1, (3, 0): 2, (3, 1): 3, (4, 0): 4, (4, 1): 5, (5, 0): 6, (5, 1): 7, (5, 2): 8, (0, 0): 9, (2, 1): 10, (4, 2): 11}
RETURNED = 6
SPARE = (0, 3)
RETURNED_FROM = 5
COPY_ENDS = (0, 32, 64, 128, 256, 384, 512, 640, 768, 896, 1024, 1152, 1280, 1408, 1536)
COPY_PARTS = len(COPY_ENDS) - 1


def dot_nt(lhs, rhs):
    return lax.dot_general(lhs, rhs, (((1,), (1,)), ((), ())), preferred_element_type=jnp.float32)


def kernel(lower, right, grad, out_right, out_low, out_cross,
           grad_v, right_v, other_v, lower_v, slot, hop, corner, fin_same, fin_cross, total, stage, turned,
           grad_send, grad_recv, last_send, last_recv, detour_send, detour_recv, load_sem, low_load, low_cross_send, low_cross_recv, low_send, low_recv,
           core_send, core_recv, hop_send, hop_recv, back_send, back_recv, corner_send, corner_recv, out_sem, put_sem, fin_sem, core_free, hop_free):
    row = lax.axis_index("row")
    col = lax.axis_index("col")
    x = col // 2
    owner = (col % 2) == row
    guest = jnp.logical_not(owner)
    to_row = {"row": 1 - row}
    to_core = {"col": col + 1 - 2 * (col % 2)}
    to_chip = {"col": lax.rem(col + 2, 4)}
    to_diag = {"row": 1 - row, "col": col + 1 - 2 * (col % 2)}

    def remote(src, dst, send, recv, where):
        return pltpu.make_async_remote_copy(src_ref=src, dst_ref=dst, send_sem=send, recv_sem=recv, device_id=where, device_id_type=MESH)

    def send_grad(m):
        return remote(grad.at[pl.ds(m * BLOCK, BLOCK)], other_v.at[pl.ds(m * BLOCK, BLOCK)], grad_send.at[m], grad_recv.at[m], to_row)

    def send_last(t):
        cols = pl.ds(t * LAST, LAST)
        return remote(grad.at[pl.ds(0, BLOCK), cols], other_v.at[pl.ds(0, BLOCK), cols], last_send.at[t], last_recv.at[t], to_row)

    def send_right(t):
        cols = pl.ds(t * LAST, LAST)
        return remote(right.at[pl.ds(0, BLOCK), cols], other_v.at[pl.ds(0, BLOCK), cols], last_send.at[t], last_recv.at[t], to_row)

    def load_low(target, p, m):
        return pltpu.make_async_copy(lower.at[pl.ds(m * BLOCK, BLOCK), pl.ds(p * BLOCK, BLOCK)], target.at[PLACE[m, p]], low_load.at[PLACE[m, p]])

    def each_low(target, act):
        for p in range(3):
            for m in range(2 * p, NUM):
                act(load_low(target, p, m))

    def cross_near(count):
        return remote(fin_same.at[pl.ds(0, count)], lower_v.at[x, 1, pl.ds(0, count)], low_cross_send.at[0], low_cross_recv.at[0], to_row)

    def cross_hand():
        return remote(fin_same.at[pl.ds(3, 9)], fin_cross.at[pl.ds(0, 9)], low_cross_send.at[1], low_cross_recv.at[1], to_core)

    def cross_far(first, count):
        return remote(fin_cross.at[pl.ds(first - 3, count)], lower_v.at[x, 1, pl.ds(first, count)], low_cross_send.at[2], low_cross_recv.at[2], to_diag)

    def detour(k):
        source, target, where = (
            (fin_same.at[pl.ds(8, 4)], fin_cross.at[pl.ds(0, 4)], to_chip),
            (fin_cross.at[pl.ds(0, 4)], fin_same.at[pl.ds(0, 4)], to_row),
            (fin_same.at[pl.ds(0, 4)], lower_v.at[0, 1, pl.ds(8, 4)], to_chip))[k]
        return remote(source, target, detour_send.at[k], detour_recv.at[k], where)

    def cross_cases(sender_row, act):
        for case, counts in ((sender_row == 0, (5, 5, 4)),
                             (jnp.logical_and(sender_row == 1, x == 0), (4, 4, 4)),
                             (jnp.logical_and(sender_row == 1, x == 1), (4, 4, 5))):
            @pl.when(case)
            def _(counts=counts):
                act(*counts)

    def send_back(k):
        part = (pl.ds(0, 9), pl.ds(10, 2), pl.ds(RETURNED, 3))[k]
        return remote(fin_cross.at[part], out_low.at[part], back_send.at[k], back_recv.at[k], to_row)

    def send_low(index, half, where):
        return remote(lower_v.at[half], lower_v.at[half], low_send.at[index], low_recv.at[index], where)

    def load(src, dst, m, k):
        return pltpu.make_async_copy(src.at[pl.ds(m * BLOCK, BLOCK)], dst.at[pl.ds(m * BLOCK, BLOCK)], load_sem.at[k, m])

    def put_low(first, count, source):
        return pltpu.make_async_copy(source.at[pl.ds(first, count)], out_low.at[pl.ds(first, count)], fin_sem.at[0])

    def put_zero():
        return pltpu.make_async_copy(fin_cross.at[pl.ds(9, 1)], out_low.at[pl.ds(8, 1)], fin_sem.at[1])

    def put_cross(act):
        def part(first, count, place, k):
            return pltpu.make_async_copy(fin_cross.at[pl.ds(first, count)], out_cross.at[pl.ds(place, count)], fin_sem.at[k])

        @pl.when(x == 0)
        def _():
            act(part(0, RETURNED, 0, 1))

        @pl.when(x == 1)
        def _():
            act(part(RETURNED, 1, 0, 1))
            act(part(1, 2, 1, 2))
            act(part(RETURNED + 1, 1, 3, 3))
            act(part(4, 2, 4, 4))

    def send_core(group, m):
        part = slot.at[pl.ds(m * (m + 1) // 2, m + 1)]
        return remote(part, part, core_send.at[group, m], core_recv.at[group, m], to_core)

    def send_hop(group, m, side):
        base = m * (m + 1) // 2
        first, count = (base + m // 2 + 1, (m + 1) // 2) if side == 0 else (base, m // 2 + 1)
        return remote(slot.at[pl.ds(first, count)], hop.at[pl.ds(HOP_START[m], count)], hop_send.at[group, m], hop_recv.at[group, m], to_chip)

    @pl.when(guest)
    def _():
        fin_cross[9:] = jnp.zeros((3, BLOCK, BLOCK), jnp.bfloat16)

    barrier = pltpu.get_barrier_semaphore()
    for where in (to_diag, to_row, to_chip, to_core):
        pl.semaphore_signal(barrier, inc=1, device_id=where, device_id_type=MESH)
    pl.semaphore_wait(barrier, 4)

    send_grad(NUM - 1).start()

    @pl.when(guest)
    def _():
        each_low(fin_same, lambda copy: copy.start())

    @pl.when(owner)
    def _():
        each_low(lower_v.at[x, 0], lambda copy: copy.start())

    for m in range(NUM):
        load(grad, grad_v, m, 0).start()
        load(right, right_v, m, 1).start()

    @pl.when(guest)
    def _():
        each_low(fin_same, lambda copy: copy.wait())
        cross_hand().start()

        @pl.when(jnp.logical_and(row == 1, x == 0))
        def _():
            detour(0).start()

        cross_cases(row, lambda near, first, far: cross_near(near).start())

        @pl.when(jnp.logical_and(row == 1, x == 1))
        def _():
            detour(0).wait_recv()
            detour(1).start()

    @pl.when(owner)
    def _():
        @pl.when(jnp.logical_or(row == 1, x == 1))
        def _():
            lower_v[x, 1, 9:] = jnp.zeros((3, BLOCK, BLOCK), jnp.bfloat16)

        cross_hand().wait_recv()
        cross_cases(row, lambda near, first, far: cross_far(first, far).start())

    for m in range(NUM - 2, 1, -1):
        send_grad(m).start()

    send_grad(1).start()

    @pl.when(row == 0)
    def _():
        for t in FAR:
            send_right(t).start()

    @pl.when(row == 1)
    def _():
        for t in range(COLS // LAST):
            send_last(t).start()

    @pl.when(jnp.logical_and(guest, row == 0))
    def _():
        put_low(9, 3, fin_cross).start()

        @pl.when(x == 1)
        def _():
            put_zero().start()

    def partial_sums(source, group, m):
        @pl.when(owner)
        def _():
            send_core(group, m).wait_recv()

        def one(n, carry):
            index = m * (m + 1) // 2 + (n % 2) * (m // 2 + 1) + n // 2
            value = dot_nt(source[pl.ds(m * BLOCK, BLOCK), :], right_v[pl.ds(pl.multiple_of(n * BLOCK, BLOCK), BLOCK), :])
            slot[index] = jnp.where(owner, slot[index], 0.0) + value
            return carry

        lax.fori_loop(0, m + 1, one, 0)

        @pl.when(guest)
        def _():
            send_core(group, m).start()

        for side in range(2):
            if side == 1 or m > 0:
                @pl.when(jnp.logical_and(owner, x == side))
                def _(side=side):
                    send_hop(group, m, side).start()

    def finish(group, m):
        for side in range(2):
            @pl.when(jnp.logical_and(owner, x == side))
            def _(side=side):
                if side == 0 or m > 0:
                    send_hop(group, m, 1 - side).wait_recv()
                if side == 1 or m > 0:
                    send_hop(group, m, side).wait_send()
                for p in range(m // 2 + 1):
                    n = 2 * p + side
                    target = fin_cross if group else fin_same
                    if n > m:
                        target[PLACE[m, p]] = jnp.zeros((BLOCK, BLOCK), jnp.bfloat16)
                        continue
                    value = slot[m * (m + 1) // 2 + side * (m // 2 + 1) + p] + hop[HOP_START[m] + p]
                    if n == m and group == 0:
                        rows = lax.broadcasted_iota(jnp.int32, (BLOCK, BLOCK), 0)
                        cols = lax.broadcasted_iota(jnp.int32, (BLOCK, BLOCK), 1)
                        value = jnp.where(rows >= cols, value, 0.0)
                    if n == m and group == 1:
                        value = jnp.where(row == 0, value, 0.0)
                    target[PLACE[m, p]] = value.astype(jnp.bfloat16)

    for m in range(NUM):
        load(grad, grad_v, m, 0).wait()
        load(right, right_v, m, 1).wait()
        partial_sums(grad_v, 0, m)

    @pl.when(owner)
    def _():
        each_low(lower_v.at[x, 0], lambda copy: copy.wait())
        def arrived(near, first, far):
            cross_near(near).wait_recv()
            cross_far(first, far).wait_recv()

        cross_cases(1 - row, arrived)

        @pl.when(jnp.logical_and(row == 0, x == 1))
        def _():
            detour(1).wait_recv()
            detour(2).start()
            detour(2).wait_send()

        @pl.when(jnp.logical_and(row == 0, x == 0))
        def _():
            detour(2).wait_recv()

        send_low(0, x, to_chip).start()
        send_low(1, x, to_core).start()

    for m in range(NUM):
        finish(0, m)

    @pl.when(owner)
    def _():
        pl.semaphore_signal(core_free, inc=1, device_id=to_core, device_id_type=MESH)
        pl.semaphore_signal(hop_free, inc=1, device_id=to_chip, device_id_type=MESH)
        send_low(0, 1 - x, to_chip).wait_recv()
        send_low(2, 1 - x, to_core).start()
        pl.semaphore_wait(hop_free, 1)
        put_low(0, 12, fin_same).start()

        cross_cases(row, lambda near, first, far: cross_far(first, far).wait_send())

    @pl.when(guest)
    def _():
        send_low(1, x, to_core).wait_recv()
        send_low(2, 1 - x, to_core).wait_recv()
        for m in range(NUM):
            send_core(0, m).wait_send()
        pl.semaphore_wait(core_free, 1)

    def turn(n):
        p, half = n // 2, n % 2
        for parity in range(2):
            for m in range(n, NUM):
                turned[parity, :, pl.ds((m - n) * BLOCK, BLOCK)] = lower_v[half, parity, PLACE[m, p]].T

    def put(n):
        return pltpu.make_async_copy(stage, out_right.at[pl.ds(n * BLOCK, BLOCK)], out_sem)

    def tiles(body):
        def one(t, carry):
            body(pl.ds(pl.multiple_of(t * TILE, TILE), TILE))
            return carry
        lax.fori_loop(0, COLS // TILE, one, 0)

    first_core = (col % 2) == 0

    def corner_core():
        return remote(slot.at[0], corner.at[0], corner_send.at[0], corner_recv.at[0], to_core)

    def corner_chip():
        return remote(slot.at[0], corner.at[1], corner_send.at[1], corner_recv.at[1], to_chip)

    def corner_row():
        return remote(slot.at[0], corner.at[2], corner_send.at[2], corner_recv.at[2], to_row)

    def corner_start(grads, rights, pieces):
        for t in pieces:
            cols = pl.ds(t * LAST, LAST)
            value = dot_nt(grads[:BLOCK, cols], rights[:BLOCK, cols])
            slot[0] = value if t == pieces[0] else slot[0] + value

        @pl.when(jnp.logical_not(first_core))
        def _():
            corner_core().start()

        @pl.when(first_core)
        def _():
            corner_core().wait_recv()
            slot[0] = slot[0] + corner[0]

            @pl.when(x == 1)
            def _():
                corner_chip().start()

    def corner_end():
        @pl.when(jnp.logical_not(first_core))
        def _():
            corner_core().wait_send()

        @pl.when(jnp.logical_and(first_core, x == 1))
        def _():
            corner_chip().wait_send()

    for m in range(NUM - 1, 0, -1):
        send_grad(m).wait_recv()
        partial_sums(other_v, 1, m)
        turn(m)
        if m < NUM - 1:
            put(m + 1).wait()
        depth = (NUM - m) * BLOCK

        def product(cols, m=m, depth=depth):
            value = jnp.dot(turned[0, :, :depth], grad_v[m * BLOCK:, cols], preferred_element_type=jnp.float32)
            value += jnp.dot(turned[1, :, :depth], other_v[m * BLOCK:, cols], preferred_element_type=jnp.float32)
            stage[:, cols] = value.astype(jnp.bfloat16)

        tiles(product)
        put(m).start()
        if m < NUM - 1:
            finish(1, m + 1)
        if m + 1 == RETURNED_FROM:
            @pl.when(jnp.logical_and(owner, jnp.logical_and(row == 1, x == 0)))
            def _():
                send_back(2).start()

    turn(0)

    def all_but_last(cols):
        value = jnp.dot(turned[0], grad_v[:, cols], preferred_element_type=jnp.float32)
        total[:, cols] = value + jnp.dot(turned[1, :, BLOCK:], other_v[BLOCK:, cols], preferred_element_type=jnp.float32)

    tiles(all_but_last)
    finish(1, 1)

    @pl.when(jnp.logical_and(owner, row == 0))
    def _():
        send_back(0).start()
        send_back(1).start()

    @pl.when(jnp.logical_and(owner, row == 1))
    def _():
        put_cross(lambda copy: copy.start())

    put(1).wait()

    def put_last(t):
        cols = pl.ds(t * LAST, LAST)
        return pltpu.make_async_copy(stage.at[:, cols], out_right.at[pl.ds(0, BLOCK), cols], put_sem.at[t])

    @pl.when(row == 0)
    def _():
        for t in range(COLS // LAST):
            cols = pl.ds(t * LAST, LAST)
            send_last(t).wait_recv()
            value = jnp.dot(turned[1, :, :BLOCK], other_v[:BLOCK, cols], preferred_element_type=jnp.float32)
            stage[:, cols] = (total[:, cols] + value).astype(jnp.bfloat16)
            put_last(t).start()
            if t == NEAR[-1]:
                corner_start(other_v, right_v, NEAR)

            if t == NEAR[-1] + 1:
                @pl.when(jnp.logical_and(first_core, x == 0))
                def _():
                    corner_chip().wait_recv()
                    slot[0] = slot[0] + corner[1]
                    corner_row().start()

        corner_end()

        @pl.when(jnp.logical_and(first_core, x == 0))
        def _():
            corner_row().wait_send()

    @pl.when(row == 1)
    def _():
        for t in range(COLS // LAST):
            cols = pl.ds(t * LAST, LAST)
            stage[:, cols] = total[:, cols].astype(jnp.bfloat16)
            put_last(t).start()
        for t in FAR:
            send_right(t).wait_recv()
        corner_start(grad_v, other_v, FAR)
        corner_end()

        @pl.when(jnp.logical_and(first_core, x == 0))
        def _():
            corner_chip().wait_recv()
            corner_row().wait_recv()
            fin_cross[9] = (slot[0] + corner[1] + corner[2]).astype(jnp.bfloat16)


    @pl.when(guest)
    def _():
        @pl.when(row == 0)
        def _():
            put_low(9, 3, fin_cross).wait()

            @pl.when(x == 0)
            def _():
                send_back(2).wait_recv()

            @pl.when(x == 1)
            def _():
                put_zero().wait()

        @pl.when(row == 1)
        def _():
            put_low(9, 1, fin_cross).start()
            put_low(9, 1, fin_cross).wait()
            send_back(0).wait_recv()
            send_back(1).wait_recv()

        cross_hand().wait_send()
        cross_cases(row, lambda near, first, far: cross_near(near).wait_send())

        @pl.when(jnp.logical_and(row == 1, x == 0))
        def _():
            detour(0).wait_send()

        @pl.when(jnp.logical_and(row == 1, x == 1))
        def _():
            detour(1).wait_send()

        for m in range(1, NUM):
            send_core(1, m).wait_send()

    @pl.when(owner)
    def _():
        put_low(0, 12, fin_same).wait()
        send_low(0, x, to_chip).wait_send()
        send_low(1, x, to_core).wait_send()
        send_low(2, 1 - x, to_core).wait_send()

        @pl.when(row == 0)
        def _():
            send_back(0).wait_send()
            send_back(1).wait_send()

        @pl.when(row == 1)
        def _():
            put_cross(lambda copy: copy.wait())

            @pl.when(x == 0)
            def _():
                send_back(2).wait_send()

    for t in range(COLS // LAST):
        put_last(t).wait()
    for m in range(NUM - 1, 0, -1):
        send_grad(m).wait_send()

    @pl.when(row == 0)
    def _():
        for t in FAR:
            send_right(t).wait_send()

    @pl.when(row == 1)
    def _():
        for t in range(COLS // LAST):
            send_last(t).wait_send()


def copy_kernel(source, target, buffer, read_sem, write_sem):
    part = lambda ref, k: ref.at[pl.ds(COPY_ENDS[k], COPY_ENDS[k + 1] - COPY_ENDS[k])]
    reads = [pltpu.make_async_copy(part(source, k), part(buffer, k), read_sem.at[k]) for k in range(COPY_PARTS)]
    writes = [pltpu.make_async_copy(part(buffer, k), part(target, k), write_sem.at[k]) for k in range(COPY_PARTS)]
    for read in reads:
        read.start()
    for read, write in zip(reads, writes):
        read.wait()
        write.start()
    for write in writes:
        write.wait()


def solution(mesh):
    block_spec = P(("batch", "row"), "col")
    device = lambda row, col: row * 4 + col
    owners = [(row, 2 * chip + row) for row in range(2) for chip in range(2)]
    return_pairs = [(device(row, col), device(1 - row, col)) for row, col in owners if row == 1]

    def per_device(lower_tri, right_side, grad_out):
        bf16, f32 = jnp.bfloat16, jnp.float32
        dma = pltpu.SemaphoreType.DMA
        block = lambda count: jax.ShapeDtypeStruct((count, BLOCK, BLOCK), bf16)
        hbm = pl.BlockSpec(memory_space=pl.ANY)
        right_here, low, cross = pl.pallas_call(
            kernel,
            out_shape=(jax.ShapeDtypeStruct(grad_out.shape, bf16), block(12), block(RETURNED)),
            in_specs=[hbm] * 3,
            out_specs=[hbm] * 3,
            scratch_shapes=[
                pltpu.VMEM((NUM * BLOCK, COLS), bf16), pltpu.VMEM((NUM * BLOCK, COLS), bf16), pltpu.VMEM((NUM * BLOCK, COLS), bf16),
                pltpu.VMEM((2, 2, 12, BLOCK, BLOCK), bf16),
                pltpu.VMEM((21, BLOCK, BLOCK), f32), pltpu.VMEM((12, BLOCK, BLOCK), f32), pltpu.VMEM((3, BLOCK, BLOCK), f32),
                pltpu.VMEM((12, BLOCK, BLOCK), bf16), pltpu.VMEM((12, BLOCK, BLOCK), bf16),
                pltpu.VMEM((BLOCK, COLS), f32), pltpu.VMEM((BLOCK, COLS), bf16), pltpu.VMEM((2, BLOCK, NUM * BLOCK), bf16),
                dma((NUM,)), dma((NUM,)), dma((COLS // LAST,)), dma((COLS // LAST,)), dma((3,)), dma((3,)), dma((2, NUM)), dma((12,)), dma((3,)), dma((3,)), dma((3,)), dma((3,)),
                dma((2, NUM)), dma((2, NUM)), dma((2, NUM)), dma((2, NUM)), dma((3,)), dma((3,)), dma((3,)), dma((3,)), dma, dma((COLS // LAST,)), dma((5,)),
                pltpu.SemaphoreType.REGULAR, pltpu.SemaphoreType.REGULAR,
            ],
            compiler_params=pltpu.CompilerParams(collective_id=1, has_side_effects=True, vmem_limit_bytes=VMEM_BYTES),
        )(lower_tri, right_side, grad_out)

        grad_right = pl.pallas_call(
            copy_kernel,
            out_shape=jax.ShapeDtypeStruct(grad_out.shape, bf16),
            in_specs=[hbm],
            out_specs=hbm,
            scratch_shapes=[pltpu.VMEM(grad_out.shape, bf16), dma((COPY_PARTS,)), dma((COPY_PARTS,))],
            cost_estimate=pl.CostEstimate(flops=10 ** 10, bytes_accessed=4 * grad_out.size, transcendentals=0),
        )(right_here)
        got = lax.ppermute(cross, ("row", "col"), return_pairs)
        row, col = lax.axis_index("row"), lax.axis_index("col")
        is_back = jnp.logical_and(col % 2 == 1, row == 0)
        swapped = jnp.logical_and(is_back, col // 2 == 1)
        zero = jnp.zeros((BLOCK, BLOCK), bf16)
        got = jnp.where(is_back, got, low[:RETURNED])
        spare = [jnp.where(swapped, zero, got[place]) for place in SPARE]
        moved = [jnp.where(swapped, got[place], low[RETURNED + k]) for k, place in enumerate(SPARE)]
        got, spare, moved = lax.optimization_barrier((got, spare, moved))
        blocks = [spare[0], got[1], got[2], spare[1], got[4], got[5], moved[0], moved[1]] + [low[k] for k in range(8, 12)]
        piece = lambda m, p: blocks[PLACE[m, p]] if p <= m // 2 else zero
        grad_lower = jnp.concatenate([jnp.concatenate([piece(m, p) for p in range(3)], axis=1) for m in range(NUM)], axis=0)
        return grad_right, grad_lower

    return jax.shard_map(per_device, mesh=mesh, in_specs=(block_spec, block_spec, block_spec), out_specs=(block_spec, block_spec), check_vma=False)
```
